128 devices in a mesh: rep: 2 (over core), dp: 64 (over x, y, z).
Axes of the slice: x: 4, y: 4, z: 4, core: 2. Of those that a mesh axis runs over, the one named last changes fastest.
Arguments:
- x: bfloat16 [128, 2048, 1280], P(('rep', 'dp')), parts along dimension 0
- dy: bfloat16 [128, 2048, 1280], P(('rep', 'dp')), parts along dimension 0
- w_gate: bfloat16 [2, 1280, 3072], P(None, 'dp')
- w_up: bfloat16 [2, 1280, 3072], P(None, 'dp')
- w_down: bfloat16 [2, 3072, 1280], P(None, 'dp')
Outputs:
- output 1: bfloat16 [128, 2048, 1280], P(('rep', 'dp')), parts along dimension 0
- output 2: bfloat16 [4, 1280, 3072], P('rep', 'dp'), parts along dimension 0
- output 3: bfloat16 [4, 1280, 3072], P('rep', 'dp'), parts along dimension 0
- output 4: bfloat16 [4, 3072, 1280], P('rep', 'dp'), parts along dimension 0
There are 2 independent parts. The reference program is written for one: setup_inputs(seed, part) draws one part's arguments, and reference() takes and returns one part's arrays. A program takes and returns all parts, laid end to end along the dimension named above; an argument that names none is the same for every part.
All inputs are finite; a program needn't handle non-finite values.
Results may differ from the reference program's by a relative error of at most 0.018.
Values are sent between devices in bfloat16 or wider.
A program may use at most 1.5 GiB of HBM per device.

```python
import jax
import jax.numpy as jnp
from jax import lax

SEQUENCES = 64
TOKENS = 2048
D = 1280
FF = 3072
LAYERS = 2
NAMES = ("w_gate", "w_up", "w_down")
SHAPES = {"w_gate": (LAYERS, D, FF), "w_up": (LAYERS, D, FF), "w_down": (LAYERS, FF, D)}


def bump(key, n, height):
    away = (jnp.arange(n, dtype=jnp.int32) - jax.random.randint(key, (), 0, n, jnp.int32)) % n
    return jnp.where(away < n // 8, height, 1.0)


def together(key, own, strength):
    shared = jax.random.normal(key, own.shape[1:], jnp.float32)
    return (own + strength * shared) * lax.rsqrt(1 + strength * strength)


def setup_inputs(seed: int = 0, part: int = 0) -> dict:
    kx, kdy, ka, kb, kz, kf, kh, kl, *kw = jax.random.split(jax.random.key(seed), 8 + len(NAMES))
    kx, kdy, ka, kb = (jax.random.fold_in(k, part) for k in (kx, kdy, ka, kb))
    shape = (SEQUENCES, TOKENS, D)
    much_x, much_dy = jax.random.uniform(kz, (2,), jnp.float32, 0.0, 1.0)
    layers = 2.0 ** jax.random.uniform(kl, (LAYERS, 1, 1), jnp.float32, -1.0, 1.0)
    x = together(ka, jax.random.normal(kx, shape, jnp.float32), much_x) * bump(kf, D, 4.0)
    dy = together(kb, jax.random.normal(kdy, shape, jnp.float32), much_dy)
    drawn = {"x": x.astype(jnp.bfloat16), "dy": (dy * (SEQUENCES * TOKENS) ** -0.5).astype(jnp.bfloat16)}
    for key, name in zip(kw, NAMES, strict=True):
        w = jax.random.normal(key, SHAPES[name], jnp.float32) * SHAPES[name][1] ** -0.5
        drawn[name] = (w * {"w_gate": 1.0, "w_up": bump(kh, FF, 4.0), "w_down": layers}[name]).astype(jnp.bfloat16)
    return drawn


def matmul(a, w):
    return jnp.dot(a, w, preferred_element_type=jnp.float32).astype(jnp.bfloat16)


def normed(h):
    wide = h.astype(jnp.float32)
    scale = lax.rsqrt(jnp.mean(wide**2, -1, keepdims=True) + 1e-6)
    return (wide * scale).astype(jnp.bfloat16)


def layer(h, w):
    a = normed(h)
    gate = jnp.dot(a, w["w_gate"], preferred_element_type=jnp.float32)
    up = jnp.dot(a, w["w_up"], preferred_element_type=jnp.float32)
    return h + matmul((jax.nn.silu(gate) * up).astype(jnp.bfloat16), w["w_down"])


def stack(weights, h):
    return lax.scan(lambda h, w: (layer(h, w), None), h, weights)[0]


def reference(x, dy, w_gate, w_up, w_down):
    weights = dict(zip(NAMES, (w_gate, w_up, w_down), strict=True))

    def take(so_far, sequence):
        h, by_y = sequence
        _, back = jax.vjp(stack, weights, h)
        by_weights, by_h = back(by_y)
        return jax.tree.map(lambda total, term: total + term.astype(jnp.float32), so_far, by_weights), by_h

    none_yet = {name: jnp.zeros(w.shape, jnp.float32) for name, w in weights.items()}
    by_weights, by_x = lax.scan(take, none_yet, (x, dy))
    return (by_x, *(by_weights[name].astype(jnp.bfloat16) for name in NAMES))
```

```python
import jax
import jax.numpy as jnp
from jax import lax
from jax.experimental import pallas as pl
from jax.experimental.pallas import tpu as pltpu
from jax.sharding import PartitionSpec as P

MESH = pl.DeviceIdType.MESH
BF = jnp.bfloat16
F32 = jnp.float32
L, D, FF, T = 2, 1280, 3072, 2048
RING = 4
ROWS = D // 64
JOINED = RING * ROWS
DROWS = FF // 64
CH = 512
HC = CH // 2
NJ = FF // CH
UNITS = L * NJ
MXU = 256
ND = D // MXU
ALL = slice(None)
HALVES = (lambda: ALL, lambda: pl.ds(0, 2), lambda: pl.ds(2, 2))
NN = (((1,), (0,)), ((), ()))
NT = (((1,), (1,)), ((), ()))
LANES = 128


def dot(a, b, dims=NN):
    return lax.dot_general(a, b, dims, preferred_element_type=F32)


def local(src, dst, sem):
    return pltpu.make_async_copy(src, dst, sem)


def remote(src, dst, send, recv, device):
    return pltpu.make_async_remote_copy(src_ref=src, dst_ref=dst, send_sem=send, recv_sem=recv, device_id=device, device_id_type=MESH)


def aligned(start, size):
    return pl.ds(pl.multiple_of(start, LANES), size)


def piece(index, size):
    return aligned(index * size, size)


def mod(a, n):
    return lax.rem(a, n)


def div(a, n):
    return lax.div(a, n)


class Place:
    def __init__(self):
        self.core = lax.axis_index("rep")
        self.dp = lax.axis_index("dp")
        self.other = 1 - self.core
        self.place, self.device = {}, {}
        for stride, axis in ((RING**2, "x"), (RING, "y"), (1, "z")):
            at = mod(div(self.dp, stride), RING)
            for by in range(RING):
                self.place[axis, by] = mod(at + by, RING)
                self.device[axis, by] = (self.core, self.dp + (self.place[axis, by] - at) * stride)

    def to(self, axis, by):
        return self.device[axis, by % RING]

    def index(self, axis, by=0):
        return self.place[axis, by % RING]

    def partner(self):
        return (self.other, self.dp)

    def greet(self, others):
        barrier = pltpu.get_barrier_semaphore()
        for other in others:
            pl.semaphore_signal(barrier, inc=1, device_id=other, device_id_type=MESH)
        pl.semaphore_wait(barrier, len(others))


class Gather:
    def __init__(self, place, full, own, send, recv):
        self.p, self.full, self.own, self.send, self.recv = place, full, own, send, recv

    def ring(self, axis, ref, parts, receive):
        s, r = (-1, 1) if receive else (0, 0)
        whole, low, high = parts
        right, left = self.p.to(axis, 1), self.p.to(axis, -1)
        return [(lambda: ref(s, whole()), right), (lambda: ref(r, whole()), left), (lambda: ref(s - 1, low()), right), (lambda: ref(r + 1, high()), left)]

    def hand(self, ref):
        return [(lambda by=by: ref(by), self.p.partner()) for by in (0, -1, 1, 2)]

    def copy(self, k, u, receive=False):
        table = self.table(u, receive)
        ref, device = table[k][0](), table[k][1]
        src = self.mine(u) if k < 2 and not receive else ref
        return remote(src, ref, self.send.at[(*self.sems(u), k)], self.recv.at[(*self.sems(u), k)], device)

    def keep(self, u):
        return local(self.mine(u), self.table(u, False)[0][0](), self.send.at[(*self.sems(u), self.COPIES)])

    def event(self, k, u):
        ends = self.COPIES - 4
        waits, starts = [], []
        if 0 < 2 * k <= ends:
            waits = [2 * k - 2, 2 * k - 1]
        if 2 * k < ends:
            starts = [2 * k, 2 * k + 1]
        if 2 * k == ends - 4:
            starts += [ends]
        if 2 * k == ends - 2:
            starts += [ends + 1, ends + 2]
        if 2 * k == ends:
            starts = [ends + 3]
        if 2 * k > ends:
            waits = range(ends, ends + 4)
        if k == 0:
            self.keep(u).start()
        for i in waits:
            self.copy(i, u, True).wait_recv()
        if k == 2:
            self.keep(u).wait()
        for i in starts:
            self.copy(i, u).start()

    def drain(self, u):
        for k in range(self.COPIES):
            self.copy(k, u).wait_send()


class GatherUp(Gather):
    COPIES = 12

    def __init__(self, which, *rest):
        super().__init__(*rest)
        self.which = which
        self.axes = "yx" if which else "xy"

    def sems(self, u):
        return (u, self.which)

    def mine(self, u):
        return self.own.at[u, self.which]

    def row(self, u, b, cols, a):
        full = self.full.reshape(L, RING, RING, JOINED, FF)
        return full.at[div(u, NJ), b, a, :, cols] if self.which else full.at[div(u, NJ), a, b, :, cols]

    def table(self, u, receive):
        p = self.p
        a, b = self.axes

        def cols(lo, size, core=p.core):
            return lambda: aligned(mod(u, NJ) * CH + core * HC + lo, size)

        mine = cols(0, HC)
        given = cols(0, HC, p.other) if receive else mine
        parts = (mine, cols(0, LANES), cols(LANES, LANES))
        first = self.ring(a, lambda by, c: self.row(u, p.index(b), c, p.index(a, by)), parts, receive)
        second = self.ring(b, lambda by, part: self.row(u, p.index(b, by), mine(), part), HALVES, receive)
        return first + second + self.hand(lambda by: self.row(u, p.index(b, by), given(), ALL))


class GatherDown(Gather):
    COPIES = 16
    HALF = D // 2
    CUT = 384
    TICKS = ((0, 1, 2, 3, 4, 7, 9, 10), (5, 6, 7, 8, 9, 12, 14, 16))

    def sems(self, v):
        return (v,)

    def cols(self, core):
        return aligned(core * self.HALF, self.HALF)

    def mine(self, v):
        return self.own.at[v, :, self.cols(self.p.core)]

    def table(self, v, receive):
        p = self.p
        x, y, z = (p.index(a) for a in "xyz")
        given = p.other if receive else p.core
        start = p.core * self.HALF
        parts = (lambda: self.cols(p.core), lambda: aligned(start, self.CUT), lambda: aligned(start + self.CUT, self.HALF - self.CUT))
        full = self.full.reshape(L, RING, RING, RING, DROWS, D)
        first = self.ring("x", lambda by, c: full.at[v, p.index("x", by), y, z, :, c], parts, receive)
        second = self.ring("y", lambda by, part: full.at[v, part, p.index("y", by), z, :, self.cols(p.core)], HALVES, receive)
        third = self.ring("z", lambda by, part: full.at[v, part, :, p.index("z", by), :, self.cols(p.core)], HALVES, receive)
        return first + second + third + self.hand(lambda by: full.at[v, :, :, p.index("z", by), :, self.cols(given)])


class Gathers:
    def __init__(self, place, fulls, zcat, wd, us, ur, ds, dr):
        self.ups = [GatherUp(m, place, fulls[m], zcat, us, ur) for m in range(2)]
        self.down = GatherDown(place, fulls[2], wd, ds, dr)

    def tick(self, t):
        for k, (one, two) in enumerate(zip(*GatherDown.TICKS)):

            @pl.when((t == one) | (t == two))
            def _():
                self.down.event(k, jnp.where(t == two, 1, 0))

        for k in range(GATHER_LAG + 1):
            u = t - k

            @pl.when((u >= 0) & (u < UNITS))
            def _():
                for up in self.ups:
                    up.event(k, u)

    def drain(self):
        @pl.loop(0, UNITS)
        def _(u):
            for up in self.ups:
                up.drain(u)

        @pl.loop(0, L)
        def _(v):
            self.down.drain(v)


GATHER_LAG = 5


def along_z(place, wz, zbuf, zcat, send, recv, between):
    z = place.index("z")

    def copy(l, by, receive):
        slot = place.index("z", -by) if receive else z
        return remote(wz.at[l], zbuf.at[slot, l], send.at[l, by - 1], recv.at[l, by - 1], place.to("z", by))

    pairs = [(l, by) for l in range(L) for by in range(1, RING)]
    for l, by in pairs:
        copy(l, by, False).start()
    between()
    zbuf[z] = wz[...]
    for l, by in pairs:
        copy(l, by, True).wait_recv()
    for l, by in pairs:
        copy(l, by, False).wait_send()

    @pl.loop(0, UNITS)
    def _(u):
        for m in range(2):
            pieces = [zbuf[i, div(u, NJ), m, mod(u, NJ)].astype(F32) for i in range(RING)]
            zcat[u, m] = jnp.concatenate(pieces, axis=0).astype(BF)


class Ring:
    def __init__(self, place, axis, src, opposite, block, send, recv):
        self.p, self.axis, self.src, self.opposite, self.block, self.send, self.recv = place, axis, src, opposite, block, send, recv

    def copy(self, k, src, dst):
        return remote(src, dst, self.send(k), self.recv(k), self.p.to(self.axis, -1 if k % 2 else 1))

    def first(self):
        p, a = self.p, self.axis
        far = [self.copy(w, self.src(p.index(a, 2), w), self.opposite(w)) for w in range(2)]
        near = [self.copy(2 + w, self.src(p.index(a, 1 - 2 * w), 1 - w), self.block(w, 1 - w)) for w in range(2)]
        return far + near

    def second(self, sums):
        return [self.copy(4 + w, sums.at[w], self.block(w, w)) for w in range(2)]

    def wait_opposite(self):
        for w in range(2):
            self.copy(w, self.opposite(w), self.opposite(w)).wait_recv()

    def wait_block(self):
        for w in range(2):
            for k, half in ((2, 1 - w), (4, w)):
                self.copy(k + w, self.block(w, half), self.block(w, half)).wait_recv()


def every(lead, body):
    if not lead:
        body(())
        return
    count = 1
    for n in lead:
        count *= n

    @pl.loop(0, count)
    def _(i):
        body((div(i, lead[-1]), mod(i, lead[-1])) if len(lead) == 2 else (i,))


class Reduce:
    EVENTS = 9
    SEMS = 18
    SLOTS = 3
    FAR = 6
    KINDS = {
        "gate": ("xyz", NJ, CH, (RING,), JOINED, ROWS),
        "up": ("yxz", NJ, CH, (RING,), JOINED, ROWS),
        "down": ("zxy", ND, MXU, (RING, RING), DROWS, DROWS),
    }

    def __init__(self, place, kind, term, out, hbm, far, near, sems):
        self.p, self.kind, self.out = place, kind, out
        self.axes, self.n, self.width, self.lead, _, _ = self.KINDS[kind]
        self.down = kind == "down"
        self.term_ref = term.reshape(L, RING, RING, RING, DROWS, D) if self.down else term.reshape(L, RING, RING, JOINED, FF)
        self.half = self.width // 2
        self.count = L * self.n
        self.x1o, self.x1f = hbm
        self.x2o, self.x2f, self.x3o, self.x3f = far
        self.vo, self.vw, self.v1, self.vf, self.s, self.sb, self.v2, self.t, self.tb, self.v3 = near
        self.ls, self.send, self.recv = sems

    @classmethod
    def scratch(cls, kind):
        _, n, w, lead, rows, last = cls.KINDS[kind]
        h, count = w // 2, L * n
        block, mid, end = (*lead, rows), (*lead[1:], rows), (last,)
        dma, vm = pltpu.SemaphoreType.DMA, pltpu.VMEM
        hbm = [jax.ShapeDtypeStruct((count, 2, *block, c), BF) for c in (h, w)]
        far = [vm((cls.FAR, 2, *shape, c), BF) for shape in (mid, end) for c in (h, w)]
        near = [vm((2, *block, h), BF)] * 3 + [vm((3, *block, w), BF)]
        near += [vm((cls.SLOTS, *block, w), F32), vm((cls.SLOTS, *block, w), BF), vm((2, *mid, h), BF)]
        near += [vm((cls.SLOTS, RING, *end, w), F32), vm((cls.SLOTS, RING, *end, w), BF), vm((2, *end, h), BF)]
        return hbm, far, near, [dma((7,)), dma((count, cls.SEMS)), dma((count, cls.SEMS))]

    def halves(self, half):
        return pl.ds(half * self.half, self.half)

    def cut(self, ref, half):
        return ref.at[(ALL,) * (len(ref.shape) - 1) + (self.halves(half),)]

    def layer(self, u):
        return L - 1 - div(u, self.n)

    def term(self, u, q, half=None):
        start = mod(u, self.n) * self.width
        cols = aligned(start, self.width) if half is None else aligned(start + half * self.half, self.half)
        if self.down:
            return self.term_ref.at[self.layer(u), :, :, q, :, cols]
        if self.kind == "up":
            return self.term_ref.at[self.layer(u), :, q, :, cols]
        return self.term_ref.at[self.layer(u), q, :, :, cols]

    def ring(self, phase, u):
        sems = [lambda k, r=r: r.at[u, phase * 6 + k] for r in (self.send, self.recv)]
        far, near = mod(u, self.FAR), mod(u, self.SLOTS)
        if phase == 0:
            src, opposite, block = lambda q, h: self.term(u, q, h), self.x1o.at[u], self.x1f.at[u]
        elif phase == 1:
            src, opposite, block = lambda q, h: self.cut(self.sb.at[near, q], h), self.x2o.at[far], self.x2f.at[far]
        else:
            src, opposite, block = lambda q, h: self.cut(self.tb.at[near, q], h), self.x3o.at[far], self.x3f.at[far]
        return Ring(self.p, self.axes[phase], src, lambda w: opposite.at[w], lambda w, h: self.cut(block.at[w], h), *sems)

    def loads(self, u, blocks):
        a = self.axes[0]
        if blocks:
            pairs = [(self.x1f.at[u, w], self.vf.at[w]) for w in range(2)] + [(self.term(u, self.p.index(a)), self.vf.at[2])]
        else:
            pairs = [(self.x1o.at[u, w], self.vo.at[w]) for w in range(2)]
            pairs += [(self.term(u, self.p.index(a, 1 - 2 * w), w), self.vw.at[w]) for w in range(2)]
        return [local(s, d, self.ls.at[4 * blocks + i]) for i, (s, d) in enumerate(pairs)]

    def wait_sends(self, phase, u, second):
        ring = self.ring(phase, u)
        for copy in ring.second((self.v1, self.v2, self.v3)[phase]) if second else ring.first():
            copy.wait_send()

    def reuse(self, phase, u, second):
        back = 1 if second else self.SLOTS

        @pl.when(u >= back)
        def _():
            self.wait_sends(phase, u - back, second)

    def start(self, u):
        for copy in self.ring(0, u).first():
            copy.start()

    def load_opposite(self, u):
        self.ring(0, u).wait_opposite()
        for copy in self.loads(u, False):
            copy.start()

    def add_opposite(self, u):
        for copy in self.loads(u, False):
            copy.wait()
        self.reuse(0, u, True)

        def add(i):
            for w in range(2):
                self.v1[(w, *i)] = (self.vo[(w, *i)].astype(F32) + self.vw[(w, *i)].astype(F32)).astype(BF)

        every(self.lead, add)
        for copy in self.ring(0, u).second(self.v1):
            copy.start()

    def load_block(self, u):
        self.ring(0, u).wait_block()
        for copy in self.loads(u, True):
            copy.start()

    def add_block(self, u):
        for copy in self.loads(u, True):
            copy.wait()
        self.reuse(1, u, False)
        slot = mod(u, self.SLOTS)

        def add(i):
            own, left, right = (self.vf[(w, *i)].astype(F32) for w in (2, 0, 1))
            total = own + left + right
            self.s[(slot, *i)] = total
            self.sb[(slot, *i)] = total.astype(BF)

        every(self.lead, add)
        for copy in self.ring(1, u).first():
            copy.start()

    def opposite(self, u, phase, lead, kept, came, sums):
        ring = self.ring(phase, u)
        ring.wait_opposite()
        self.reuse(phase, u, True)
        axis = self.axes[phase]
        slot, far = mod(u, self.SLOTS), mod(u, self.FAR)

        def add(i):
            for w in range(2):
                own = kept[(slot, self.p.index(axis, 1 - 2 * w), *i, ALL, self.halves(w))]
                sums[(w, *i)] = (own + came[(far, w, *i)].astype(F32)).astype(BF)

        every(lead, add)
        for copy in ring.second(sums):
            copy.start()

    def middle(self, u):
        self.opposite(u, 1, self.lead[1:], self.s, self.x2o, self.v2)

    def turn(self, u):
        self.ring(1, u).wait_block()
        self.reuse(2, u, False)
        slot, far = mod(u, self.SLOTS), mod(u, self.FAR)
        q = self.p.index(self.axes[1])

        def total(i):
            return self.s[(slot, q, *i)] + self.x2f[(far, 0, *i)].astype(F32) + self.x2f[(far, 1, *i)].astype(F32)

        def put(i, value):
            self.t[slot, i] = value
            self.tb[slot, i] = value.astype(BF)

        if self.down:
            every(self.lead[1:], lambda i: put(*i, total(i)))
        else:
            whole = total(())
            for i in range(RING):
                put(i, whole[ROWS * i : ROWS * (i + 1)])
        for copy in self.ring(2, u).first():
            copy.start()

    def last(self, u):
        self.opposite(u, 2, (), self.t, self.x3o, self.v3)

    def finish(self, u):
        self.ring(2, u).wait_block()
        far = mod(u, self.FAR)
        total = self.t[mod(u, self.SLOTS), self.p.index(self.axes[2])] + self.x3f[far, 0].astype(F32) + self.x3f[far, 1].astype(F32)
        self.out[self.layer(u), :, piece(mod(u, self.n), self.width)] = total.astype(BF)

    def events(self):
        return (self.start, self.load_opposite, self.add_opposite, self.load_block, self.add_block, self.middle, self.turn, self.last, self.finish)

    def drain(self):
        @pl.loop(0, self.count)
        def _(u):
            self.wait_sends(0, u, False)

            @pl.when(u >= self.count - 1)
            def _():
                for phase in range(3):
                    self.wait_sends(phase, u, True)

            @pl.when(u >= self.count - self.SLOTS)
            def _():
                for phase in (1, 2):
                    self.wait_sends(phase, u, False)


class Reduces:
    PERIOD = ND + 2 * NJ + 8
    START = {"down": (2, 3), "gate": (ND + 3, 2), "up": (ND + 3, 2)}
    LAGS = {"down": (0, 3, 4, 7, 8, 10, 12, 14, 16), "gate": (0, 2, 3, 6, 7, 9, 11, 13, 15), "up": (0, 2, 3, 6, 7, 9, 11, 13, 15)}

    def __init__(self, units):
        self.units = units

    def ticks(self):
        return max(first + (u.n - 1) * gap + self.LAGS[u.kind][-1] for u, *_ in self.units for first, gap in (self.START[u.kind],)) + 1

    def tick(self, s):
        order = (0, *range(Reduce.EVENTS - 1, 0, -1))
        for k in order:
            for units in self.units:
                one = units[0]
                first, gap = self.START[one.kind]
                q = s - (first + self.LAGS[one.kind][k])
                r = mod(q, self.PERIOD)

                @pl.when((q >= 0) & (mod(r, gap) == 0) & (r < gap * one.n))
                def _():
                    u = div(q, self.PERIOD) * one.n + div(r, gap)

                    @pl.when(u < one.count)
                    def _():
                        for unit in units:
                            unit.events()[k](u)

    def drain(self):
        for units in self.units:
            for unit in units:
                unit.drain()


def scale_of(wide):
    return lax.rsqrt(jnp.mean(wide * wide, -1, keepdims=True) + 1e-6)


def save_normed(h, rows, a, at, dst, sems, i):
    wide = h.astype(F32)
    tile = (wide * scale_of(wide)).astype(BF)
    a[rows, :] = tile
    slot = mod(i, 2)
    copy = local(at.at[slot], dst.at[:, rows], sems.at[slot])

    @pl.when(i >= 2)
    def _():
        copy.wait()

    at[slot] = tile.T
    copy.start()


def wait_normed(at, dst, sems):
    for slot in range(2):
        local(at.at[slot], dst.at[:, piece(slot, MXU)], sems.at[slot]).wait()


TILE = 4 * MXU


def forward(gathers, fulls, ps, qs, ats, acts, hs, xb, a, at, wb, pq, actt, act, dn, sx, sa, sw, so, sd):
    def weights(l, j):
        return [local(fulls[m].at[l, :, piece(j, CH)], wb.at[mod(j, 2), m], sw.at[mod(j, 2), m]) for m in range(2)]

    def outs(l, s):
        slot = mod(s, 2)
        rows, cols = piece(slot, TILE), piece(div(s, 2), CH)
        pairs = [(pq.at[slot, 0], ps.at[l, rows, cols]), (pq.at[slot, 1], qs.at[l, rows, cols]), (actt.at[slot], acts.at[l, cols, rows])]
        return [local(src, dst, so.at[slot, i]) for i, (src, dst) in enumerate(pairs)]

    keep = local(xb, hs.at[0], sx.at[0])
    keep.start()
    down = local(fulls[2].at[0], dn, sd.at[0])

    @pl.loop(0, GATHER_LAG + 1)
    def _(t):
        gathers.tick(t)

    @pl.loop(0, L)
    def _(l):
        for copy in weights(l, 0):
            copy.start()

        @pl.loop(0, 2 * NJ)
        def _(s):
            j, i = div(s, 2), mod(s, 2)
            slot = mod(j, 2)

            @pl.when(i == 0)
            def _():
                for copy in weights(l, j):
                    copy.wait()

            @pl.when(i == 1)
            def _():
                gathers.tick(GATHER_LAG + 1 + j + l * (NJ + 2))

                @pl.when(j < NJ - 1)
                def _():
                    for copy in weights(l, j + 1):
                        copy.start()

                @pl.when((j == NJ - 1) & (l == 0))
                def _():
                    down.start()

            @pl.when(s >= 2)
            def _():
                for copy in outs(l, s - 2):
                    copy.wait()

            for n in range(TILE // MXU):
                rows = piece(i * (TILE // MXU) + n, MXU)
                part = pl.ds(n * MXU, MXU)
                for half in range(2):
                    cols = pl.ds(half * MXU, MXU)
                    gate, up = (dot(a[rows, :], wb[slot, m, :, cols]) for m in range(2))
                    h = 0.5 * gate
                    t = jnp.tanh(h)
                    e = 1.0 + t
                    silu = h * e
                    pq[i, 0, part, cols] = silu
                    pq[i, 1, part, cols] = (0.5 * up) * (e * (1.0 + h * (1.0 - t)))
                    tile = (silu * up).astype(BF)
                    act[rows, aligned(j * CH + half * MXU, MXU)] = tile
                    actt[i, cols, part] = tile.T
            for copy in outs(l, s):
                copy.start()

        for s in (2 * NJ - 2, 2 * NJ - 1):
            for copy in outs(l, s):
                copy.wait()

        @pl.when(l == 0)
        def _():
            keep.wait()
            down.wait()

            @pl.loop(0, T // CH)
            def _(i):
                @pl.when(mod(i, 2) == 1)
                def _():
                    gathers.tick(GATHER_LAG + NJ + 1 + div(i, 2))

                rows = piece(i, CH)
                y = dot(act[rows, :], dn[...]).astype(BF)
                xb[rows, :] = (xb[rows, :].astype(F32) + y.astype(F32)).astype(BF)
                for n in range(2):
                    sub = piece(2 * i + n, MXU)
                    save_normed(xb[sub, :], sub, a, at, ats.at[1], sa, 2 * i + n)

            wait_normed(at, ats.at[1], sa)
            local(xb, hs.at[1], sx.at[0]).start()

    local(xb, hs.at[1], sx.at[0]).wait()


def by_down(l, base, tick, acts, td, dh, av, st, sl, so):
    load = local(acts.at[l], av, sl)
    load.start()

    def out(i):
        return local(st.at[mod(i, 2)], td.at[l, :, piece(i, MXU)], so.at[mod(i, 2)])

    @pl.loop(0, ND)
    def _(i):
        @pl.when(i == 0)
        def _():
            load.wait()

        @pl.when(i >= 2)
        def _():
            out(i - 2).wait()

        tick(base + i)
        st[mod(i, 2)] = dot(av[...], dh[:, piece(i, MXU)]).astype(BF)
        out(i).start()

    for i in (ND - 2, ND - 1):
        out(i).wait()


def by_gate_and_up(l, base, tick, wdf, ps, qs, ats, dgs, terms, dh, atv, wdb, pq, dgu, stw, sl, sw, sp, sd, so):
    tiles = T // CH

    def weights(j):
        return local(wdf.at[l, piece(j, CH), :], wdb.at[mod(j, 2)], sw.at[mod(j, 2)])

    def factors(s):
        rows, cols, slot = piece(mod(s, tiles), CH), piece(div(s, tiles), CH), mod(s, 2)
        return [local(src.at[l, rows, cols], pq.at[slot, i], sp.at[slot, i]) for i, src in enumerate((ps, qs))]

    def hidden(j):
        return [local(dgu.at[m], dgs[m].at[:, piece(j, CH)], sd.at[m]) for m in range(2)]

    def out(j):
        return [local(stw.at[m], terms[m].at[l, :, piece(j, CH)], so.at[m]) for m in range(2)]

    load = local(ats.at[l], atv, sl)
    weights(0).start()
    for copy in factors(0):
        copy.start()
    load.start()

    def to_hidden(j):
        weights(j).wait()

        @pl.when(j < NJ - 1)
        def _():
            weights(j + 1).start()

        @pl.when(j > 0)
        def _():
            for copy in hidden(j - 1):
                copy.wait()

        @pl.loop(0, tiles)
        def _(i):
            s = j * tiles + i
            slot = mod(s, 2)
            for copy in factors(s):
                copy.wait()

            @pl.when(s < NJ * tiles - 1)
            def _():
                for copy in factors(s + 1):
                    copy.start()

            for n in range(2):
                rows, part = piece(2 * i + n, MXU), pl.ds(n * MXU, MXU)
                by_act = dot(dh[rows, :], wdb[mod(j, 2)], NT).astype(BF).astype(F32)
                for m in range(2):
                    dgu[m, rows, :] = (by_act * pq[slot, 1 - m, part, :]).astype(BF)

        for copy in hidden(j):
            copy.start()

    def to_weights(j):
        @pl.when(j == 0)
        def _():
            load.wait()

        for m in range(2):
            stw[m] = dot(atv[...], dgu[m]).astype(BF)
        for copy in out(j):
            copy.start()

    @pl.loop(0, 2 * NJ)
    def _(h):
        j, late = div(h, 2), mod(h, 2)

        @pl.when((late == 1) & (j > 0))
        def _():
            for copy in out(j - 1):
                copy.wait()

        tick(base + h)
        pl.when(late == 0)(lambda: to_hidden(j))
        pl.when(late == 1)(lambda: to_weights(j))

    for copy in hidden(NJ - 1) + out(NJ - 1):
        copy.wait()


def by_input(l, base, tick, fulls, dgs, hs, dh, wv, gt, ht, sw, sg, sh):
    load = [local(fulls[m].at[l], wv.at[m], sw.at[m]) for m in range(2)]
    tiles = T // MXU

    def rows_of(i):
        rows, slot = piece(i, MXU), mod(i, 2)
        return [local(dgs[m].at[rows, :], gt.at[slot, m], sg.at[slot, m]) for m in range(2)] + [local(hs.at[l, rows, :], ht.at[slot], sh.at[slot])]

    for copy in rows_of(0) + load:
        copy.start()

    @pl.loop(0, tiles)
    def _(i):
        tick(base + i)
        for copy in rows_of(i):
            copy.wait()

        @pl.when(i < tiles - 1)
        def _():
            for copy in rows_of(i + 1):
                copy.start()

        @pl.when(i == 0)
        def _():
            for copy in load:
                copy.wait()

        rows, slot = piece(i, MXU), mod(i, 2)
        by_a = [dot(gt[slot, m], wv[m], NT).astype(BF).astype(F32) for m in range(2)]
        total = by_a[0] + by_a[1]
        wide = ht[slot].astype(F32)
        scale = scale_of(wide)
        along = jnp.mean(total * wide, -1, keepdims=True) * (scale * scale * scale)
        by_h = (total * scale - wide * along).astype(BF).astype(F32)
        dh[rows, :] = (dh[rows, :].astype(F32) + by_h).astype(BF)


def kernel(x, dy, wz, wd, dx, og, ou, od, *refs):
    def take(n):
        nonlocal refs
        head, refs = refs[:n], refs[n:]
        return head

    fulls, (ps, qs, ats, acts, hs), dgs, terms = take(3), take(5), take(2), take(3)
    hbm = [take(2) for _ in KINDS]
    zbuf, zcat, zs, zr = take(4)
    sems = take(4)
    far = [take(4) for _ in KINDS]
    rsems = [take(3) for _ in KINDS]
    sx, sa, sw, so, sd, sp, sg = take(7)
    place = Place()
    place.greet([place.to(a, by) for a in "xy" for by in (1, -1)] + [place.to("z", by) for by in range(1, RING)] + [place.partner()])
    gathers = Gathers(place, fulls, zcat, wd, *sems)
    dma, vm = pltpu.SemaphoreType.DMA, pltpu.VMEM

    def ahead(xb, a, at, wb, pq, actt, act, dn):
        first = local(x, xb, sx.at[0])
        first.start()

        def norm():
            first.wait()

            @pl.loop(0, T // MXU)
            def _(i):
                rows = piece(i, MXU)
                save_normed(xb[rows, :], rows, a, at, ats.at[0], sa, i)

            wait_normed(at, ats.at[0], sa)

        along_z(place, wz, zbuf, zcat, zs, zr, norm)
        forward(gathers, fulls, ps, qs, ats, acts, hs, xb, a, at, wb, pq, actt, act, dn, sx, sa, sw, so, sd)
        gathers.drain()

    pl.run_scoped(
        ahead,
        vm((T, D), BF),
        vm((T, D), BF),
        vm((2, D, MXU), BF),
        vm((2, 2, D, CH), BF),
        vm((2, 2, TILE, CH), F32),
        vm((2, CH, TILE), BF),
        vm((T, FF), BF),
        vm((FF, D), BF),
    )

    def back(dh, *near):
        split = [near[i * 10 : i * 10 + 10] for i in range(3)]
        units = [
            Reduce(place, kind, terms[i], (og, ou, od)[i], hbm[i], far[i], split[i], rsems[i]) for i, kind in enumerate(KINDS)
        ]
        reduces = Reduces([units[2:], units[:2]])
        first = local(dy, dh, sx.at[0])
        first.start()
        first.wait()
        period = Reduces.PERIOD

        @pl.loop(0, L)
        def _(step):
            l, base = L - 1 - step, step * period
            pl.run_scoped(
                lambda av, st: by_down(l, base, reduces.tick, acts, terms[2], dh, av, st, sd.at[0], so.at[0]),
                vm((FF, T), BF),
                vm((2, FF, MXU), BF),
            )
            pl.run_scoped(
                lambda *v: by_gate_and_up(
                    l, base + ND, reduces.tick, fulls[2], ps, qs, ats, dgs, terms, dh, *v, sd.at[0], sw.at[0], sp, sg.at[0], so.at[0]
                ),
                vm((D, T), BF),
                vm((2, CH, D), BF),
                vm((2, 2, CH, CH), F32),
                vm((2, T, CH), BF),
                vm((2, D, CH), BF),
            )
            pl.run_scoped(
                lambda *v: by_input(l, base + ND + 2 * NJ, reduces.tick, fulls, dgs, hs, dh, *v, sw.at[0], sg, sd),
                vm((2, D, FF), BF),
                vm((2, 2, MXU, FF), BF),
                vm((2, MXU, D), BF),
            )

        end = local(dh, dx, sx.at[0])
        end.start()

        @pl.loop(L * period, reduces.ticks() + (L - 1) * period)
        def _(s):
            reduces.tick(s)

        end.wait()
        reduces.drain()

    pl.run_scoped(back, vm((T, D), BF), *(v for kind in KINDS for v in Reduce.scratch(kind)[2]))


KINDS = ("gate", "up", "down")


def call(x, dy, wz, wd):
    made = [Reduce.scratch(kind) for kind in KINDS]
    vmem, hbm = pl.BlockSpec(memory_space=pltpu.VMEM), pl.BlockSpec(memory_space=pltpu.HBM)
    dma, vm = pltpu.SemaphoreType.DMA, pltpu.VMEM

    def shape(*dims, dtype=BF):
        return jax.ShapeDtypeStruct(dims, dtype)

    work = [shape(L, D, FF), shape(L, D, FF), shape(L, FF, D)]
    work += [shape(L, T, FF, dtype=F32), shape(L, T, FF, dtype=F32), shape(L, D, T), shape(L, FF, T), shape(L, T, D)]
    work += [shape(T, FF), shape(T, FF), shape(L, D, FF), shape(L, D, FF), shape(L, FF, D)]
    work += [s for m in made for s in m[0]]
    outs = [shape(L, ROWS, FF), shape(L, ROWS, FF), shape(L, DROWS, D)]
    return pl.pallas_call(
        kernel,
        out_shape=(shape(T, D), *outs, *work),
        in_specs=[hbm, hbm, vmem, vmem],
        out_specs=(hbm, *(vmem for _ in outs), *(hbm for _ in work)),
        scratch_shapes=[
            vm((RING, L, 2, NJ, ROWS, HC), BF),
            vm((UNITS, 2, JOINED, HC), BF),
            dma((L, RING - 1)),
            dma((L, RING - 1)),
            dma((UNITS, 2, GatherUp.COPIES + 1)),
            dma((UNITS, 2, GatherUp.COPIES)),
            dma((L, GatherDown.COPIES + 1)),
            dma((L, GatherDown.COPIES)),
            *(s for m in made for s in m[1]),
            *(s for m in made for s in m[3]),
            dma((1,)),
            dma((2,)),
            dma((2, 2)),
            dma((2, 3)),
            dma((2,)),
            dma((2, 2)),
            dma((2, 2)),
        ],
        name="train",
        compiler_params=pltpu.CompilerParams(collective_id=0, has_side_effects=True, vmem_limit_bytes=67_000_000),
    )(x, dy, wz, wd)[:4]


def solution(mesh):
    def step(x, dy, w_gate, w_up, w_down):
        wz = jnp.stack([w_gate, w_up], 1).reshape(L, 2, ROWS, NJ, 2, HC)
        wz = lax.dynamic_index_in_dim(wz, lax.axis_index("rep"), 4, keepdims=False).transpose(0, 1, 3, 2, 4)
        by_x, *by_w = call(x[0], dy[0], wz, w_down)
        return (by_x[None], *by_w)

    both, rows = P(("rep", "dp"), None, None), P(None, "dp", None)
    return jax.shard_map(
        step,
        mesh=mesh,
        in_specs=(both, both, rows, rows, rows),
        out_specs=(both, *(P("rep", "dp", None),) * 3),
        check_vma=False,
    )
```

```python
import jax
import jax.numpy as jnp
from jax import lax
from jax.experimental import pallas as pl
from jax.experimental.pallas import tpu as pltpu
from jax.sharding import PartitionSpec as P

MESH = pl.DeviceIdType.MESH
BF = jnp.bfloat16
F32 = jnp.float32
L, D, FF, T = 2, 1280, 3072, 2048
RING = 4
ROWS = D // 64
JOINED = RING * ROWS
DROWS = FF // 64
CH = 512
HC = CH // 2
NJ = FF // CH
UNITS = L * NJ
MXU = 256
ND = D // MXU
ALL = slice(None)
HALVES = (lambda: ALL, lambda: pl.ds(0, 2), lambda: pl.ds(2, 2))
NN = (((1,), (0,)), ((), ()))
NT = (((1,), (1,)), ((), ()))
LANES = 128


def dot(a, b, dims=NN):
    return lax.dot_general(a, b, dims, preferred_element_type=F32)


def local(src, dst, sem):
    return pltpu.make_async_copy(src, dst, sem)


def remote(src, dst, send, recv, device):
    return pltpu.make_async_remote_copy(src_ref=src, dst_ref=dst, send_sem=send, recv_sem=recv, device_id=device, device_id_type=MESH)


def aligned(start, size):
    return pl.ds(pl.multiple_of(start, LANES), size)


def piece(index, size):
    return aligned(index * size, size)


def mod(a, n):
    return lax.rem(a, n)


def div(a, n):
    return lax.div(a, n)


class Place:
    def __init__(self):
        self.core = lax.axis_index("rep")
        self.dp = lax.axis_index("dp")
        self.other = 1 - self.core
        self.place, self.device = {}, {}
        for stride, axis in ((RING**2, "x"), (RING, "y"), (1, "z")):
            at = mod(div(self.dp, stride), RING)
            for by in range(RING):
                self.place[axis, by] = mod(at + by, RING)
                self.device[axis, by] = (self.core, self.dp + (self.place[axis, by] - at) * stride)

    def to(self, axis, by):
        return self.device[axis, by % RING]

    def index(self, axis, by=0):
        return self.place[axis, by % RING]

    def partner(self):
        return (self.other, self.dp)

    def greet(self, others):
        barrier = pltpu.get_barrier_semaphore()
        for other in others:
            pl.semaphore_signal(barrier, inc=1, device_id=other, device_id_type=MESH)
        pl.semaphore_wait(barrier, len(others))


class Gather:
    def __init__(self, place, full, own, send, recv):
        self.p, self.full, self.own, self.send, self.recv = place, full, own, send, recv

    def ring(self, axis, ref, parts):
        whole, low, high = parts
        right, left = self.p.to(axis, 1), self.p.to(axis, -1)
        return [(lambda: ref(0, whole()), right), (lambda: ref(0, whole()), left), (lambda: ref(-1, low()), right), (lambda: ref(1, high()), left)]

    def hand(self, ref):
        return [(lambda by=by: ref(by), self.p.partner()) for by in (0, -1, 1, 2)]

    def copy(self, k, u):
        ref, device = self.table(u)[k][0](), self.table(u)[k][1]
        group = min(k // 2, self.GROUPS - 1)
        return remote(self.mine(u) if k < 2 else ref, ref, self.send.at[(*self.sems(u), group)], self.recv.at[(*self.sems(u), group)], device)

    def all_of(self, group, u):
        blocks = RING ** (group // 2) * (1 if group % 2 else 2)
        ref = self.some(u, RING**self.RINGS if group == self.GROUPS - 1 else blocks)
        return remote(ref, ref, self.send.at[(*self.sems(u), group)], self.recv.at[(*self.sems(u), group)], self.p.partner())

    def keep(self, u):
        return local(self.mine(u), self.table(u)[0][0](), self.send.at[(*self.sems(u), self.GROUPS)])

    def event(self, k, u):
        ends = 2 * self.RINGS
        starts = [2 * k, 2 * k + 1] if k < ends else []
        hand = {ends - 2: [0], ends - 1: [1, 2], ends: [3]}.get(k, [])
        if k == 0:
            self.keep(u).start()
        else:
            self.all_of(k - 1, u).wait_recv()
        if k == 2:
            self.keep(u).wait()
        for i in starts + [2 * ends + i for i in hand]:
            self.copy(i, u).start()

    def drain(self, u):
        for group in range(self.GROUPS):
            self.all_of(group, u).wait_send()


def first_blocks(count, dims):
    index = []
    for _ in range(dims):
        index.insert(0, ALL if count >= RING else pl.ds(0, count) if count > 1 else 0)
        count = max(count // RING, 1)
    return tuple(index)


class GatherUp(Gather):
    RINGS = 2
    GROUPS = 2 * RINGS + 1

    def __init__(self, which, *rest):
        super().__init__(*rest)
        self.which = which
        self.axes = "yx" if which else "xy"

    def sems(self, u):
        return (u, self.which)

    def mine(self, u):
        return self.own.at[u, self.which]

    def row(self, u, b, cols, a):
        full = self.full.reshape(L, RING, RING, JOINED, FF)
        return full.at[div(u, NJ), b, a, :, cols] if self.which else full.at[div(u, NJ), a, b, :, cols]

    def cols(self, u, lo=0, size=HC):
        return aligned(mod(u, NJ) * CH + self.p.core * HC + lo, size)

    def some(self, u, count):
        return self.full.reshape(L, RING, RING, JOINED, FF).at[(div(u, NJ), *first_blocks(count, 2), ALL, self.cols(u))]

    def table(self, u):
        p = self.p
        a, b = self.axes
        parts = (lambda: self.cols(u), lambda: self.cols(u, 0, LANES), lambda: self.cols(u, LANES, LANES))
        first = self.ring(a, lambda by, c: self.row(u, p.index(b), c, p.index(a, by)), parts)
        second = self.ring(b, lambda by, part: self.row(u, p.index(b, by), self.cols(u), part), HALVES)
        return first + second + self.hand(lambda by: self.row(u, p.index(b, by), self.cols(u), ALL))


class GatherDown(Gather):
    RINGS = 3
    GROUPS = 2 * RINGS + 1
    HALF = D // 2
    CUT = 384
    TICKS = ((2, 6, 7, 9, 11, 19, 23, 24), (14, 16, 24, 27, 29, 35, 40, 41))

    def sems(self, v):
        return (v,)

    def cols(self):
        return aligned(self.p.core * self.HALF, self.HALF)

    def mine(self, v):
        return self.own.at[v, :, self.cols()]

    def some(self, v, count):
        return self.full.reshape(L, RING, RING, RING, DROWS, D).at[(v, *first_blocks(count, 3), ALL, self.cols())]

    def table(self, v):
        p = self.p
        x, y, z = (p.index(a) for a in "xyz")
        start = p.core * self.HALF
        parts = (self.cols, lambda: aligned(start, self.CUT), lambda: aligned(start + self.CUT, self.HALF - self.CUT))
        full = self.full.reshape(L, RING, RING, RING, DROWS, D)
        first = self.ring("x", lambda by, c: full.at[v, p.index("x", by), y, z, :, c], parts)
        second = self.ring("y", lambda by, part: full.at[v, part, p.index("y", by), z, :, self.cols()], HALVES)
        third = self.ring("z", lambda by, part: full.at[v, part, :, p.index("z", by), :, self.cols()], HALVES)
        return first + second + third + self.hand(lambda by: full.at[v, :, :, p.index("z", by), :, self.cols()])


class Gathers:
    GAP = 2
    LAGS = (0, 4, 7, 10, 12, 13)
    AHEAD = LAGS[-1] + 1
    DEEP = T // CH

    def __init__(self, place, fulls, zcat, wd, us, ur, ds, dr):
        self.ups = [GatherUp(m, place, fulls[m], zcat, us, ur) for m in range(2)]
        self.down = GatherDown(place, fulls[2], wd, ds, dr)

    def tick(self, t):
        for k, (one, two) in enumerate(zip(*GatherDown.TICKS)):

            @pl.when((t == one) | (t == two))
            def _():
                self.down.event(k, jnp.where(t == two, 1, 0))

        for k in reversed(range(len(self.LAGS))):
            q = t - self.LAGS[k]
            u = div(q, self.GAP)

            @pl.when((q >= 0) & (mod(q, self.GAP) == 0) & (u < UNITS))
            def _():
                for up in self.ups:
                    up.event(k, u)

    def drain(self):
        @pl.loop(0, UNITS)
        def _(u):
            for up in self.ups:
                up.drain(u)

        @pl.loop(0, L)
        def _(v):
            self.down.drain(v)


class AlongZ:
    def __init__(self, place, wz, zbuf, zcat, send, recv):
        self.p, self.wz, self.zbuf, self.zcat, self.send, self.recv = place, wz, zbuf, zcat, send, recv
        self.z = place.index("z")

    def copy(self, l, by, receive):
        slot = self.p.index("z", -by) if receive else self.z
        return remote(self.wz.at[l], self.zbuf.at[slot, l], self.send.at[l, by - 1], self.recv.at[l, by - 1], self.p.to("z", by))

    def start(self):
        for l in range(L):
            for by in range(1, RING):
                self.copy(l, by, False).start()
        self.zbuf[self.z] = self.wz[...]

    def wait(self, l):
        for by in range(1, RING):
            self.copy(l, by, True).wait_recv()
        for by in range(1, RING):
            self.copy(l, by, False).wait_send()

    def join(self, u):
        for m in range(2):
            pieces = [self.zbuf[i, div(u, NJ), m, mod(u, NJ)].astype(F32) for i in range(RING)]
            self.zcat[u, m] = jnp.concatenate(pieces, axis=0).astype(BF)


class Ring:
    def __init__(self, place, axis, src, opposite, block, send, recv):
        self.p, self.axis, self.src, self.opposite, self.block, self.send, self.recv = place, axis, src, opposite, block, send, recv

    def copy(self, step, part, way, src, dst):
        return remote(src, dst, self.send(step), self.recv(2 * part + way), self.p.to(self.axis, 1 - 2 * way))

    def first(self):
        p, a = self.p, self.axis
        far = [self.copy(0, 0, w, self.src(p.index(a, 2), w), self.opposite(w)) for w in range(2)]
        near = [self.copy(0, 1, w, self.src(p.index(a, 1 - 2 * w), 1 - w), self.block(w, 1 - w)) for w in range(2)]
        return far + near

    def second(self, sums):
        return [self.copy(1, 1, w, sums.at[w], self.block(w, w)) for w in range(2)]

    def wait_opposite(self):
        for w in range(2):
            self.copy(0, 0, w, self.opposite(w), self.opposite(w)).wait_recv()

    def wait_block(self):
        for w in range(2):
            self.copy(0, 1, w, self.block(w), self.block(w)).wait_recv()

    def wait_sent(self, step, ref):
        self.copy(step, 0, 0, ref, ref).wait_send()


def every(lead, body):
    if not lead:
        body(())
        return
    count = 1
    for n in lead:
        count *= n

    @pl.loop(0, count)
    def _(i):
        body((div(i, lead[-1]), mod(i, lead[-1])) if len(lead) == 2 else (i,))


class Reduce:
    EVENTS = 9
    SLOTS = 2
    FAR = 6
    KINDS = {
        "gate": ("xyz", NJ, CH, (RING,), JOINED, ROWS),
        "up": ("yxz", NJ, CH, (RING,), JOINED, ROWS),
        "down": ("zxy", ND, MXU, (RING, RING), DROWS, DROWS),
    }

    def __init__(self, place, kind, term, out, hbm, far, near, sems):
        self.p, self.kind, self.out = place, kind, out
        self.axes, self.n, self.width, self.lead, _, _ = self.KINDS[kind]
        self.down = kind == "down"
        self.term_ref = term.reshape(L, RING, RING, RING, DROWS, D) if self.down else term.reshape(L, RING, RING, JOINED, FF)
        self.half = self.width // 2
        self.count = L * self.n
        self.x1o, self.x1f = hbm
        self.x2o, self.x2f, self.x3o, self.x3f = far
        self.vo, self.vw, self.v1, self.vf, self.s, self.sb, self.v2, self.t, self.tb, self.v3 = near
        self.ls, self.send, self.recv = sems

    @classmethod
    def scratch(cls, kind):
        _, n, w, lead, rows, last = cls.KINDS[kind]
        h, count = w // 2, L * n
        block, mid, end = (*lead, rows), (*lead[1:], rows), (last,)
        dma, vm = pltpu.SemaphoreType.DMA, pltpu.VMEM
        hbm = [jax.ShapeDtypeStruct((count, 2, *block, c), BF) for c in (h, w)]
        far = [vm((cls.FAR, 2, *shape, c), BF) for shape in (mid, end) for c in (h, w)]
        near = [vm((2, *block, h), BF)] * 3 + [vm((3, *block, w), BF)]
        near += [vm((cls.SLOTS, *block, w), F32), vm((cls.SLOTS, *block, w), BF), vm((2, *mid, h), BF)]
        near += [vm((cls.SLOTS, RING, *end, w), F32), vm((cls.SLOTS, RING, *end, w), BF), vm((2, *end, h), BF)]
        return hbm, far, near, [dma((7,)), dma((cls.FAR, 3 * 2)), dma((cls.FAR, 3 * 4))]

    def halves(self, half):
        return pl.ds(half * self.half, self.half)

    def cut(self, ref, half):
        return ref.at[(ALL,) * (len(ref.shape) - 1) + (self.halves(half),)]

    def layer(self, u):
        return L - 1 - div(u, self.n)

    def term(self, u, q, half=None):
        start = mod(u, self.n) * self.width
        cols = aligned(start, self.width) if half is None else aligned(start + half * self.half, self.half)
        if self.down:
            return self.term_ref.at[self.layer(u), :, :, q, :, cols]
        if self.kind == "up":
            return self.term_ref.at[self.layer(u), :, q, :, cols]
        return self.term_ref.at[self.layer(u), q, :, :, cols]

    def ring(self, phase, u):
        far, near = mod(u, self.FAR), mod(u, self.SLOTS)
        sems = (lambda k: self.send.at[far, 2 * phase + k], lambda k: self.recv.at[far, 4 * phase + k])
        if phase == 0:
            src, opposite, block = lambda q, h: self.term(u, q, h), self.x1o.at[u], self.x1f.at[u]
        elif phase == 1:
            src, opposite, block = lambda q, h: self.cut(self.sb.at[near, q], h), self.x2o.at[far], self.x2f.at[far]
        else:
            src, opposite, block = lambda q, h: self.cut(self.tb.at[near, q], h), self.x3o.at[far], self.x3f.at[far]
        return Ring(self.p, self.axes[phase], src, lambda w: opposite.at[w], lambda w, h=None: block.at[w] if h is None else self.cut(block.at[w], h), *sems)

    def loads(self, u, blocks):
        a = self.axes[0]
        if blocks:
            pairs = [(self.x1f.at[u, w], self.vf.at[w]) for w in range(2)] + [(self.term(u, self.p.index(a)), self.vf.at[2])]
        else:
            pairs = [(self.x1o.at[u, w], self.vo.at[w]) for w in range(2)]
            pairs += [(self.term(u, self.p.index(a, 1 - 2 * w), w), self.vw.at[w]) for w in range(2)]
        return [local(s, d, self.ls.at[4 * blocks + i]) for i, (s, d) in enumerate(pairs)]

    def wait_sends(self, phase, u, second):
        far = mod(u, self.FAR)
        sums, blocks = ((self.v1, self.x1f.at[u]), (self.v2, self.x2f.at[far]), (self.v3, self.x3f.at[far]))[phase]
        self.ring(phase, u).wait_sent(second, sums if second else blocks)

    def reuse(self, phase, u, second):
        back = 1 if second else self.SLOTS if phase else self.FAR

        @pl.when(u >= back)
        def _():
            self.wait_sends(phase, u - back, second)

    def start(self, u):
        self.reuse(0, u, False)
        for copy in self.ring(0, u).first():
            copy.start()

    def load_opposite(self, u):
        self.ring(0, u).wait_opposite()
        for copy in self.loads(u, False):
            copy.start()

    def add_opposite(self, u):
        for copy in self.loads(u, False):
            copy.wait()
        self.reuse(0, u, True)

        def add(i):
            for w in range(2):
                self.v1[(w, *i)] = (self.vo[(w, *i)].astype(F32) + self.vw[(w, *i)].astype(F32)).astype(BF)

        every(self.lead, add)
        for copy in self.ring(0, u).second(self.v1):
            copy.start()

    def load_block(self, u):
        self.ring(0, u).wait_block()
        for copy in self.loads(u, True):
            copy.start()

    def add_block(self, u):
        for copy in self.loads(u, True):
            copy.wait()
        self.reuse(1, u, False)
        slot = mod(u, self.SLOTS)

        def add(i):
            own, left, right = (self.vf[(w, *i)].astype(F32) for w in (2, 0, 1))
            total = own + left + right
            self.s[(slot, *i)] = total
            self.sb[(slot, *i)] = total.astype(BF)

        every(self.lead, add)
        for copy in self.ring(1, u).first():
            copy.start()

    def opposite(self, u, phase, lead, kept, came, sums):
        ring = self.ring(phase, u)
        ring.wait_opposite()
        self.reuse(phase, u, True)
        axis = self.axes[phase]
        slot, far = mod(u, self.SLOTS), mod(u, self.FAR)

        def add(i):
            for w in range(2):
                own = kept[(slot, self.p.index(axis, 1 - 2 * w), *i, ALL, self.halves(w))]
                sums[(w, *i)] = (own + came[(far, w, *i)].astype(F32)).astype(BF)

        every(lead, add)
        for copy in ring.second(sums):
            copy.start()

    def middle(self, u):
        self.opposite(u, 1, self.lead[1:], self.s, self.x2o, self.v2)

    def turn(self, u):
        self.ring(1, u).wait_block()
        self.reuse(2, u, False)
        slot, far = mod(u, self.SLOTS), mod(u, self.FAR)
        q = self.p.index(self.axes[1])

        def total(i):
            return self.s[(slot, q, *i)] + self.x2f[(far, 0, *i)].astype(F32) + self.x2f[(far, 1, *i)].astype(F32)

        def put(i, value):
            self.t[slot, i] = value
            self.tb[slot, i] = value.astype(BF)

        if self.down:
            every(self.lead[1:], lambda i: put(*i, total(i)))
        else:
            whole = total(())
            for i in range(RING):
                put(i, whole[ROWS * i : ROWS * (i + 1)])
        for copy in self.ring(2, u).first():
            copy.start()

    def last(self, u):
        self.opposite(u, 2, (), self.t, self.x3o, self.v3)

    def finish(self, u):
        self.ring(2, u).wait_block()
        far = mod(u, self.FAR)
        total = self.t[mod(u, self.SLOTS), self.p.index(self.axes[2])] + self.x3f[far, 0].astype(F32) + self.x3f[far, 1].astype(F32)
        self.out[self.layer(u), :, piece(mod(u, self.n), self.width)] = total.astype(BF)

    def events(self):
        return (self.start, self.load_opposite, self.add_opposite, self.load_block, self.add_block, self.middle, self.turn, self.last, self.finish)

    def drain(self):
        @pl.loop(0, self.count)
        def _(u):
            @pl.when(u >= self.count - self.FAR)
            def _():
                self.wait_sends(0, u, False)

            @pl.when(u >= self.count - 1)
            def _():
                for phase in range(3):
                    self.wait_sends(phase, u, True)

            @pl.when(u >= self.count - self.SLOTS)
            def _():
                for phase in (1, 2):
                    self.wait_sends(phase, u, False)


class Reduces:
    PERIOD = ND + 2 * NJ + 8
    START = {"down": (7, 2), "gate": (ND + 3, 2)}
    LAGS = {"down": (0, 3, 5, 8, 10, 12, 14, 17, 18), "gate": (0, 2, 3, 7, 8, 10, 12, 14, 16)}

    def __init__(self, units):
        self.units = units

    def ticks(self):
        return max(first + (u.n - 1) * gap + self.LAGS[u.kind][-1] for u, *_ in self.units for first, gap in (self.START[u.kind],)) + 1

    def tick(self, s):
        for k in reversed(range(Reduce.EVENTS)):
            for units in self.units:
                one = units[0]
                first, gap = self.START[one.kind]
                q = s - (first + self.LAGS[one.kind][k])
                r = mod(q, self.PERIOD)

                @pl.when((q >= 0) & (mod(r, gap) == 0) & (r < gap * one.n))
                def _():
                    u = div(q, self.PERIOD) * one.n + div(r, gap)

                    @pl.when(u < one.count)
                    def _():
                        for unit in units:
                            unit.events()[k](u)

    def drain(self):
        for units in self.units:
            for unit in units:
                unit.drain()


def scale_of(wide):
    return lax.rsqrt(jnp.mean(wide * wide, -1, keepdims=True) + 1e-6)


def save_normed(h, rows, a, at, dst, sems, i):
    wide = h.astype(F32)
    tile = (wide * scale_of(wide)).astype(BF)
    a[rows, :] = tile
    slot = mod(i, 2)
    copy = local(at.at[slot], dst.at[:, rows], sems.at[slot])

    @pl.when(i >= 2)
    def _():
        copy.wait()

    at[slot] = tile.T
    copy.start()


def wait_normed(at, dst, sems):
    for slot in range(2):
        local(at.at[slot], dst.at[:, piece(slot, MXU)], sems.at[slot]).wait()


TILE = 4 * MXU


def forward(first, along_z, gathers, fulls, ps, qs, ats, acts, hs, xb, a, at, wb, pq, actt, act, dn, sx, sa, sw, so, sd):
    def weights(l, j):
        return [local(fulls[m].at[l, :, piece(j, CH)], wb.at[mod(j, 2), m], sw.at[mod(j, 2), m]) for m in range(2)]

    def outs(l, s):
        slot = mod(s, 2)
        rows, cols = piece(slot, TILE), piece(div(s, 2), CH)
        pairs = [(pq.at[slot, 0], ps.at[l, rows, cols]), (pq.at[slot, 1], qs.at[l, rows, cols]), (actt.at[slot], acts.at[l, cols, rows])]
        return [local(src, dst, so.at[slot, i]) for i, (src, dst) in enumerate(pairs)]

    keep = local(xb, hs.at[0], sx.at[0])
    down = local(fulls[2].at[0], dn, sd.at[0])
    along_z.start()
    along_z.wait(0)
    pl.loop(0, NJ)(along_z.join)
    first.wait()
    keep.start()

    @pl.loop(0, gathers.AHEAD)
    def _(t):
        gathers.tick(t)

        @pl.when(t == 0)
        def _():
            along_z.wait(1)

        @pl.when(t < NJ)
        def _():
            along_z.join(NJ + t)

        @pl.when(t < T // MXU)
        def _():
            rows = piece(t, MXU)
            save_normed(xb[rows, :], rows, a, at, ats.at[0], sa, t)

    wait_normed(at, ats.at[0], sa)

    @pl.loop(0, L)
    def _(l):
        for copy in weights(l, 0):
            copy.start()

        @pl.loop(0, 2 * NJ)
        def _(s):
            j, i = div(s, 2), mod(s, 2)
            slot = mod(j, 2)

            @pl.when(i == 0)
            def _():
                for copy in weights(l, j):
                    copy.wait()

            gathers.tick(gathers.AHEAD + l * (2 * NJ + gathers.DEEP) + s)

            @pl.when(i == 1)
            def _():
                @pl.when(j < NJ - 1)
                def _():
                    for copy in weights(l, j + 1):
                        copy.start()

                @pl.when((j == NJ - 1) & (l == 0))
                def _():
                    down.start()

            @pl.when(s >= 2)
            def _():
                for copy in outs(l, s - 2):
                    copy.wait()

            for n in range(TILE // MXU):
                rows = piece(i * (TILE // MXU) + n, MXU)
                part = pl.ds(n * MXU, MXU)
                for half in range(2):
                    cols = pl.ds(half * MXU, MXU)
                    gate, up = (dot(a[rows, :], wb[slot, m, :, cols]) for m in range(2))
                    h = 0.5 * gate
                    t = jnp.tanh(h)
                    e = 1.0 + t
                    silu = h * e
                    pq[i, 0, part, cols] = silu
                    pq[i, 1, part, cols] = (0.5 * up) * (e * (1.0 + h * (1.0 - t)))
                    tile = (silu * up).astype(BF)
                    act[rows, aligned(j * CH + half * MXU, MXU)] = tile
                    actt[i, cols, part] = tile.T
            for copy in outs(l, s):
                copy.start()

        for s in (2 * NJ - 2, 2 * NJ - 1):
            for copy in outs(l, s):
                copy.wait()

        @pl.when(l == 0)
        def _():
            keep.wait()
            down.wait()

            @pl.loop(0, T // CH)
            def _(i):
                gathers.tick(gathers.AHEAD + 2 * NJ + i)
                rows = piece(i, CH)
                y = dot(act[rows, :], dn[...]).astype(BF)
                xb[rows, :] = (xb[rows, :].astype(F32) + y.astype(F32)).astype(BF)
                for n in range(2):
                    sub = piece(2 * i + n, MXU)
                    save_normed(xb[sub, :], sub, a, at, ats.at[1], sa, 2 * i + n)

            wait_normed(at, ats.at[1], sa)
            local(xb, hs.at[1], sx.at[0]).start()

    local(xb, hs.at[1], sx.at[0]).wait()


def by_down(l, base, tick, first, acts, td, dh, av, st, sl, so):
    parts = 3

    def load(part):
        rows = piece(part, FF // parts)
        return local(acts.at[l, rows, :], av.at[rows, :], sl.at[part])

    for part in range(parts):
        load(part).start()

    def out(i):
        return local(st.at[mod(i, 2)], td.at[l, :, piece(i, MXU)], so.at[mod(i, 2)])

    @pl.loop(0, ND)
    def _(i):
        @pl.when(i >= 2)
        def _():
            out(i - 2).wait()

        tick(base + i)

        @pl.when(i == 0)
        def _():
            first()

            @pl.loop(0, parts)
            def _(part):
                load(part).wait()
                rows = piece(part, FF // parts)
                st[0, rows, :] = dot(av[rows, :], dh[:, :MXU]).astype(BF)

        @pl.when(i > 0)
        def _():
            st[mod(i, 2)] = dot(av[...], dh[:, piece(i, MXU)]).astype(BF)

        out(i).start()

    for i in (ND - 2, ND - 1):
        out(i).wait()


def by_gate_and_up(l, base, tick, ahead, wdf, ps, qs, ats, dgs, terms, dh, atv, wdb, pq, dgu, stw, sl, sw, sp, sd, so):
    tiles = T // TILE

    def weights(j):
        return local(wdf.at[l, piece(j, CH), :], wdb.at[mod(j, 2)], sw.at[mod(j, 2)])

    def factors(j, i):
        rows, cols = piece(i, TILE), piece(j, CH)
        return [local(src.at[l, rows, cols], pq.at[m, rows], sp.at[i, m]) for m, src in enumerate((qs, ps))]

    def load_factors(j):
        for i in range(tiles):
            for copy in factors(j, i):
                copy.start()

    def hidden(j):
        return [local(dgu.at[m], dgs[m].at[:, piece(j, CH)], sd.at[m]) for m in range(2)]

    def out(j):
        return [local(stw.at[m], terms[m].at[l, :, piece(j, CH)], so.at[m]) for m in range(2)]

    load = local(ats.at[l], atv, sl)
    weights(0).start()
    load_factors(0)
    load.start()

    def to_hidden(j):
        weights(j).wait()

        @pl.when(j < NJ - 1)
        def _():
            weights(j + 1).start()

        @pl.when(j > 0)
        def _():
            for copy in hidden(j - 1):
                copy.wait()

        @pl.loop(0, tiles)
        def _(i):
            for copy in factors(j, i):
                copy.wait()

            for n in range(TILE // MXU):
                rows = piece(i * (TILE // MXU) + n, MXU)
                for half in range(2):
                    cols = pl.ds(half * MXU, MXU)
                    by_act = dot(dh[rows, :], wdb[mod(j, 2), cols, :], NT).astype(BF).astype(F32)
                    for m in range(2):
                        dgu[m, rows, cols] = (by_act * pq[m, rows, cols]).astype(BF)

        for copy in hidden(j):
            copy.start()

    def to_weights(j):
        @pl.when(j == 0)
        def _():
            load.wait()

        @pl.when(j < NJ - 1)
        def _():
            load_factors(j + 1)

        @pl.when(j == NJ - 1)
        def _():
            ahead.start()

        for m in range(2):
            stw[m] = dot(atv[...], dgu[m]).astype(BF)
        for copy in out(j):
            copy.start()

    @pl.loop(0, 2 * NJ)
    def _(h):
        j, late = div(h, 2), mod(h, 2)

        @pl.when((late == 1) & (j > 0))
        def _():
            for copy in out(j - 1):
                copy.wait()

        tick(base + h)
        pl.when(late == 0)(lambda: to_hidden(j))
        pl.when(late == 1)(lambda: to_weights(j))

    for copy in hidden(NJ - 1) + out(NJ - 1):
        copy.wait()


def by_input(l, base, tick, ahead, full, dgs, hs, dh, first, second, gt, ht, sw, sg, sh):
    after = local(full.at[l], second, sw)
    tiles = T // MXU

    def rows_of(i):
        rows, slot = piece(i, MXU), mod(i, 2)
        return [local(dgs[m].at[rows, :], gt.at[slot, m], sg.at[slot, m]) for m in range(2)] + [local(hs.at[l, rows, :], ht.at[slot], sh.at[slot])]

    for copy in rows_of(0) + [after]:
        copy.start()

    @pl.loop(0, tiles)
    def _(i):
        tick(base + i)
        for copy in rows_of(i):
            copy.wait()

        @pl.when(i < tiles - 1)
        def _():
            for copy in rows_of(i + 1):
                copy.start()

        @pl.when(i == 0)
        def _():
            ahead.wait()
            after.wait()

        rows, slot = piece(i, MXU), mod(i, 2)
        by_a = [dot(gt[slot, m], w[...], NT).astype(BF).astype(F32) for m, w in enumerate((first, second))]
        total = by_a[0] + by_a[1]
        wide = ht[slot].astype(F32)
        scale = scale_of(wide)
        along = jnp.mean(total * wide, -1, keepdims=True) * (scale * scale * scale)
        by_h = (total * scale - wide * along).astype(BF).astype(F32)
        dh[rows, :] = (dh[rows, :].astype(F32) + by_h).astype(BF)


def kernel(x, dy, wz, wd, dx, og, ou, od, *refs):
    def take(n):
        nonlocal refs
        head, refs = refs[:n], refs[n:]
        return head

    fulls, (ps, qs, ats, acts, hs), dgs, terms = take(3), take(5), take(2), take(3)
    hbm = [take(2) for _ in KINDS]
    zbuf, zcat, zs, zr = take(4)
    sems = take(4)
    far = [take(4) for _ in KINDS]
    rsems = [take(3) for _ in KINDS]
    sx, sa, sw, so, sd, sp, sg = take(7)
    place = Place()
    gathers = Gathers(place, fulls, zcat, wd, *sems)
    dma, vm = pltpu.SemaphoreType.DMA, pltpu.VMEM

    def ahead(xb, a, at, wb, pq, actt, act, dn):
        first = local(x, xb, sx.at[0])
        first.start()
        place.greet([place.to(a, by) for a in "xy" for by in (1, -1)] + [place.to("z", by) for by in range(1, RING)] + [place.partner()])
        along_z = AlongZ(place, wz, zbuf, zcat, zs, zr)
        forward(first, along_z, gathers, fulls, ps, qs, ats, acts, hs, xb, a, at, wb, pq, actt, act, dn, sx, sa, sw, so, sd)
        gathers.drain()

    pl.run_scoped(
        ahead,
        vm((T, D), BF),
        vm((T, D), BF),
        vm((2, D, MXU), BF),
        vm((2, 2, D, CH), BF),
        vm((2, 2, TILE, CH), F32),
        vm((2, CH, TILE), BF),
        vm((T, FF), BF),
        vm((FF, D), BF),
    )

    def back(dh, *near):
        split = [near[i * 10 : i * 10 + 10] for i in range(3)]
        units = [
            Reduce(place, kind, terms[i], (og, ou, od)[i], hbm[i], far[i], split[i], rsems[i]) for i, kind in enumerate(KINDS)
        ]
        reduces = Reduces([units[2:], units[:2]])
        first = local(dy, dh, sx.at[0])
        first.start()
        period = Reduces.PERIOD

        @pl.loop(0, L)
        def _(step):
            l, base = L - 1 - step, step * period
            pl.run_scoped(
                lambda av, st: by_down(
                    l, base, reduces.tick, lambda: pl.when(step == 0)(first.wait), acts, terms[2], dh, av, st, sp.at[0], so.at[0]
                ),
                vm((FF, T), BF),
                vm((2, FF, MXU), BF),
            )

            def rest(weight):
                ahead = local(fulls[0].at[l], weight, sx.at[0])
                pl.run_scoped(
                    lambda *v: by_gate_and_up(
                        l, base + ND, reduces.tick, ahead, fulls[2], ps, qs, ats, dgs, terms, dh, *v, sd.at[0], sw.at[0], sp, sg.at[0], so.at[0]
                    ),
                    vm((D, T), BF),
                    vm((2, CH, D), BF),
                    vm((2, T, CH), F32),
                    vm((2, T, CH), BF),
                    vm((2, D, CH), BF),
                )
                pl.run_scoped(
                    lambda *v: by_input(l, base + ND + 2 * NJ, reduces.tick, ahead, fulls[1], dgs, hs, dh, weight, *v, sa.at[0], sg, sd),
                    vm((D, FF), BF),
                    vm((2, 2, MXU, FF), BF),
                    vm((2, MXU, D), BF),
                )

            pl.run_scoped(rest, vm((D, FF), BF))

        end = local(dh, dx, sx.at[0])
        end.start()

        @pl.loop(L * period, reduces.ticks() + (L - 1) * period)
        def _(s):
            reduces.tick(s)

        end.wait()
        reduces.drain()

    pl.run_scoped(back, vm((T, D), BF), *(v for kind in KINDS for v in Reduce.scratch(kind)[2]))


KINDS = ("gate", "up", "down")


def call(x, dy, wz, wd):
    made = [Reduce.scratch(kind) for kind in KINDS]
    vmem, hbm = pl.BlockSpec(memory_space=pltpu.VMEM), pl.BlockSpec(memory_space=pltpu.HBM)
    dma, vm = pltpu.SemaphoreType.DMA, pltpu.VMEM

    def shape(*dims, dtype=BF):
        return jax.ShapeDtypeStruct(dims, dtype)

    work = [shape(L, D, FF), shape(L, D, FF), shape(L, FF, D)]
    work += [shape(L, T, FF, dtype=F32), shape(L, T, FF, dtype=F32), shape(L, D, T), shape(L, FF, T), shape(L, T, D)]
    work += [shape(T, FF), shape(T, FF), shape(L, D, FF), shape(L, D, FF), shape(L, FF, D)]
    work += [s for m in made for s in m[0]]
    outs = [shape(L, ROWS, FF), shape(L, ROWS, FF), shape(L, DROWS, D)]
    return pl.pallas_call(
        kernel,
        out_shape=(shape(T, D), *outs, *work),
        in_specs=[hbm, hbm, vmem, vmem],
        out_specs=(hbm, *(vmem for _ in outs), *(hbm for _ in work)),
        scratch_shapes=[
            vm((RING, L, 2, NJ, ROWS, HC), BF),
            vm((UNITS, 2, JOINED, HC), BF),
            dma((L, RING - 1)),
            dma((L, RING - 1)),
            dma((UNITS, 2, GatherUp.GROUPS + 1)),
            dma((UNITS, 2, GatherUp.GROUPS)),
            dma((L, GatherDown.GROUPS + 1)),
            dma((L, GatherDown.GROUPS)),
            *(s for m in made for s in m[1]),
            *(s for m in made for s in m[3]),
            dma((1,)),
            dma((2,)),
            dma((2, 2)),
            dma((2, 3)),
            dma((2,)),
            dma((2, 3)),
            dma((2, 2)),
        ],
        name="train",
        compiler_params=pltpu.CompilerParams(collective_id=0, has_side_effects=True, vmem_limit_bytes=67_000_000),
    )(x, dy, wz, wd)[:4]


def solution(mesh):
    def step(x, dy, w_gate, w_up, w_down):
        wz = jnp.stack([w_gate, w_up], 1).reshape(L, 2, ROWS, NJ, 2, HC)
        wz = lax.dynamic_index_in_dim(wz, lax.axis_index("rep"), 4, keepdims=False).transpose(0, 1, 3, 2, 4)
        by_x, *by_w = call(x[0], dy[0], wz, w_down)
        return (by_x[None], *by_w)

    both, rows = P(("rep", "dp"), None, None), P(None, "dp", None)
    return jax.shard_map(
        step,
        mesh=mesh,
        in_specs=(both, both, rows, rows, rows),
        out_specs=(both, *(P("rep", "dp", None),) * 3),
        check_vma=False,
    )
```

```python
import jax
import jax.numpy as jnp
from jax import lax
from jax.experimental import pallas as pl
from jax.experimental.pallas import tpu as pltpu
from jax.sharding import PartitionSpec as P

MESH = pl.DeviceIdType.MESH
BF = jnp.bfloat16
F32 = jnp.float32
L, D, FF, T = 2, 1280, 3072, 2048
BOTH = range(2)
RING = 4
ROWS = D // 64
JOINED = RING * ROWS
DROWS = FF // 64
CH = 512
HC = CH // 2
NJ = FF // CH
UNITS = L * NJ
MXU = 256
ND = D // MXU
ALL = slice(None)
HALVES = (lambda: ALL, lambda: pl.ds(0, 2), lambda: pl.ds(2, 2))
NN = (((1,), (0,)), ((), ()))
NT = (((1,), (1,)), ((), ()))
LANES = 128


def dot(a, b, dims=NN):
    return lax.dot_general(a, b, dims, preferred_element_type=F32)


def local(src, dst, sem):
    return pltpu.make_async_copy(src, dst, sem)


def remote(src, dst, send, recv, device):
    return pltpu.make_async_remote_copy(src_ref=src, dst_ref=dst, send_sem=send, recv_sem=recv, device_id=device, device_id_type=MESH)


def aligned(start, size):
    return pl.ds(pl.multiple_of(start, LANES), size)


def piece(index, size):
    return aligned(index * size, size)


def mod(a, n):
    return lax.rem(a, n)


def div(a, n):
    return lax.div(a, n)


def side(way):
    return 1 - 2 * way


class Place:
    def __init__(self):
        self.core = lax.axis_index("rep")
        self.dp = lax.axis_index("dp")
        self.other = 1 - self.core
        self.place, self.device = {}, {}
        for stride, axis in ((RING**2, "x"), (RING, "y"), (1, "z")):
            at = mod(div(self.dp, stride), RING)
            for by in range(RING):
                self.place[axis, by] = mod(at + by, RING)
                self.device[axis, by] = (self.core, self.dp + (self.place[axis, by] - at) * stride)

    def to(self, axis, by):
        return self.device[axis, by % RING]

    def index(self, axis, by=0):
        return self.place[axis, by % RING]

    def partner(self):
        return (self.other, self.dp)

    def greet(self, others):
        barrier = pltpu.get_barrier_semaphore()
        for other in others:
            pl.semaphore_signal(barrier, inc=1, device_id=other, device_id_type=MESH)
        pl.semaphore_wait(barrier, len(others))


class Gather:
    def __init__(self, place, full, own, send, recv):
        self.p, self.full, self.own, self.send, self.recv = place, full, own, send, recv

    def ring(self, axis, ref, parts):
        whole, low, high = parts
        right, left = self.p.to(axis, 1), self.p.to(axis, -1)
        return [(lambda: ref(0, whole()), right), (lambda: ref(0, whole()), left), (lambda: ref(-1, low()), right), (lambda: ref(1, high()), left)]

    def hand(self, ref):
        return [(lambda by=by: ref(by), self.p.partner()) for by in (0, -1, 1, 2)]

    def copy(self, k):
        ref, device = self.table()[k][0](), self.table()[k][1]
        group = min(k // 2, self.GROUPS - 1)
        return remote(self.mine() if k < 2 else ref, ref, self.send.at[(*self.slot, group)], self.recv.at[(*self.slot, group)], device)

    def all_of(self, group):
        blocks = RING ** (group // 2) * (1 if group % 2 else 2)
        ref = self.some(RING**self.RINGS if group == self.GROUPS - 1 else blocks)
        return remote(ref, ref, self.send.at[(*self.slot, group)], self.recv.at[(*self.slot, group)], self.p.partner())

    def keep(self):
        return local(self.mine(), self.table()[0][0](), self.send.at[(*self.slot, self.GROUPS)])

    def event(self, k, l, j=0):
        self.unit(l, j)
        ends = 2 * self.RINGS
        starts = [2 * k, 2 * k + 1] if k < ends else []
        hand = {ends - 2: [0], ends - 1: [1, 2], ends: [3]}.get(k, [])
        if k < ends:
            self.free(k)
        if k == ends - 2:
            self.free(ends)
        if k == 0:
            self.keep().start()
        else:
            self.all_of(k - 1).wait_recv()
        if k == 2:
            self.keep().wait()
        for i in starts + [2 * ends + i for i in hand]:
            self.copy(i).start()

    def free(self, group):
        pass

    def drain(self, l, j=0):
        self.unit(l, j)
        for group in range(self.GROUPS):
            self.all_of(group).wait_send()


def first_blocks(count, dims):
    index = []
    for _ in range(dims):
        index.insert(0, ALL if count >= RING else pl.ds(0, count) if count > 1 else 0)
        count = max(count // RING, 1)
    return tuple(index)


class GatherUp(Gather):
    RINGS = 2
    GROUPS = 2 * RINGS + 1

    def __init__(self, which, *rest):
        super().__init__(*rest)
        self.which = which
        self.axes = "yx" if which else "xy"

    def unit(self, l, j):
        self.l, self.j, self.slot = l, j, (j, self.which)
        self.start = j * CH + self.p.core * HC

    def free(self, group):
        @pl.when(self.l > 0)
        def _():
            self.all_of(group).wait_send()

    def mine(self):
        return self.own.at[self.l * NJ + self.j, self.which]

    def cols(self, lo=0, size=HC):
        return aligned(self.start + lo, size)

    def view(self):
        return self.full.reshape(L, RING, RING, JOINED, FF)

    def row(self, b, cols, a):
        return self.view().at[self.l, b, a, :, cols] if self.which else self.view().at[self.l, a, b, :, cols]

    def some(self, count):
        return self.view().at[(self.l, *first_blocks(count, 2), ALL, self.cols())]

    def table(self):
        p = self.p
        a, b = self.axes
        parts = (self.cols, lambda: self.cols(0, LANES), lambda: self.cols(LANES, LANES))
        first = self.ring(a, lambda by, c: self.row(p.index(b), c, p.index(a, by)), parts)
        second = self.ring(b, lambda by, part: self.row(p.index(b, by), self.cols(), part), HALVES)
        return first + second + self.hand(lambda by: self.row(p.index(b, by), self.cols(), ALL))


class GatherDown(Gather):
    RINGS = 3
    GROUPS = 2 * RINGS + 1
    HALF = D // 2
    CUT = 384
    TICKS = ((0, 3, 7, 13, 16, 23, 26, 27), (20, 24, 26, 29, 31, 38, 42, 43))

    def unit(self, l, _):
        self.l, self.slot = l, (l,)

    def cols(self):
        return aligned(self.p.core * self.HALF, self.HALF)

    def mine(self):
        return self.own.at[self.l, :, self.cols()]

    def view(self):
        return self.full.reshape(L, RING, RING, RING, DROWS, D)

    def some(self, count):
        return self.view().at[(self.l, *first_blocks(count, 3), ALL, self.cols())]

    def table(self):
        p = self.p
        x, y, z = (p.index(a) for a in "xyz")
        start = p.core * self.HALF
        parts = (self.cols, lambda: aligned(start, self.CUT), lambda: aligned(start + self.CUT, self.HALF - self.CUT))
        full, v = self.view(), self.l
        first = self.ring("x", lambda by, c: full.at[v, p.index("x", by), y, z, :, c], parts)
        second = self.ring("y", lambda by, part: full.at[v, part, p.index("y", by), z, :, self.cols()], HALVES)
        third = self.ring("z", lambda by, part: full.at[v, part, :, p.index("z", by), :, self.cols()], HALVES)
        return first + second + third + self.hand(lambda by: full.at[v, :, :, p.index("z", by), :, self.cols()])


class Gathers:
    LAGS = (0, 6, 9, 12, 14, 15)
    AHEAD = LAGS[-1] + 1
    DEEP = T // CH

    def __init__(self, place, fulls, zcat, wd, us, ur, ds, dr):
        self.ups = [GatherUp(m, place, fulls[m], zcat, us, ur) for m in BOTH]
        self.down = GatherDown(place, fulls[2], wd, ds, dr)

    def tick(self, t):
        for odd in BOTH:

            @pl.when(t & 1 == odd)
            def _():
                for k in reversed(range(len(self.LAGS))):
                    if self.LAGS[k] % 2 == odd:
                        self.step(k, t - self.LAGS[k])

        for k, (one, two) in enumerate(zip(*GatherDown.TICKS)):

            @pl.when((t == one) | (t == two))
            def _():
                self.down.event(k, jnp.where(t == two, 1, 0))

    def step(self, k, q):
        @pl.when((q >= 0) & (q < 2 * UNITS))
        def _():
            u = q >> 1
            l = jnp.where(u >= NJ, 1, 0)
            for up in self.ups:
                up.event(k, l, u - NJ * l)

    def drain(self):
        @pl.loop(0, NJ)
        def _(j):
            for up in self.ups:
                up.drain(L - 1, j)

        @pl.loop(0, L)
        def _(v):
            self.down.drain(v)


class AlongZ:
    def __init__(self, place, wz, zbuf, zcat, send, recv):
        self.p, self.wz, self.zbuf, self.zcat, self.send, self.recv = place, wz, zbuf, zcat, send, recv
        self.z = place.index("z")

    PARTS = (0, 1, 3, NJ, UNITS)

    def copy(self, part, by, receive):
        units = pl.ds(self.PARTS[part], self.PARTS[part + 1] - self.PARTS[part])
        slot = self.p.index("z", -by) if receive else self.z
        sems = (self.send.at[part, by - 1], self.recv.at[part, by - 1])
        return remote(self.wz.at[units], self.zbuf.at[slot, units], *sems, self.p.to("z", by))

    def start(self):
        for part in range(len(self.PARTS) - 1):
            for by in range(1, RING):
                self.copy(part, by, False).start()
        self.zbuf[self.z] = self.wz[...]

    def finish(self, part):
        for receive in (True, False):
            for by in range(1, RING):
                copy = self.copy(part, by, receive)
                copy.wait_recv() if receive else copy.wait_send()

        @pl.loop(self.PARTS[part], self.PARTS[part + 1])
        def _(u):
            for m in BOTH:
                pieces = [self.zbuf[i, u, m].astype(F32) for i in range(RING)]
                self.zcat[u, m] = jnp.concatenate(pieces, axis=0).astype(BF)


class Ring:
    def __init__(self, place, axis, src, opposite, block, send, recv):
        self.p, self.axis, self.src, self.opposite, self.block, self.send, self.recv = place, axis, src, opposite, block, send, recv

    def copy(self, step, part, way, src, dst):
        return remote(src, dst, self.send(step), self.recv(2 * part + way), self.p.to(self.axis, side(way)))

    def first(self):
        p, a = self.p, self.axis
        far = [self.copy(0, 0, w, self.src(p.index(a, 2), w), self.opposite(w)) for w in BOTH]
        near = [self.copy(0, 1, w, self.src(p.index(a, side(w)), 1 - w), self.block(w, 1 - w)) for w in BOTH]
        return far + near

    def second(self, sums):
        return [self.copy(1, 1, w, sums.at[w], self.block(w, w)) for w in BOTH]

    def wait_opposite(self):
        for w in BOTH:
            self.copy(0, 0, w, self.opposite(w), self.opposite(w)).wait_recv()

    def wait_block(self):
        for w in BOTH:
            self.copy(0, 1, w, self.block(w), self.block(w)).wait_recv()

    def wait_sent(self, step, ref):
        self.copy(step, 0, 0, ref, ref).wait_send()


def every(lead, body):
    if not lead:
        body(())
        return
    count = 1
    for n in lead:
        count *= n

    @pl.loop(0, count)
    def _(i):
        body((div(i, lead[-1]), mod(i, lead[-1])) if len(lead) == 2 else (i,))


class Reduce:
    EVENTS = 9
    SLOTS = 2
    KINDS = {
        "gate": ("xyz", NJ, CH, (RING,), JOINED, ROWS),
        "up": ("yxz", NJ, CH, (RING,), JOINED, ROWS),
        "down": ("zxy", ND, MXU, (RING, RING), DROWS, DROWS),
    }

    def __init__(self, place, kind, term, out, hbm, far, near, sems):
        self.p, self.kind, self.out = place, kind, out
        self.axes, self.n, self.width, self.lead, _, _ = self.KINDS[kind]
        self.down = kind == "down"
        self.term_ref = term.reshape(L, RING, RING, RING, DROWS, D) if self.down else term.reshape(L, RING, RING, JOINED, FF)
        self.half = self.width // 2
        self.count = L * self.n
        self.x1o, self.x1f = hbm
        self.x2o, self.x2f, self.x3o, self.x3f = far
        self.vo, self.vw, self.v1, self.vf, self.s, self.sb, self.v2, self.t, self.tb, self.v3 = near
        self.ls, self.send, self.recv = sems

    def unit(self, step, j):
        self.l, self.j, self.u = L - 1 - step, j, step * self.n + j
        self.slot = self.u & 1

    @classmethod
    def scratch(cls, kind):
        _, n, w, lead, rows, last = cls.KINDS[kind]
        h, count = w // 2, L * n
        block, mid, end = (*lead, rows), (*lead[1:], rows), (last,)
        dma, vm = pltpu.SemaphoreType.DMA, pltpu.VMEM
        hbm = [jax.ShapeDtypeStruct((count, 2, *block, c), BF) for c in (h, w)]
        far = [vm((n, 2, *shape, c), BF) for shape in (mid, end) for c in (h, w)]
        near = [vm((2, *block, h), BF)] * 3 + [vm((3, *block, w), BF)]
        near += [vm((cls.SLOTS, *block, w), F32), vm((cls.SLOTS, *block, w), BF), vm((2, *mid, h), BF)]
        near += [vm((cls.SLOTS, RING, *end, w), F32), vm((cls.SLOTS, RING, *end, w), BF), vm((2, *end, h), BF)]
        return hbm, far, near, [dma((7,)), dma((n, 3 * 2)), dma((n, 3 * 4))]

    def halves(self, half):
        return pl.ds(half * self.half, self.half)

    def cut(self, ref, half):
        return ref.at[(ALL,) * (len(ref.shape) - 1) + (self.halves(half),)]

    def term(self, q, half=None):
        start = self.j * self.width
        cols = aligned(start, self.width) if half is None else aligned(start + half * self.half, self.half)
        if self.down:
            return self.term_ref.at[self.l, :, :, q, :, cols]
        if self.kind == "up":
            return self.term_ref.at[self.l, :, q, :, cols]
        return self.term_ref.at[self.l, q, :, :, cols]

    def ring(self, phase, j=None):
        j = self.j if j is None else j
        sems = (lambda k: self.send.at[j, 2 * phase + k], lambda k: self.recv.at[j, 4 * phase + k])
        if phase == 0:
            src, opposite, block = self.term, self.x1o.at[self.u], self.x1f.at[self.u]
        elif phase == 1:
            src, opposite, block = lambda q, h: self.cut(self.sb.at[self.slot, q], h), self.x2o.at[j], self.x2f.at[j]
        else:
            src, opposite, block = lambda q, h: self.cut(self.tb.at[self.slot, q], h), self.x3o.at[j], self.x3f.at[j]
        return Ring(self.p, self.axes[phase], src, lambda w: opposite.at[w], lambda w, h=None: block.at[w] if h is None else self.cut(block.at[w], h), *sems)

    def loads(self, blocks):
        a = self.axes[0]
        if blocks:
            pairs = [(self.x1f.at[self.u, w], self.vf.at[w]) for w in BOTH] + [(self.term(self.p.index(a)), self.vf.at[2])]
        else:
            pairs = [(self.x1o.at[self.u, w], self.vo.at[w]) for w in BOTH]
            pairs += [(self.term(self.p.index(a, side(w)), w), self.vw.at[w]) for w in BOTH]
        return [local(s, d, self.ls.at[4 * blocks + i]) for i, (s, d) in enumerate(pairs)]

    def wait_sends(self, phase, j, second):
        sums, blocks = ((self.v1, self.x1f.at[0]), (self.v2, self.x2f.at[0]), (self.v3, self.x3f.at[0]))[phase]
        self.ring(phase, j).wait_sent(second, sums if second else blocks)

    def reuse(self, phase, second):
        back = 1 if second else self.SLOTS if phase else self.n

        @pl.when(self.u >= back)
        def _():
            j = self.j - back
            self.wait_sends(phase, jnp.where(j < 0, j + self.n, j), second)

    def start(self):
        self.reuse(0, False)
        for copy in self.ring(0).first():
            copy.start()

    def load_opposite(self):
        self.ring(0).wait_opposite()
        for copy in self.loads(False):
            copy.start()

    def add_opposite(self):
        for copy in self.loads(False):
            copy.wait()
        self.reuse(0, True)

        def add(i):
            for w in BOTH:
                self.v1[(w, *i)] = (self.vo[(w, *i)].astype(F32) + self.vw[(w, *i)].astype(F32)).astype(BF)

        every(self.lead, add)
        for copy in self.ring(0).second(self.v1):
            copy.start()

    def load_block(self):
        self.ring(0).wait_block()
        for copy in self.loads(True):
            copy.start()

    def add_block(self):
        for copy in self.loads(True):
            copy.wait()
        self.reuse(1, False)

        def add(i):
            own, left, right = (self.vf[(w, *i)].astype(F32) for w in (2, 0, 1))
            total = own + left + right
            self.s[(self.slot, *i)] = total
            self.sb[(self.slot, *i)] = total.astype(BF)

        every(self.lead, add)
        for copy in self.ring(1).first():
            copy.start()

    def opposite(self, phase, lead, kept, came, sums):
        ring = self.ring(phase)
        ring.wait_opposite()
        self.reuse(phase, True)
        axis = self.axes[phase]

        def add(i):
            for w in BOTH:
                own = kept[(self.slot, self.p.index(axis, side(w)), *i, ALL, self.halves(w))]
                sums[(w, *i)] = (own + came[(self.j, w, *i)].astype(F32)).astype(BF)

        every(lead, add)
        for copy in ring.second(sums):
            copy.start()

    def middle(self):
        self.opposite(1, self.lead[1:], self.s, self.x2o, self.v2)

    def turn(self):
        self.ring(1).wait_block()
        self.reuse(2, False)
        q = self.p.index(self.axes[1])

        def total(i):
            return self.s[(self.slot, q, *i)] + self.x2f[(self.j, 0, *i)].astype(F32) + self.x2f[(self.j, 1, *i)].astype(F32)

        def put(i, value):
            self.t[self.slot, i] = value
            self.tb[self.slot, i] = value.astype(BF)

        if self.down:
            every(self.lead[1:], lambda i: put(*i, total(i)))
        else:
            whole = total(())
            for i in range(RING):
                put(i, whole[ROWS * i : ROWS * (i + 1)])
        for copy in self.ring(2).first():
            copy.start()

    def last(self):
        self.opposite(2, (), self.t, self.x3o, self.v3)

    def finish(self):
        self.ring(2).wait_block()
        total = self.t[self.slot, self.p.index(self.axes[2])] + self.x3f[self.j, 0].astype(F32) + self.x3f[self.j, 1].astype(F32)
        self.out[self.l, :, piece(self.j, self.width)] = total.astype(BF)

    def events(self):
        return (self.start, self.load_opposite, self.add_opposite, self.load_block, self.add_block, self.middle, self.turn, self.last, self.finish)

    def drain(self):
        @pl.loop(0, self.n)
        def _(j):
            self.unit(L - 1, j)
            self.wait_sends(0, j, False)

            @pl.when(j >= self.n - 1)
            def _():
                for phase in range(3):
                    self.wait_sends(phase, j, True)

            @pl.when(j >= self.n - self.SLOTS)
            def _():
                for phase in (1, 2):
                    self.wait_sends(phase, j, False)


class Reduces:
    PERIOD = ND + 1 + 2 * NJ + 8
    START = {"down": 8, "gate": ND + 1 + 3}
    LAGS = {"down": (0, 3, 5, 8, 10, 12, 14, 17, 18), "gate": (0, 2, 3, 7, 8, 10, 12, 14, 16)}

    def __init__(self, units):
        self.units = units

    def after(self):
        return max(self.at(units[0], -1) + 2 * units[0].n - 2 for units in self.units) + 1 - self.PERIOD

    def at(self, unit, k):
        return self.START[unit.kind] + self.LAGS[unit.kind][k]

    def tick(self, step, i):
        for odd in BOTH:

            @pl.when(i & 1 == odd)
            def _():
                for k in reversed(range(Reduce.EVENTS)):
                    for units in self.units:
                        at = self.at(units[0], k)
                        if at % 2 == odd:
                            self.event(units, k, step, i - at)

    def event(self, units, k, step, q):
        early = q < 0
        q = jnp.where(early, q + self.PERIOD, q)
        step = jnp.where(early, step - 1, step)

        @pl.when((q >= 0) & (q < 2 * units[0].n) & (step >= 0) & (step < L))
        def _():
            for unit in units:
                unit.unit(step, q >> 1)
                unit.events()[k]()

    def drain(self):
        for units in self.units:
            for unit in units:
                unit.drain()


def scale_of(wide):
    return lax.rsqrt(jnp.mean(wide * wide, -1, keepdims=True) + 1e-6)


def save_normed(h, rows, a, at, dst, sems, i):
    wide = h.astype(F32)
    tile = (wide * scale_of(wide)).astype(BF)
    a[rows, :] = tile
    slot = mod(i, 2)
    copy = local(at.at[slot], dst.at[:, rows], sems.at[slot])

    @pl.when(i >= 2)
    def _():
        copy.wait()

    at[slot] = tile.T
    copy.start()


def wait_normed(at, dst, sems):
    for slot in BOTH:
        local(at.at[slot], dst.at[:, piece(slot, MXU)], sems.at[slot]).wait()


TILE = 4 * MXU


def forward(first, along_z, gathers, fulls, ps, qs, ats, acts, hs, xb, a, at, wb, pq, actt, act, dn, sx, sa, sw, so, sd):
    def weights(l, j):
        return [local(fulls[m].at[l, :, piece(j, CH)], wb.at[mod(j, 2), m], sw.at[mod(j, 2), m]) for m in BOTH]

    def outs(l, s):
        slot = mod(s, 2)
        rows, cols = piece(slot, TILE), piece(div(s, 2), CH)
        pairs = [(pq.at[slot, 0], ps.at[l, rows, cols]), (pq.at[slot, 1], qs.at[l, rows, cols]), (actt.at[slot], acts.at[l, cols, rows])]
        return [local(src, dst, so.at[slot, i]) for i, (src, dst) in enumerate(pairs)]

    keep = local(xb, hs.at[0], sx.at[0])
    down = local(fulls[2].at[0], dn, sd.at[0])
    along_z.start()
    along_z.finish(0)
    first.wait()
    keep.start()

    @pl.loop(0, gathers.AHEAD)
    def _(t):
        gathers.tick(t)
        for part in range(1, len(AlongZ.PARTS) - 1):

            @pl.when(t == 2 * AlongZ.PARTS[part] - 1)
            def _():
                along_z.finish(part)

        @pl.when(t < T // MXU)
        def _():
            rows = piece(t, MXU)
            save_normed(xb[rows, :], rows, a, at, ats.at[0], sa, t)

    wait_normed(at, ats.at[0], sa)

    for copy in weights(0, 0):
        copy.start()

    @pl.loop(0, L)
    def _(l):
        @pl.loop(0, 2 * NJ)
        def _(s):
            j, i = div(s, 2), mod(s, 2)
            slot = mod(j, 2)

            @pl.when(i == 0)
            def _():
                for copy in weights(l, j):
                    copy.wait()

            gathers.tick(gathers.AHEAD + l * (2 * NJ + gathers.DEEP) + s)

            @pl.when(i == 1)
            def _():
                @pl.when(j < NJ - 1)
                def _():
                    for copy in weights(l, j + 1):
                        copy.start()

                @pl.when((j == NJ - 1) & (l == 0))
                def _():
                    down.start()
                    for copy in weights(1, 0):
                        copy.start()

            @pl.when(s >= 2)
            def _():
                for copy in outs(l, s - 2):
                    copy.wait()

            for n in range(TILE // MXU):
                rows = piece(i * (TILE // MXU) + n, MXU)
                part = pl.ds(n * MXU, MXU)
                for half in BOTH:
                    cols = pl.ds(half * MXU, MXU)
                    gate, up = (dot(a[rows, :], wb[slot, m, :, cols]) for m in BOTH)
                    h = 0.5 * gate
                    t = jnp.tanh(h)
                    e = 1.0 + t
                    silu = h * e
                    pq[i, 0, part, cols] = silu
                    pq[i, 1, part, cols] = (0.5 * up) * (e * (1.0 + h * (1.0 - t)))
                    tile = (silu * up).astype(BF)
                    act[rows, aligned(j * CH + half * MXU, MXU)] = tile
                    actt[i, cols, part] = tile.T
            for copy in outs(l, s):
                copy.start()

        for s in (2 * NJ - 2, 2 * NJ - 1):
            for copy in outs(l, s):
                copy.wait()

        @pl.when(l == 0)
        def _():
            keep.wait()
            down.wait()

            @pl.loop(0, T // CH)
            def _(i):
                gathers.tick(gathers.AHEAD + 2 * NJ + i)
                rows = piece(i, CH)
                y = dot(act[rows, :], dn[...]).astype(BF)
                xb[rows, :] = (xb[rows, :].astype(F32) + y.astype(F32)).astype(BF)
                for n in BOTH:
                    sub = piece(2 * i + n, MXU)
                    save_normed(xb[sub, :], sub, a, at, ats.at[1], sa, 2 * i + n)

            wait_normed(at, ats.at[1], sa)
            local(xb, hs.at[1], sx.at[0]).start()

    local(xb, hs.at[1], sx.at[0]).wait()


def by_down(l, tick, first, acts, td, dh, av, st, sl, so):
    parts = 3

    def load(part):
        rows = piece(part, FF // parts)
        return local(acts.at[l, rows, :], av.at[rows, :], sl.at[part])

    for part in range(parts):
        load(part).start()

    def out(i):
        return local(st.at[mod(i, 2)], td.at[l, :, piece(i, MXU)], so.at[mod(i, 2)])

    @pl.loop(0, ND + 1)
    def _(n):
        i = n - 1

        @pl.when(i >= 2)
        def _():
            out(i - 2).wait()

        tick(n)

        @pl.when(i == 0)
        def _():
            first()

            @pl.loop(0, parts)
            def _(part):
                load(part).wait()
                rows = piece(part, FF // parts)
                st[0, rows, :] = dot(av[rows, :], dh[:, :MXU]).astype(BF)

        @pl.when(i > 0)
        def _():
            st[mod(i, 2)] = dot(av[...], dh[:, piece(i, MXU)]).astype(BF)

        @pl.when(i >= 0)
        def _():
            out(i).start()

    for i in (ND - 2, ND - 1):
        out(i).wait()


def by_gate_and_up(l, tick, ahead, wdf, ps, qs, ats, dgs, terms, dh, atv, wdb, pq, dgu, stw, sl, sw, sp, sd, so):
    tiles = T // TILE

    def weights(j):
        return local(wdf.at[l, piece(j, CH), :], wdb.at[mod(j, 2)], sw.at[mod(j, 2)])

    def factors(j, i):
        rows, cols = piece(i, TILE), piece(j, CH)
        return [local(src.at[l, rows, cols], pq.at[m, rows], sp.at[i, m]) for m, src in enumerate((qs, ps))]

    def load_factors(j):
        for i in range(tiles):
            for copy in factors(j, i):
                copy.start()

    def hidden(j):
        return [local(dgu.at[m], dgs[m].at[:, piece(j, CH)], sd.at[m]) for m in BOTH]

    def out(j):
        return [local(stw.at[m], terms[m].at[l, :, piece(j, CH)], so.at[m]) for m in BOTH]

    load = local(ats.at[l], atv, sl)
    weights(0).start()
    load_factors(0)
    load.start()

    def to_hidden(j):
        weights(j).wait()

        @pl.when(j < NJ - 1)
        def _():
            weights(j + 1).start()

        @pl.when(j > 0)
        def _():
            for copy in hidden(j - 1):
                copy.wait()

        @pl.loop(0, tiles)
        def _(i):
            for copy in factors(j, i):
                copy.wait()

            for n in range(TILE // MXU):
                rows = piece(i * (TILE // MXU) + n, MXU)
                for half in BOTH:
                    cols = pl.ds(half * MXU, MXU)
                    by_act = dot(dh[rows, :], wdb[mod(j, 2), cols, :], NT).astype(BF).astype(F32)
                    for m in BOTH:
                        dgu[m, rows, cols] = (by_act * pq[m, rows, cols]).astype(BF)

        for copy in hidden(j):
            copy.start()

    def to_weights(j):
        @pl.when(j == 0)
        def _():
            load.wait()

        @pl.when(j < NJ - 1)
        def _():
            load_factors(j + 1)

        @pl.when(j == NJ - 1)
        def _():
            ahead.start()

        for m in BOTH:
            stw[m] = dot(atv[...], dgu[m]).astype(BF)
        for copy in out(j):
            copy.start()

    @pl.loop(0, 2 * NJ)
    def _(h):
        j, late = div(h, 2), mod(h, 2)

        @pl.when((late == 1) & (j > 0))
        def _():
            for copy in out(j - 1):
                copy.wait()

        tick(ND + 1 + h)
        pl.when(late == 0)(lambda: to_hidden(j))
        pl.when(late == 1)(lambda: to_weights(j))

    for copy in hidden(NJ - 1) + out(NJ - 1):
        copy.wait()


def by_input(l, tick, ahead, full, dgs, hs, dh, first, second, gt, ht, sw, sg, sh):
    after = local(full.at[l], second, sw)
    tiles = T // MXU

    def rows_of(i):
        rows, slot = piece(i, MXU), mod(i, 2)
        return [local(dgs[m].at[rows, :], gt.at[slot, m], sg.at[slot, m]) for m in BOTH] + [local(hs.at[l, rows, :], ht.at[slot], sh.at[slot])]

    for copy in rows_of(0) + [after]:
        copy.start()

    @pl.loop(0, tiles)
    def _(i):
        tick(ND + 1 + 2 * NJ + i)
        for copy in rows_of(i):
            copy.wait()

        @pl.when(i < tiles - 1)
        def _():
            for copy in rows_of(i + 1):
                copy.start()

        @pl.when(i == 0)
        def _():
            ahead.wait()
            after.wait()

        rows, slot = piece(i, MXU), mod(i, 2)
        by_a = [dot(gt[slot, m], w[...], NT).astype(BF).astype(F32) for m, w in enumerate((first, second))]
        total = by_a[0] + by_a[1]
        wide = ht[slot].astype(F32)
        scale = scale_of(wide)
        along = jnp.mean(total * wide, -1, keepdims=True) * (scale * scale * scale)
        by_h = (total * scale - wide * along).astype(BF).astype(F32)
        dh[rows, :] = (dh[rows, :].astype(F32) + by_h).astype(BF)


def kernel(x, dy, wz, wd, dx, og, ou, od, *refs):
    def take(n):
        nonlocal refs
        head, refs = refs[:n], refs[n:]
        return head

    fulls, (ps, qs, ats, acts, hs), dgs, terms = take(3), take(5), take(2), take(3)
    hbm = [take(2) for _ in KINDS]
    zbuf, zcat, zs, zr = take(4)
    sems = take(4)
    far = [take(4) for _ in KINDS]
    rsems = [take(3) for _ in KINDS]
    sx, sa, sw, so, sd, sp, sg = take(7)
    place = Place()
    gathers = Gathers(place, fulls, zcat, wd, *sems)
    dma, vm = pltpu.SemaphoreType.DMA, pltpu.VMEM

    def ahead(xb, a, at, wb, pq, actt, act, dn):
        first = local(x, xb, sx.at[0])
        first.start()
        place.greet([place.to(a, by) for a in "xy" for by in (1, -1)] + [place.to("z", by) for by in range(1, RING)] + [place.partner()])
        along_z = AlongZ(place, wz, zbuf, zcat, zs, zr)
        forward(first, along_z, gathers, fulls, ps, qs, ats, acts, hs, xb, a, at, wb, pq, actt, act, dn, sx, sa, sw, so, sd)
        gathers.drain()

    pl.run_scoped(
        ahead,
        vm((T, D), BF),
        vm((T, D), BF),
        vm((2, D, MXU), BF),
        vm((2, 2, D, CH), BF),
        vm((2, 2, TILE, CH), F32),
        vm((2, CH, TILE), BF),
        vm((T, FF), BF),
        vm((FF, D), BF),
    )

    def back(dh, *near):
        split = [near[i * 10 : i * 10 + 10] for i in range(3)]
        units = [
            Reduce(place, kind, terms[i], (og, ou, od)[i], hbm[i], far[i], split[i], rsems[i]) for i, kind in enumerate(KINDS)
        ]
        reduces = Reduces([units[2:], units[:2]])
        first = local(dy, dh, sx.at[0])
        first.start()

        @pl.loop(0, L)
        def _(step):
            l = L - 1 - step

            def tick(i):
                reduces.tick(step, i)

            pl.run_scoped(
                lambda av, st: by_down(
                    l, tick, lambda: pl.when(step == 0)(first.wait), acts, terms[2], dh, av, st, sp.at[0], so.at[0]
                ),
                vm((FF, T), BF),
                vm((2, FF, MXU), BF),
            )

            def rest(weight):
                ahead = local(fulls[0].at[l], weight, sx.at[0])
                pl.run_scoped(
                    lambda *v: by_gate_and_up(
                        l, tick, ahead, fulls[2], ps, qs, ats, dgs, terms, dh, *v, sd.at[0], sw.at[0], sp, sg.at[0], so.at[0]
                    ),
                    vm((D, T), BF),
                    vm((2, CH, D), BF),
                    vm((2, T, CH), F32),
                    vm((2, T, CH), BF),
                    vm((2, D, CH), BF),
                )
                pl.run_scoped(
                    lambda *v: by_input(l, tick, ahead, fulls[1], dgs, hs, dh, weight, *v, sa.at[0], sg, sd),
                    vm((D, FF), BF),
                    vm((2, 2, MXU, FF), BF),
                    vm((2, MXU, D), BF),
                )

            pl.run_scoped(rest, vm((D, FF), BF))

        end = local(dh, dx, sx.at[0])
        end.start()

        @pl.loop(0, reduces.after())
        def _(i):
            reduces.tick(L, i)

        end.wait()
        reduces.drain()

    pl.run_scoped(back, vm((T, D), BF), *(v for kind in KINDS for v in Reduce.scratch(kind)[2]))


KINDS = ("gate", "up", "down")


def call(x, dy, wz, wd):
    made = [Reduce.scratch(kind) for kind in KINDS]
    vmem, hbm = pl.BlockSpec(memory_space=pltpu.VMEM), pl.BlockSpec(memory_space=pltpu.HBM)
    dma, vm = pltpu.SemaphoreType.DMA, pltpu.VMEM

    def shape(*dims, dtype=BF):
        return jax.ShapeDtypeStruct(dims, dtype)

    work = [shape(L, D, FF), shape(L, D, FF), shape(L, FF, D)]
    work += [shape(L, T, FF, dtype=F32), shape(L, T, FF, dtype=F32), shape(L, D, T), shape(L, FF, T), shape(L, T, D)]
    work += [shape(T, FF), shape(T, FF), shape(L, D, FF), shape(L, D, FF), shape(L, FF, D)]
    work += [s for m in made for s in m[0]]
    outs = [shape(L, ROWS, FF), shape(L, ROWS, FF), shape(L, DROWS, D)]
    return pl.pallas_call(
        kernel,
        out_shape=(shape(T, D), *outs, *work),
        in_specs=[hbm, hbm, vmem, vmem],
        out_specs=(hbm, *(vmem for _ in outs), *(hbm for _ in work)),
        scratch_shapes=[
            vm((RING, UNITS, 2, ROWS, HC), BF),
            vm((UNITS, 2, JOINED, HC), BF),
            dma((len(AlongZ.PARTS) - 1, RING - 1)),
            dma((len(AlongZ.PARTS) - 1, RING - 1)),
            dma((NJ, 2, GatherUp.GROUPS + 1)),
            dma((NJ, 2, GatherUp.GROUPS)),
            dma((L, GatherDown.GROUPS + 1)),
            dma((L, GatherDown.GROUPS)),
            *(s for m in made for s in m[1]),
            *(s for m in made for s in m[3]),
            dma((1,)),
            dma((2,)),
            dma((2, 2)),
            dma((2, 3)),
            dma((2,)),
            dma((2, 3)),
            dma((2, 2)),
        ],
        name="train",
        compiler_params=pltpu.CompilerParams(collective_id=0, has_side_effects=True, vmem_limit_bytes=67_000_000),
    )(x, dy, wz, wd)[:4]


def solution(mesh):
    def step(x, dy, w_gate, w_up, w_down):
        wz = jnp.stack([w_gate, w_up], 1).reshape(L, 2, ROWS, NJ, 2, HC)
        wz = lax.dynamic_index_in_dim(wz, lax.axis_index("rep"), 4, keepdims=False).transpose(0, 3, 1, 2, 4).reshape(UNITS, 2, ROWS, HC)
        by_x, *by_w = call(x[0], dy[0], wz, w_down)
        return (by_x[None], *by_w)

    both, rows = P(("rep", "dp"), None, None), P(None, "dp", None)
    return jax.shard_map(
        step,
        mesh=mesh,
        in_specs=(both, both, rows, rows, rows),
        out_specs=(both, *(P("rep", "dp", None),) * 3),
        check_vma=False,
    )
```

```python
import jax
import jax.numpy as jnp
from jax import lax
from jax.experimental import pallas as pl
from jax.experimental.pallas import tpu as pltpu
from jax.sharding import PartitionSpec as P

MESH = pl.DeviceIdType.MESH
BF = jnp.bfloat16
F32 = jnp.float32
L, D, FF, T = 2, 1280, 3072, 2048
BOTH = range(2)
RING = 4
ROWS = D // 64
JOINED = RING * ROWS
DROWS = FF // 64
CH = 512
HC = CH // 2
NJ = FF // CH
UNITS = L * NJ
MXU = 256
ND = D // MXU
ALL = slice(None)
HALVES = (lambda: ALL, lambda: pl.ds(0, 2), lambda: pl.ds(2, 2))
NN = (((1,), (0,)), ((), ()))
NT = (((1,), (1,)), ((), ()))
LANES = 128


def dot(a, b, dims=NN):
    return lax.dot_general(a, b, dims, preferred_element_type=F32)


def local(src, dst, sem):
    return pltpu.make_async_copy(src, dst, sem)


def remote(src, dst, send, recv, device):
    return pltpu.make_async_remote_copy(src_ref=src, dst_ref=dst, send_sem=send, recv_sem=recv, device_id=device, device_id_type=MESH)


def aligned(start, size):
    return pl.ds(pl.multiple_of(start, LANES), size)


def piece(index, size):
    return aligned(index * size, size)


def mod(a, n):
    return lax.rem(a, n)


def div(a, n):
    return lax.div(a, n)


def side(way):
    return 1 - 2 * way


class Place:
    def __init__(self):
        self.core = lax.axis_index("rep")
        self.dp = lax.axis_index("dp")
        self.other = 1 - self.core
        self.place, self.device = {}, {}
        for stride, axis in ((RING**2, "x"), (RING, "y"), (1, "z")):
            at = mod(div(self.dp, stride), RING)
            for by in range(RING):
                self.place[axis, by] = mod(at + by, RING)
                self.device[axis, by] = (self.core, self.dp + (self.place[axis, by] - at) * stride)

    def to(self, axis, by):
        return self.device[axis, by % RING]

    def index(self, axis, by=0):
        return self.place[axis, by % RING]

    def partner(self):
        return (self.other, self.dp)

    def greet(self, others):
        barrier = pltpu.get_barrier_semaphore()
        for other in others:
            pl.semaphore_signal(barrier, inc=1, device_id=other, device_id_type=MESH)
        pl.semaphore_wait(barrier, len(others))


class Gather:
    def __init__(self, place, full, own, send, recv):
        self.p, self.full, self.own, self.send, self.recv = place, full, own, send, recv

    def ring(self, axis, ref, parts):
        whole, low, high = parts
        right, left = self.p.to(axis, 1), self.p.to(axis, -1)
        return [(lambda: ref(0, whole()), right), (lambda: ref(0, whole()), left), (lambda: ref(-1, low()), right), (lambda: ref(1, high()), left)]

    def hand(self, ref):
        return [(lambda by=by: ref(by), self.p.partner()) for by in (0, -1, 1, 2)]

    def copy(self, k):
        ref, device = self.table()[k][0](), self.table()[k][1]
        group = min(k // 2, self.GROUPS - 1)
        return remote(self.mine() if k < 2 else ref, ref, self.send.at[(*self.slot, group)], self.recv.at[(*self.slot, group)], device)

    def all_of(self, group):
        blocks = RING ** (group // 2) * (1 if group % 2 else 2)
        ref = self.some(RING**self.RINGS if group == self.GROUPS - 1 else blocks)
        return remote(ref, ref, self.send.at[(*self.slot, group)], self.recv.at[(*self.slot, group)], self.p.partner())

    def keep(self):
        return local(self.mine(), self.table()[0][0](), self.send.at[(*self.slot, self.GROUPS)])

    def event(self, k, l, j=0):
        self.unit(l, j)
        ends = 2 * self.RINGS
        starts = [2 * k, 2 * k + 1] if k < ends else []
        hand = {ends - 2: [0], ends - 1: [1, 2], ends: [3]}.get(k, [])
        if k < ends:
            self.free(k)
        if k == ends - 2:
            self.free(ends)
        if k == 0:
            self.keep().start()
        else:
            self.all_of(k - 1).wait_recv()
        if k == 2:
            self.keep().wait()
        for i in starts + [2 * ends + i for i in hand]:
            self.copy(i).start()

    def free(self, group):
        pass

    def drain(self, l, j=0):
        self.unit(l, j)
        for group in range(self.GROUPS):
            self.all_of(group).wait_send()


def first_blocks(count, dims):
    index = []
    for _ in range(dims):
        index.insert(0, ALL if count >= RING else pl.ds(0, count) if count > 1 else 0)
        count = max(count // RING, 1)
    return tuple(index)


class GatherUp(Gather):
    RINGS = 2
    GROUPS = 2 * RINGS + 1

    def __init__(self, which, *rest):
        super().__init__(*rest)
        self.which = which
        self.axes = "yx" if which else "xy"

    def unit(self, l, j):
        self.l, self.j, self.slot = l, j, (j, self.which)
        self.start = j * CH + self.p.core * HC

    def free(self, group):
        @pl.when(self.l > 0)
        def _():
            self.all_of(group).wait_send()

    def mine(self):
        return self.own.at[self.l * NJ + self.j, self.which]

    def cols(self, lo=0, size=HC):
        return aligned(self.start + lo, size)

    def view(self):
        return self.full.reshape(L, RING, RING, JOINED, FF)

    def row(self, b, cols, a):
        return self.view().at[self.l, b, a, :, cols] if self.which else self.view().at[self.l, a, b, :, cols]

    def some(self, count):
        return self.view().at[(self.l, *first_blocks(count, 2), ALL, self.cols())]

    def table(self):
        p = self.p
        a, b = self.axes
        parts = (self.cols, lambda: self.cols(0, LANES), lambda: self.cols(LANES, LANES))
        first = self.ring(a, lambda by, c: self.row(p.index(b), c, p.index(a, by)), parts)
        second = self.ring(b, lambda by, part: self.row(p.index(b, by), self.cols(), part), HALVES)
        return first + second + self.hand(lambda by: self.row(p.index(b, by), self.cols(), ALL))


class GatherDown(Gather):
    RINGS = 3
    GROUPS = 2 * RINGS + 1
    HALF = D // 2
    CUT = 384
    TICKS = ((-1, 1, 4, 8, 10, 17, 20, 21), (17, 19, 21, 23, 25, 32, 36, 37))

    def unit(self, l, _):
        self.l, self.slot = l, (l,)

    def cols(self):
        return aligned(self.p.core * self.HALF, self.HALF)

    def mine(self):
        return self.own.at[self.l, :, self.cols()]

    def view(self):
        return self.full.reshape(L, RING, RING, RING, DROWS, D)

    def some(self, count):
        return self.view().at[(self.l, *first_blocks(count, 3), ALL, self.cols())]

    def table(self):
        p = self.p
        x, y, z = (p.index(a) for a in "xyz")
        start = p.core * self.HALF
        parts = (self.cols, lambda: aligned(start, self.CUT), lambda: aligned(start + self.CUT, self.HALF - self.CUT))
        full, v = self.view(), self.l
        first = self.ring("x", lambda by, c: full.at[v, p.index("x", by), y, z, :, c], parts)
        second = self.ring("y", lambda by, part: full.at[v, part, p.index("y", by), z, :, self.cols()], HALVES)
        third = self.ring("z", lambda by, part: full.at[v, part, :, p.index("z", by), :, self.cols()], HALVES)
        return first + second + third + self.hand(lambda by: full.at[v, :, :, p.index("z", by), :, self.cols()])


class Gathers:
    LAGS = (0, 3, 5, 7, 8, 9)
    AHEAD = LAGS[-1] + 1
    DEEP = T // CH

    def __init__(self, place, fulls, zcat, wd, us, ur, ds, dr):
        self.ups = [GatherUp(m, place, fulls[m], zcat, us, ur) for m in BOTH]
        self.down = GatherDown(place, fulls[2], wd, ds, dr)

    def tick(self, t):
        for odd in BOTH:

            @pl.when(t & 1 == odd)
            def _():
                for k in reversed(range(len(self.LAGS))):
                    if self.LAGS[k] % 2 == odd:
                        self.step(k, t - self.LAGS[k])

        for k, (one, two) in enumerate(zip(*GatherDown.TICKS)):

            @pl.when((t == one) | (t == two))
            def _():
                self.down.event(k, jnp.where(t == two, 1, 0))

    def step(self, k, q):
        late = q >= 2 * NJ + self.DEEP
        q = jnp.where(late, q - self.DEEP, jnp.where(q < 2 * NJ, q, -1))

        @pl.when((q >= 0) & (q < 2 * UNITS))
        def _():
            l = jnp.where(late, 1, 0)
            for up in self.ups:
                up.event(k, l, (q >> 1) - NJ * l)

    def drain(self):
        @pl.loop(0, NJ)
        def _(j):
            for up in self.ups:
                up.drain(L - 1, j)

        @pl.loop(0, L)
        def _(v):
            self.down.drain(v)


class AlongZ:
    def __init__(self, place, wz, zbuf, zcat, send, recv):
        self.p, self.wz, self.zbuf, self.zcat, self.send, self.recv = place, wz, zbuf, zcat, send, recv
        self.z = place.index("z")

    PARTS = (0, 1, 3, NJ, UNITS)

    def copy(self, part, by, receive):
        units = pl.ds(self.PARTS[part], self.PARTS[part + 1] - self.PARTS[part])
        slot = self.p.index("z", -by) if receive else self.z
        sems = (self.send.at[part, by - 1], self.recv.at[part, by - 1])
        return remote(self.wz.at[units], self.zbuf.at[slot, units], *sems, self.p.to("z", by))

    def start(self):
        for part in range(len(self.PARTS) - 1):
            for by in range(1, RING):
                self.copy(part, by, False).start()
        self.zbuf[self.z] = self.wz[...]

    def finish(self, part):
        for receive in (True, False):
            for by in range(1, RING):
                copy = self.copy(part, by, receive)
                copy.wait_recv() if receive else copy.wait_send()

        @pl.loop(self.PARTS[part], self.PARTS[part + 1])
        def _(u):
            for m in BOTH:
                pieces = [self.zbuf[i, u, m].astype(F32) for i in range(RING)]
                self.zcat[u, m] = jnp.concatenate(pieces, axis=0).astype(BF)


class Ring:
    def __init__(self, place, axis, src, opposite, block, send, recv):
        self.p, self.axis, self.src, self.opposite, self.block, self.send, self.recv = place, axis, src, opposite, block, send, recv

    def copy(self, step, part, way, src, dst):
        return remote(src, dst, self.send(step), self.recv(2 * part + way), self.p.to(self.axis, side(way)))

    def first(self):
        p, a = self.p, self.axis
        far = [self.copy(0, 0, w, self.src(p.index(a, 2), w), self.opposite(w)) for w in BOTH]
        near = [self.copy(0, 1, w, self.src(p.index(a, side(w)), 1 - w), self.block(w, 1 - w)) for w in BOTH]
        return far + near

    def second(self, sums):
        return [self.copy(1, 1, w, sums.at[w], self.block(w, w)) for w in BOTH]

    def wait_opposite(self):
        for w in BOTH:
            self.copy(0, 0, w, self.opposite(w), self.opposite(w)).wait_recv()

    def wait_block(self):
        for w in BOTH:
            self.copy(0, 1, w, self.block(w), self.block(w)).wait_recv()

    def wait_sent(self, step, ref):
        self.copy(step, 0, 0, ref, ref).wait_send()


class Spread:
    def __init__(self, place, axis, src, came, send, recv):
        self.p, self.axis, self.src, self.came, self.send, self.recv = place, axis, src, came, send, recv

    def start(self):
        for by in range(1, RING):
            to = self.p.to(self.axis, by)
            remote(self.src.at[self.p.index(self.axis, by)], self.came.at[by - 1], self.send, self.recv, to).start()

    def all(self):
        return remote(self.came, self.came, self.send, self.recv, self.p.to(self.axis, 1))


def every(lead, body):
    if not lead:
        body(())
        return
    count = 1
    for n in lead:
        count *= n

    @pl.loop(0, count)
    def _(i):
        body((div(i, lead[-1]), mod(i, lead[-1])) if len(lead) == 2 else (i,))


class Reduce:
    EVENTS = 7
    SLOTS = 2
    KINDS = {
        "gate": ("xyz", NJ, CH, (RING,), JOINED, ROWS),
        "up": ("yxz", NJ, CH, (RING,), JOINED, ROWS),
        "down": ("zxy", ND, MXU, (RING, RING), DROWS, DROWS),
    }

    def __init__(self, place, kind, term, out, hbm, far, near, sems):
        self.p, self.kind, self.out = place, kind, out
        self.axes, self.n, self.width, self.lead, _, _ = self.KINDS[kind]
        self.down = kind == "down"
        self.term_ref = term.reshape(L, RING, RING, RING, DROWS, D) if self.down else term.reshape(L, RING, RING, JOINED, FF)
        self.half = self.width // 2
        self.count = L * self.n
        self.x1o, self.x1f = hbm
        self.x2, self.x3 = far
        self.vo, self.vw, self.v1, self.vf, self.s, self.sb, self.t, self.tb = near
        self.ls, self.send, self.recv = sems

    def unit(self, step, j):
        self.l, self.j, self.u = L - 1 - step, j, step * self.n + j
        self.slot = self.u & 1

    @classmethod
    def scratch(cls, kind):
        _, n, w, lead, rows, last = cls.KINDS[kind]
        h, count = w // 2, L * n
        block, mid, end = (*lead, rows), (*lead[1:], rows), (last,)
        dma, vm = pltpu.SemaphoreType.DMA, pltpu.VMEM
        hbm = [jax.ShapeDtypeStruct((count, 2, *block, c), BF) for c in (h, w)]
        far = [vm((n, RING - 1, *shape, w), BF) for shape in (mid, end)]
        near = [vm((2, *block, h), BF)] * 2 + [vm((cls.SLOTS, 2, *block, h), BF), vm((3, *block, w), BF)]
        near += [vm((cls.SLOTS, *block, w), dtype) for dtype in (F32, BF)]
        near += [vm((cls.SLOTS, RING, *end, w), dtype) for dtype in (F32, BF)]
        return hbm, far, near, [dma((7,)), dma((n, RING)), dma((n, 2 * RING))]

    def halves(self, half):
        return pl.ds(half * self.half, self.half)

    def cut(self, ref, half):
        return ref.at[(ALL,) * (len(ref.shape) - 1) + (self.halves(half),)]

    def term(self, q, half=None):
        start = self.j * self.width
        cols = aligned(start, self.width) if half is None else aligned(start + half * self.half, self.half)
        if self.down:
            return self.term_ref.at[self.l, :, :, q, :, cols]
        if self.kind == "up":
            return self.term_ref.at[self.l, :, q, :, cols]
        return self.term_ref.at[self.l, q, :, :, cols]

    def ring(self, j=None):
        j = self.j if j is None else j
        opposite, block = self.x1o.at[self.u], self.x1f.at[self.u]
        sems = (lambda k: self.send.at[j, k], lambda k: self.recv.at[j, k])
        return Ring(self.p, self.axes[0], self.term, lambda w: opposite.at[w], lambda w, h=None: block.at[w] if h is None else self.cut(block.at[w], h), *sems)

    def spread(self, phase, j=None):
        j = self.j if j is None else j
        src, came = ((self.sb, self.x2), (self.tb, self.x3))[phase - 1]
        return Spread(self.p, self.axes[phase], src.at[self.slot], came.at[j], self.send.at[j, 1 + phase], self.recv.at[j, RING - 1 + phase])

    def loads(self, blocks):
        a = self.axes[0]
        if blocks:
            pairs = [(self.x1f.at[self.u, w], self.vf.at[w]) for w in BOTH] + [(self.term(self.p.index(a)), self.vf.at[2])]
        else:
            pairs = [(self.x1o.at[self.u, w], self.vo.at[w]) for w in BOTH]
            pairs += [(self.term(self.p.index(a, side(w)), w), self.vw.at[w]) for w in BOTH]
        return [local(s, d, self.ls.at[4 * blocks + i]) for i, (s, d) in enumerate(pairs)]

    def wait_sends(self, phase, j, second):
        if phase:
            self.spread(phase, j).all().wait_send()
        else:
            self.ring(j).wait_sent(int(second), self.v1.at[0] if second else self.x1f.at[0])

    def reuse(self, phase, second=False):
        back = self.SLOTS if second or phase else self.n

        @pl.when(self.u >= back)
        def _():
            j = self.j - back
            self.wait_sends(phase, jnp.where(j < 0, j + self.n, j), second)

    def start(self):
        self.reuse(0)
        for copy in self.ring().first():
            copy.start()

    def load_opposite(self):
        self.ring().wait_opposite()
        for copy in self.loads(False):
            copy.start()

    def add_opposite(self):
        for copy in self.loads(False):
            copy.wait()
        self.reuse(0, True)

        def add(i):
            for w in BOTH:
                self.v1[(self.slot, w, *i)] = (self.vo[(w, *i)].astype(F32) + self.vw[(w, *i)].astype(F32)).astype(BF)

        every(self.lead, add)
        for copy in self.ring().second(self.v1.at[self.slot]):
            copy.start()

    def load_block(self):
        self.ring().wait_block()
        for copy in self.loads(True):
            copy.start()

    def add_block(self):
        for copy in self.loads(True):
            copy.wait()
        self.reuse(1)

        def add(i):
            own, left, right = (self.vf[(w, *i)].astype(F32) for w in (2, 0, 1))
            total = own + left + right
            self.s[(self.slot, *i)] = total
            self.sb[(self.slot, *i)] = total.astype(BF)

        every(self.lead, add)
        self.spread(1).start()

    def total(self, own, came):
        for w in range(RING - 1):
            own = own + came(w).astype(F32)
        return own

    def turn(self):
        self.spread(1).all().wait_recv()
        self.reuse(2)
        q = self.p.index(self.axes[1])

        def total(i):
            return self.total(self.s[(self.slot, q, *i)], lambda w: self.x2[(self.j, w, *i)])

        def put(i, value):
            self.t[self.slot, i] = value
            self.tb[self.slot, i] = value.astype(BF)

        if self.down:
            every(self.lead[1:], lambda i: put(*i, total(i)))
        else:
            whole = total(())
            for i in range(RING):
                put(i, whole[ROWS * i : ROWS * (i + 1)])
        self.spread(2).start()

    def finish(self):
        self.spread(2).all().wait_recv()
        total = self.total(self.t[self.slot, self.p.index(self.axes[2])], lambda w: self.x3[self.j, w])
        self.out[self.l, :, piece(self.j, self.width)] = total.astype(BF)

    def events(self):
        return (self.start, self.load_opposite, self.add_opposite, self.load_block, self.add_block, self.turn, self.finish)

    def drain(self):
        @pl.loop(0, self.n)
        def _(j):
            self.unit(L - 1, j)
            self.wait_sends(0, j, False)

            @pl.when(j >= self.n - self.SLOTS)
            def _():
                for phase in range(3):
                    self.wait_sends(phase, j, True)


class Reduces:
    PERIOD = ND + 1 + 2 * NJ + 8
    START = {"down": 8, "gate": ND + 1 + 3}
    LAGS = {"down": (0, 3, 4, 7, 8, 12, 14), "gate": (0, 2, 3, 6, 7, 11, 13)}

    def __init__(self, units):
        self.units = units

    def after(self):
        return max(self.at(units[0], -1) + 2 * units[0].n - 2 for units in self.units) + 1 - self.PERIOD

    def at(self, unit, k):
        return self.START[unit.kind] + self.LAGS[unit.kind][k]

    def tick(self, step, i):
        for odd in BOTH:

            @pl.when(i & 1 == odd)
            def _():
                for k in reversed(range(Reduce.EVENTS)):
                    for units in self.units:
                        at = self.at(units[0], k)
                        if at % 2 == odd:
                            self.event(units, k, step, i - at)

    def event(self, units, k, step, q):
        early = q < 0
        q = jnp.where(early, q + self.PERIOD, q)
        step = jnp.where(early, step - 1, step)

        @pl.when((q >= 0) & (q < 2 * units[0].n) & (step >= 0) & (step < L))
        def _():
            for unit in units:
                unit.unit(step, q >> 1)
                unit.events()[k]()

    def drain(self):
        for units in self.units:
            for unit in units:
                unit.drain()


def scale_of(wide):
    return lax.rsqrt(jnp.mean(wide * wide, -1, keepdims=True) + 1e-6)


def save_normed(h, rows, a, at, dst, sems, i):
    wide = h.astype(F32)
    tile = (wide * scale_of(wide)).astype(BF)
    a[rows, :] = tile
    slot = mod(i, 2)
    copy = local(at.at[slot], dst.at[:, rows], sems.at[slot])

    @pl.when(i >= 2)
    def _():
        copy.wait()

    at[slot] = tile.T
    copy.start()


def wait_normed(at, dst, sems):
    for slot in BOTH:
        local(at.at[slot], dst.at[:, piece(slot, MXU)], sems.at[slot]).wait()


TILE = 4 * MXU


def forward(first, along_z, gathers, fulls, ps, qs, ats, acts, hs, xb, a, at, wb, pq, actt, act, dn, sx, sa, sw, so, sd):
    def weights(l, j):
        return [local(fulls[m].at[l, :, piece(j, CH)], wb.at[mod(j, 2), m], sw.at[mod(j, 2), m]) for m in BOTH]

    def outs(l, s):
        slot = mod(s, 2)
        rows, cols = piece(slot, TILE), piece(div(s, 2), CH)
        pairs = [(pq.at[slot, 0], ps.at[l, rows, cols]), (pq.at[slot, 1], qs.at[l, rows, cols]), (actt.at[slot], acts.at[l, cols, rows])]
        return [local(src, dst, so.at[slot, i]) for i, (src, dst) in enumerate(pairs)]

    keep = local(xb, hs.at[0], sx.at[0])
    down = local(fulls[2].at[0], dn, sd.at[0])
    along_z.start()
    gathers.down.event(0, 0)
    along_z.finish(0)
    first.wait()
    keep.start()

    @pl.loop(0, gathers.AHEAD)
    def _(t):
        gathers.tick(t)
        for part in range(1, len(AlongZ.PARTS) - 1):

            @pl.when(t == min(2 * AlongZ.PARTS[part], gathers.AHEAD) - 1)
            def _():
                along_z.finish(part)

        @pl.when(t < T // MXU)
        def _():
            rows = piece(t, MXU)
            save_normed(xb[rows, :], rows, a, at, ats.at[0], sa, t)

    wait_normed(at, ats.at[0], sa)

    for copy in weights(0, 0):
        copy.start()

    @pl.loop(0, L)
    def _(l):
        @pl.loop(0, 2 * NJ)
        def _(s):
            j, i = div(s, 2), mod(s, 2)
            slot = mod(j, 2)

            @pl.when(i == 0)
            def _():
                for copy in weights(l, j):
                    copy.wait()

            gathers.tick(gathers.AHEAD + l * (2 * NJ + gathers.DEEP) + s)

            @pl.when(i == 1)
            def _():
                @pl.when(j < NJ - 1)
                def _():
                    for copy in weights(l, j + 1):
                        copy.start()

                @pl.when((j == NJ - 1) & (l == 0))
                def _():
                    down.start()

            @pl.when(s >= 2)
            def _():
                for copy in outs(l, s - 2):
                    copy.wait()

            for n in range(TILE // MXU):
                rows = piece(i * (TILE // MXU) + n, MXU)
                part = pl.ds(n * MXU, MXU)
                for half in BOTH:
                    cols = pl.ds(half * MXU, MXU)
                    gate, up = (dot(a[rows, :], wb[slot, m, :, cols]) for m in BOTH)
                    h = 0.5 * gate
                    t = jnp.tanh(h)
                    e = 1.0 + t
                    silu = h * e
                    pq[i, 0, part, cols] = silu
                    pq[i, 1, part, cols] = (0.5 * up) * (e * (1.0 + h * (1.0 - t)))
                    tile = (silu * up).astype(BF)
                    act[rows, aligned(j * CH + half * MXU, MXU)] = tile
                    actt[i, cols, part] = tile.T
            for copy in outs(l, s):
                copy.start()

        for s in (2 * NJ - 2, 2 * NJ - 1):
            for copy in outs(l, s):
                copy.wait()

        @pl.when(l == 0)
        def _():
            keep.wait()
            down.wait()

            @pl.loop(0, T // CH)
            def _(i):
                gathers.tick(gathers.AHEAD + 2 * NJ + i)

                @pl.when(i == T // CH - 1)
                def _():
                    for copy in weights(1, 0):
                        copy.start()

                rows = piece(i, CH)
                y = dot(act[rows, :], dn[...]).astype(BF)
                xb[rows, :] = (xb[rows, :].astype(F32) + y.astype(F32)).astype(BF)
                for n in BOTH:
                    sub = piece(2 * i + n, MXU)
                    save_normed(xb[sub, :], sub, a, at, ats.at[1], sa, 2 * i + n)

            wait_normed(at, ats.at[1], sa)
            local(xb, hs.at[1], sx.at[0]).start()

    local(xb, hs.at[1], sx.at[0]).wait()


def by_down(l, tick, first, acts, td, dh, av, st, sl, so):
    parts = 3

    def load(part):
        rows = piece(part, FF // parts)
        return local(acts.at[l, rows, :], av.at[rows, :], sl.at[part])

    for part in range(parts):
        load(part).start()

    def out(i):
        return local(st.at[mod(i, 2)], td.at[l, :, piece(i, MXU)], so.at[mod(i, 2)])

    @pl.loop(0, ND + 1)
    def _(n):
        i = n - 1

        @pl.when(i >= 2)
        def _():
            out(i - 2).wait()

        tick(n)

        @pl.when(i == 0)
        def _():
            first()

            @pl.loop(0, parts)
            def _(part):
                load(part).wait()
                rows = piece(part, FF // parts)
                st[0, rows, :] = dot(av[rows, :], dh[:, :MXU]).astype(BF)

        @pl.when(i > 0)
        def _():
            st[mod(i, 2)] = dot(av[...], dh[:, piece(i, MXU)]).astype(BF)

        @pl.when(i >= 0)
        def _():
            out(i).start()

    for i in (ND - 2, ND - 1):
        out(i).wait()


def by_gate_and_up(l, tick, ahead, wdf, ps, qs, ats, dgs, terms, dh, atv, wdb, pq, dgu, stw, sl, sw, sp, sd, so):
    tiles = T // TILE

    def weights(j):
        return local(wdf.at[l, piece(j, CH), :], wdb.at[mod(j, 2)], sw.at[mod(j, 2)])

    def factors(j, i):
        rows, cols = piece(i, TILE), piece(j, CH)
        return [local(src.at[l, rows, cols], pq.at[m, rows], sp.at[i, m]) for m, src in enumerate((qs, ps))]

    def load_factors(j):
        for i in range(tiles):
            for copy in factors(j, i):
                copy.start()

    def hidden(j):
        return [local(dgu.at[m], dgs[m].at[:, piece(j, CH)], sd.at[m]) for m in BOTH]

    def out(j):
        return [local(stw.at[m], terms[m].at[l, :, piece(j, CH)], so.at[m]) for m in BOTH]

    load = local(ats.at[l], atv, sl)
    weights(0).start()
    load_factors(0)
    load.start()

    def to_hidden(j):
        weights(j).wait()

        @pl.when(j < NJ - 1)
        def _():
            weights(j + 1).start()

        @pl.when(j > 0)
        def _():
            for copy in hidden(j - 1):
                copy.wait()

        @pl.loop(0, tiles)
        def _(i):
            for copy in factors(j, i):
                copy.wait()

            for n in range(TILE // MXU):
                rows = piece(i * (TILE // MXU) + n, MXU)
                for half in BOTH:
                    cols = pl.ds(half * MXU, MXU)
                    by_act = dot(dh[rows, :], wdb[mod(j, 2), cols, :], NT).astype(BF).astype(F32)
                    for m in BOTH:
                        dgu[m, rows, cols] = (by_act * pq[m, rows, cols]).astype(BF)

        for copy in hidden(j):
            copy.start()

    def to_weights(j):
        @pl.when(j == 0)
        def _():
            load.wait()

        @pl.when(j < NJ - 1)
        def _():
            load_factors(j + 1)

        @pl.when(j == NJ - 1)
        def _():
            ahead.start()

        for m in BOTH:
            stw[m] = dot(atv[...], dgu[m]).astype(BF)
        for copy in out(j):
            copy.start()

    @pl.loop(0, 2 * NJ)
    def _(h):
        j, late = div(h, 2), mod(h, 2)

        @pl.when((late == 1) & (j > 0))
        def _():
            for copy in out(j - 1):
                copy.wait()

        tick(ND + 1 + h)
        pl.when(late == 0)(lambda: to_hidden(j))
        pl.when(late == 1)(lambda: to_weights(j))

    for copy in hidden(NJ - 1) + out(NJ - 1):
        copy.wait()


def by_input(l, tick, ahead, full, dgs, hs, dh, first, second, gt, ht, sw, sg, sh):
    after = local(full.at[l], second, sw)
    tiles = T // MXU

    def rows_of(i):
        rows, slot = piece(i, MXU), mod(i, 2)
        return [local(dgs[m].at[rows, :], gt.at[slot, m], sg.at[slot, m]) for m in BOTH] + [local(hs.at[l, rows, :], ht.at[slot], sh.at[slot])]

    for copy in rows_of(0) + [after]:
        copy.start()

    @pl.loop(0, tiles)
    def _(i):
        tick(ND + 1 + 2 * NJ + i)
        for copy in rows_of(i):
            copy.wait()

        @pl.when(i < tiles - 1)
        def _():
            for copy in rows_of(i + 1):
                copy.start()

        @pl.when(i == 0)
        def _():
            ahead.wait()
            after.wait()

        rows, slot = piece(i, MXU), mod(i, 2)
        by_a = [dot(gt[slot, m], w[...], NT).astype(BF).astype(F32) for m, w in enumerate((first, second))]
        total = by_a[0] + by_a[1]
        wide = ht[slot].astype(F32)
        scale = scale_of(wide)
        along = jnp.mean(total * wide, -1, keepdims=True) * (scale * scale * scale)
        by_h = (total * scale - wide * along).astype(BF).astype(F32)
        dh[rows, :] = (dh[rows, :].astype(F32) + by_h).astype(BF)


def kernel(x, dy, wz, wd, dx, og, ou, od, *refs):
    def take(n):
        nonlocal refs
        head, refs = refs[:n], refs[n:]
        return head

    fulls, (ps, qs, ats, acts, hs), dgs, terms = take(3), take(5), take(2), take(3)
    hbm = [take(2) for _ in KINDS]
    zbuf, zcat, zs, zr = take(4)
    sems = take(4)
    far = [take(2) for _ in KINDS]
    rsems = [take(3) for _ in KINDS]
    sx, sa, sw, so, sd, sp, sg = take(7)
    place = Place()
    gathers = Gathers(place, fulls, zcat, wd, *sems)
    dma, vm = pltpu.SemaphoreType.DMA, pltpu.VMEM

    def ahead(xb, a, at, wb, pq, actt, act, dn):
        first = local(x, xb, sx.at[0])
        first.start()
        place.greet([place.to(a, by) for a in "xyz" for by in range(1, RING)] + [place.partner()])
        along_z = AlongZ(place, wz, zbuf, zcat, zs, zr)
        forward(first, along_z, gathers, fulls, ps, qs, ats, acts, hs, xb, a, at, wb, pq, actt, act, dn, sx, sa, sw, so, sd)
        gathers.drain()

    pl.run_scoped(
        ahead,
        vm((T, D), BF),
        vm((T, D), BF),
        vm((2, D, MXU), BF),
        vm((2, 2, D, CH), BF),
        vm((2, 2, TILE, CH), F32),
        vm((2, CH, TILE), BF),
        vm((T, FF), BF),
        vm((FF, D), BF),
    )

    def back(dh, *near):
        split = [near[i * 8 : i * 8 + 8] for i in range(3)]
        units = [
            Reduce(place, kind, terms[i], (og, ou, od)[i], hbm[i], far[i], split[i], rsems[i]) for i, kind in enumerate(KINDS)
        ]
        reduces = Reduces([units[2:], units[:2]])
        first = local(dy, dh, sx.at[0])
        first.start()

        @pl.loop(0, L)
        def _(step):
            l = L - 1 - step

            def tick(i):
                reduces.tick(step, i)

            pl.run_scoped(
                lambda av, st: by_down(
                    l, tick, lambda: pl.when(step == 0)(first.wait), acts, terms[2], dh, av, st, sp.at[0], so.at[0]
                ),
                vm((FF, T), BF),
                vm((2, FF, MXU), BF),
            )

            def rest(weight):
                ahead = local(fulls[0].at[l], weight, sx.at[0])
                pl.run_scoped(
                    lambda *v: by_gate_and_up(
                        l, tick, ahead, fulls[2], ps, qs, ats, dgs, terms, dh, *v, sd.at[0], sw.at[0], sp, sg.at[0], so.at[0]
                    ),
                    vm((D, T), BF),
                    vm((2, CH, D), BF),
                    vm((2, T, CH), F32),
                    vm((2, T, CH), BF),
                    vm((2, D, CH), BF),
                )
                pl.run_scoped(
                    lambda *v: by_input(l, tick, ahead, fulls[1], dgs, hs, dh, weight, *v, sa.at[0], sg, sd),
                    vm((D, FF), BF),
                    vm((2, 2, MXU, FF), BF),
                    vm((2, MXU, D), BF),
                )

            pl.run_scoped(rest, vm((D, FF), BF))

        end = local(dh, dx, sx.at[0])
        end.start()

        @pl.loop(0, reduces.after())
        def _(i):
            reduces.tick(L, i)

        end.wait()
        reduces.drain()

    pl.run_scoped(back, vm((T, D), BF), *(v for kind in KINDS for v in Reduce.scratch(kind)[2]))


KINDS = ("gate", "up", "down")


def call(x, dy, wz, wd):
    made = [Reduce.scratch(kind) for kind in KINDS]
    vmem, hbm = pl.BlockSpec(memory_space=pltpu.VMEM), pl.BlockSpec(memory_space=pltpu.HBM)
    dma, vm = pltpu.SemaphoreType.DMA, pltpu.VMEM

    def shape(*dims, dtype=BF):
        return jax.ShapeDtypeStruct(dims, dtype)

    work = [shape(L, D, FF), shape(L, D, FF), shape(L, FF, D)]
    work += [shape(L, T, FF, dtype=F32), shape(L, T, FF, dtype=F32), shape(L, D, T), shape(L, FF, T), shape(L, T, D)]
    work += [shape(T, FF), shape(T, FF), shape(L, D, FF), shape(L, D, FF), shape(L, FF, D)]
    work += [s for m in made for s in m[0]]
    outs = [shape(L, ROWS, FF), shape(L, ROWS, FF), shape(L, DROWS, D)]
    return pl.pallas_call(
        kernel,
        out_shape=(shape(T, D), *outs, *work),
        in_specs=[hbm, hbm, vmem, vmem],
        out_specs=(hbm, *(vmem for _ in outs), *(hbm for _ in work)),
        scratch_shapes=[
            vm((RING, UNITS, 2, ROWS, HC), BF),
            vm((UNITS, 2, JOINED, HC), BF),
            dma((len(AlongZ.PARTS) - 1, RING - 1)),
            dma((len(AlongZ.PARTS) - 1, RING - 1)),
            dma((NJ, 2, GatherUp.GROUPS + 1)),
            dma((NJ, 2, GatherUp.GROUPS)),
            dma((L, GatherDown.GROUPS + 1)),
            dma((L, GatherDown.GROUPS)),
            *(s for m in made for s in m[1]),
            *(s for m in made for s in m[3]),
            dma((1,)),
            dma((2,)),
            dma((2, 2)),
            dma((2, 3)),
            dma((2,)),
            dma((2, 3)),
            dma((2, 2)),
        ],
        name="train",
        compiler_params=pltpu.CompilerParams(collective_id=0, has_side_effects=True, vmem_limit_bytes=67_000_000),
    )(x, dy, wz, wd)[:4]


def solution(mesh):
    def step(x, dy, w_gate, w_up, w_down):
        wz = jnp.stack([w_gate, w_up], 1).reshape(L, 2, ROWS, NJ, 2, HC)
        wz = lax.dynamic_index_in_dim(wz, lax.axis_index("rep"), 4, keepdims=False).transpose(0, 3, 1, 2, 4).reshape(UNITS, 2, ROWS, HC)
        by_x, *by_w = call(x[0], dy[0], wz, w_down)
        return (by_x[None], *by_w)

    both, rows = P(("rep", "dp"), None, None), P(None, "dp", None)
    return jax.shard_map(
        step,
        mesh=mesh,
        in_specs=(both, both, rows, rows, rows),
        out_specs=(both, *(P("rep", "dp", None),) * 3),
        check_vma=False,
    )
```

```python
import jax
import jax.numpy as jnp
from jax import lax
from jax.experimental import pallas as pl
from jax.experimental.pallas import tpu as pltpu
from jax.sharding import PartitionSpec as P

MESH = pl.DeviceIdType.MESH
BF = jnp.bfloat16
F32 = jnp.float32
L, D, FF, T = 2, 1280, 3072, 2048
BOTH = range(2)
RING = 4
ROWS = D // 64
JOINED = RING * ROWS
DROWS = FF // 64
CH = 512
HC = CH // 2
NJ = FF // CH
UNITS = L * NJ
MXU = 256
ND = D // MXU
ALL = slice(None)
HALVES = (lambda: ALL, lambda: pl.ds(0, 2), lambda: pl.ds(2, 2))
NN = (((1,), (0,)), ((), ()))
NT = (((1,), (1,)), ((), ()))
LANES = 128


def dot(a, b, dims=NN):
    return lax.dot_general(a, b, dims, preferred_element_type=F32)


def local(src, dst, sem):
    return pltpu.make_async_copy(src, dst, sem)


def remote(src, dst, send, recv, device):
    return pltpu.make_async_remote_copy(src_ref=src, dst_ref=dst, send_sem=send, recv_sem=recv, device_id=device, device_id_type=MESH)


def aligned(start, size):
    return pl.ds(pl.multiple_of(start, LANES), size)


def piece(index, size):
    return aligned(index * size, size)


def mod(a, n):
    return lax.rem(a, n)


def div(a, n):
    return lax.div(a, n)


def side(way):
    return 1 - 2 * way


class Place:
    def __init__(self):
        self.core = lax.axis_index("rep")
        self.dp = lax.axis_index("dp")
        self.other = 1 - self.core
        self.place, self.device = {}, {}
        for stride, axis in ((RING**2, "x"), (RING, "y"), (1, "z")):
            at = mod(div(self.dp, stride), RING)
            for by in range(RING):
                self.place[axis, by] = mod(at + by, RING)
                self.device[axis, by] = (self.core, self.dp + (self.place[axis, by] - at) * stride)

    def to(self, axis, by):
        return self.device[axis, by % RING]

    def index(self, axis, by=0):
        return self.place[axis, by % RING]

    def partner(self):
        return (self.other, self.dp)

    def greet(self, others):
        barrier = pltpu.get_barrier_semaphore()
        for other in others:
            pl.semaphore_signal(barrier, inc=1, device_id=other, device_id_type=MESH)
        pl.semaphore_wait(barrier, len(others))


class Gather:
    def __init__(self, place, full, own, send, recv):
        self.p, self.full, self.own, self.send, self.recv = place, full, own, send, recv

    def ring(self, axis, ref, parts):
        whole, low, high = parts
        right, left = self.p.to(axis, 1), self.p.to(axis, -1)
        return [(lambda: ref(0, whole()), right), (lambda: ref(0, whole()), left), (lambda: ref(-1, low()), right), (lambda: ref(1, high()), left)]

    def hand(self, ref):
        return [(lambda by=by: ref(by), self.p.partner()) for by in (0, -1, 1, 2)]

    def copy(self, k):
        ref, device = self.table()[k][0](), self.table()[k][1]
        group = min(k // 2, self.GROUPS - 1)
        return remote(self.mine() if k < 2 else ref, ref, self.send.at[(*self.slot, group)], self.recv.at[(*self.slot, group)], device)

    def all_of(self, group):
        blocks = RING ** (group // 2) * (1 if group % 2 else 2)
        ref = self.some(RING**self.RINGS if group == self.GROUPS - 1 else blocks)
        return remote(ref, ref, self.send.at[(*self.slot, group)], self.recv.at[(*self.slot, group)], self.p.partner())

    def keep(self):
        return local(self.mine(), self.table()[0][0](), self.send.at[(*self.slot, self.GROUPS)])

    def event(self, k, l, j=0):
        self.unit(l, j)
        ends = 2 * self.RINGS
        starts = [2 * k, 2 * k + 1] if k < ends else []
        hand = {ends - 2: [0], ends - 1: [1, 2], ends: [3]}.get(k, [])
        if k < ends:
            self.free(k)
        if k == ends - 2:
            self.free(ends)
        if k == 0:
            self.keep().start()
        else:
            self.all_of(k - 1).wait_recv()
        if k == 2:
            self.keep().wait()
        for i in starts + [2 * ends + i for i in hand]:
            self.copy(i).start()

    def free(self, group):
        pass

    def drain(self, l, j=0):
        self.unit(l, j)
        for group in range(self.GROUPS):
            self.all_of(group).wait_send()


def first_blocks(count, dims):
    index = []
    for _ in range(dims):
        index.insert(0, ALL if count >= RING else pl.ds(0, count) if count > 1 else 0)
        count = max(count // RING, 1)
    return tuple(index)


class GatherUp(Gather):
    RINGS = 2
    GROUPS = 2 * RINGS + 1

    def __init__(self, which, *rest):
        super().__init__(*rest)
        self.which = which
        self.axes = "yx" if which else "xy"

    def unit(self, l, j):
        self.l, self.j, self.slot = l, j, (j, self.which)
        self.start = j * CH + self.p.core * HC

    def free(self, group):
        @pl.when(self.l > 0)
        def _():
            self.all_of(group).wait_send()

    def mine(self):
        return self.own.at[self.l * NJ + self.j, self.which]

    def cols(self, lo=0, size=HC):
        return aligned(self.start + lo, size)

    def view(self):
        return self.full.reshape(L, RING, RING, JOINED, FF)

    def row(self, b, cols, a):
        return self.view().at[self.l, b, a, :, cols] if self.which else self.view().at[self.l, a, b, :, cols]

    def some(self, count):
        return self.view().at[(self.l, *first_blocks(count, 2), ALL, self.cols())]

    def table(self):
        p = self.p
        a, b = self.axes
        parts = (self.cols, lambda: self.cols(0, LANES), lambda: self.cols(LANES, LANES))
        first = self.ring(a, lambda by, c: self.row(p.index(b), c, p.index(a, by)), parts)
        second = self.ring(b, lambda by, part: self.row(p.index(b, by), self.cols(), part), HALVES)
        return first + second + self.hand(lambda by: self.row(p.index(b, by), self.cols(), ALL))


class GatherDown(Gather):
    RINGS = 3
    GROUPS = 2 * RINGS + 1
    HALF = D // 2
    CUT = 384
    TICKS = ((-1, 1, 4, 8, 10, 17, 20, 21), (17, 19, 21, 23, 25, 32, 36, 37))

    def unit(self, l, _):
        self.l, self.slot = l, (l,)

    def cols(self):
        return aligned(self.p.core * self.HALF, self.HALF)

    def mine(self):
        return self.own.at[self.l, :, self.cols()]

    def view(self):
        return self.full.reshape(L, RING, RING, RING, DROWS, D)

    def some(self, count):
        return self.view().at[(self.l, *first_blocks(count, 3), ALL, self.cols())]

    def table(self):
        p = self.p
        x, y, z = (p.index(a) for a in "xyz")
        start = p.core * self.HALF
        parts = (self.cols, lambda: aligned(start, self.CUT), lambda: aligned(start + self.CUT, self.HALF - self.CUT))
        full, v = self.view(), self.l
        first = self.ring("x", lambda by, c: full.at[v, p.index("x", by), y, z, :, c], parts)
        second = self.ring("y", lambda by, part: full.at[v, part, p.index("y", by), z, :, self.cols()], HALVES)
        third = self.ring("z", lambda by, part: full.at[v, part, :, p.index("z", by), :, self.cols()], HALVES)
        return first + second + third + self.hand(lambda by: full.at[v, :, :, p.index("z", by), :, self.cols()])


class Gathers:
    LAGS = (0, 3, 5, 7, 8, 9)
    AHEAD = LAGS[-1] + 1
    DEEP = T // CH

    def __init__(self, place, fulls, zcat, wd, us, ur, ds, dr):
        self.ups = [GatherUp(m, place, fulls[m], zcat, us, ur) for m in BOTH]
        self.down = GatherDown(place, fulls[2], wd, ds, dr)

    def tick(self, t):
        for odd in BOTH:

            @pl.when(t & 1 == odd)
            def _():
                for k in reversed(range(len(self.LAGS))):
                    if self.LAGS[k] % 2 == odd:
                        self.step(k, t - self.LAGS[k])

        for k, (one, two) in enumerate(zip(*GatherDown.TICKS)):

            @pl.when((t == one) | (t == two))
            def _():
                self.down.event(k, jnp.where(t == two, 1, 0))

    def step(self, k, q):
        late = q >= 2 * NJ + self.DEEP
        q = jnp.where(late, q - self.DEEP, jnp.where(q < 2 * NJ, q, -1))

        @pl.when((q >= 0) & (q < 2 * UNITS))
        def _():
            l = jnp.where(late, 1, 0)
            for up in self.ups:
                up.event(k, l, (q >> 1) - NJ * l)

    def drain(self):
        @pl.loop(0, NJ)
        def _(j):
            for up in self.ups:
                up.drain(L - 1, j)

        @pl.loop(0, L)
        def _(v):
            self.down.drain(v)


class AlongZ:
    def __init__(self, place, wz, zbuf, zcat, send, recv):
        self.p, self.wz, self.zbuf, self.zcat, self.send, self.recv = place, wz, zbuf, zcat, send, recv
        self.z = place.index("z")

    PARTS = (0, 1, 3, NJ, UNITS)

    def copy(self, part, by, receive):
        units = pl.ds(self.PARTS[part], self.PARTS[part + 1] - self.PARTS[part])
        slot = self.p.index("z", -by) if receive else self.z
        sems = (self.send.at[part, by - 1], self.recv.at[part, by - 1])
        return remote(self.wz.at[units], self.zbuf.at[slot, units], *sems, self.p.to("z", by))

    def start(self):
        for part in range(len(self.PARTS) - 1):
            for by in range(1, RING):
                self.copy(part, by, False).start()
        self.zbuf[self.z] = self.wz[...]

    def finish(self, part):
        for receive in (True, False):
            for by in range(1, RING):
                copy = self.copy(part, by, receive)
                copy.wait_recv() if receive else copy.wait_send()

        @pl.loop(self.PARTS[part], self.PARTS[part + 1])
        def _(u):
            for m in BOTH:
                pieces = [self.zbuf[i, u, m].astype(F32) for i in range(RING)]
                self.zcat[u, m] = jnp.concatenate(pieces, axis=0).astype(BF)


class Ring:
    def __init__(self, place, axis, src, opposite, block, send, recv):
        self.p, self.axis, self.src, self.opposite, self.block, self.send, self.recv = place, axis, src, opposite, block, send, recv

    def copy(self, step, part, way, src, dst):
        return remote(src, dst, self.send(step), self.recv(2 * part + way), self.p.to(self.axis, side(way)))

    def first(self):
        p, a = self.p, self.axis
        far = [self.copy(0, 0, w, self.src(p.index(a, 2), w), self.opposite(w)) for w in BOTH]
        near = [self.copy(0, 1, w, self.src(p.index(a, side(w)), 1 - w), self.block(w, 1 - w)) for w in BOTH]
        return far + near

    def second(self, sums):
        return [self.copy(1, 1, w, sums.at[w], self.block(w, w)) for w in BOTH]

    def wait_opposite(self):
        for w in BOTH:
            self.copy(0, 0, w, self.opposite(w), self.opposite(w)).wait_recv()

    def wait_block(self):
        for w in BOTH:
            self.copy(0, 1, w, self.block(w), self.block(w)).wait_recv()

    def wait_sent(self, step, ref):
        self.copy(step, 0, 0, ref, ref).wait_send()


class Spread:
    def __init__(self, place, axis, src, came, send, recv):
        self.p, self.axis, self.src, self.came, self.send, self.recv = place, axis, src, came, send, recv

    def start(self):
        for by in range(1, RING):
            to = self.p.to(self.axis, by)
            remote(self.src.at[self.p.index(self.axis, by)], self.came.at[by - 1], self.send, self.recv, to).start()

    def all(self):
        return remote(self.came, self.came, self.send, self.recv, self.p.to(self.axis, 1))


def every(lead, body):
    if not lead:
        body(())
        return
    count = 1
    for n in lead:
        count *= n

    @pl.loop(0, count)
    def _(i):
        body((div(i, lead[-1]), mod(i, lead[-1])) if len(lead) == 2 else (i,))


class Reduce:
    EVENTS = 7
    SLOTS = 2
    KINDS = {
        "gate": ("xyz", NJ, CH, (RING,), JOINED, ROWS),
        "up": ("yzx", NJ, CH, (RING,), JOINED, ROWS),
        "down": ("zxy", ND, MXU, (RING, RING), DROWS, DROWS),
    }

    def __init__(self, place, kind, term, out, hbm, far, near, sems):
        self.p, self.kind, self.out = place, kind, out
        self.axes, self.n, self.width, self.lead, _, _ = self.KINDS[kind]
        self.down = kind == "down"
        self.term_ref = term.reshape(L, RING, RING, RING, DROWS, D) if self.down else term.reshape(L, RING, RING, JOINED, FF)
        self.half = self.width // 2
        self.count = L * self.n
        self.x1o, self.x1f = hbm
        self.x2, self.x3 = far
        self.vo, self.vw, self.v1, self.vf, self.s, self.sb, self.t, self.tb = near
        self.ls, self.send, self.recv = sems

    def unit(self, step, j):
        self.l, self.j, self.u = L - 1 - step, j, step * self.n + j
        self.slot = self.u & 1

    @classmethod
    def scratch(cls, kind):
        _, n, w, lead, rows, last = cls.KINDS[kind]
        h, count = w // 2, L * n
        block, end = (*lead, rows), (last,)
        kept = (RING, RING, ROWS) if kind == "up" else block
        mid = kept[1:]
        dma, vm = pltpu.SemaphoreType.DMA, pltpu.VMEM
        hbm = [jax.ShapeDtypeStruct((count, 2, *block, c), BF) for c in (h, w)]
        far = [vm((n, RING - 1, *shape, w), BF) for shape in (mid, end)]
        near = [vm((2, *block, h), BF)] * 2 + [vm((cls.SLOTS, 2, *block, h), BF), vm((3, *block, w), BF)]
        near += [vm((cls.SLOTS, *kept, w), dtype) for dtype in (F32, BF)]
        near += [vm((cls.SLOTS, RING, *end, w), dtype) for dtype in (F32, BF)]
        return hbm, far, near, [dma((7,)), dma((n, RING)), dma((n, 2 * RING))]

    def halves(self, half):
        return pl.ds(half * self.half, self.half)

    def cut(self, ref, half):
        return ref.at[(ALL,) * (len(ref.shape) - 1) + (self.halves(half),)]

    def term(self, q, half=None):
        start = self.j * self.width
        cols = aligned(start, self.width) if half is None else aligned(start + half * self.half, self.half)
        if self.down:
            return self.term_ref.at[self.l, :, :, q, :, cols]
        if self.kind == "up":
            return self.term_ref.at[self.l, :, q, :, cols]
        return self.term_ref.at[self.l, q, :, :, cols]

    def ring(self, j=None):
        j = self.j if j is None else j
        opposite, block = self.x1o.at[self.u], self.x1f.at[self.u]
        sems = (lambda k: self.send.at[j, k], lambda k: self.recv.at[j, k])
        return Ring(self.p, self.axes[0], self.term, lambda w: opposite.at[w], lambda w, h=None: block.at[w] if h is None else self.cut(block.at[w], h), *sems)

    def spread(self, phase, j=None):
        j = self.j if j is None else j
        src, came = ((self.sb, self.x2), (self.tb, self.x3))[phase - 1]
        return Spread(self.p, self.axes[phase], src.at[self.slot], came.at[j], self.send.at[j, 1 + phase], self.recv.at[j, RING - 1 + phase])

    def loads(self, blocks):
        a = self.axes[0]
        if blocks:
            pairs = [(self.x1f.at[self.u, w], self.vf.at[w]) for w in BOTH] + [(self.term(self.p.index(a)), self.vf.at[2])]
        else:
            pairs = [(self.x1o.at[self.u, w], self.vo.at[w]) for w in BOTH]
            pairs += [(self.term(self.p.index(a, side(w)), w), self.vw.at[w]) for w in BOTH]
        return [local(s, d, self.ls.at[4 * blocks + i]) for i, (s, d) in enumerate(pairs)]

    def wait_sends(self, phase, j, second):
        if phase:
            self.spread(phase, j).all().wait_send()
        else:
            self.ring(j).wait_sent(int(second), self.v1.at[0] if second else self.x1f.at[0])

    def reuse(self, phase, second=False):
        back = self.SLOTS if second or phase else self.n

        @pl.when(self.u >= back)
        def _():
            j = self.j - back
            self.wait_sends(phase, jnp.where(j < 0, j + self.n, j), second)

    def start(self):
        self.reuse(0)
        for copy in self.ring().first():
            copy.start()

    def load_opposite(self):
        self.ring().wait_opposite()
        for copy in self.loads(False):
            copy.start()

    def add_opposite(self):
        for copy in self.loads(False):
            copy.wait()
        self.reuse(0, True)

        def add(i):
            for w in BOTH:
                self.v1[(self.slot, w, *i)] = (self.vo[(w, *i)].astype(F32) + self.vw[(w, *i)].astype(F32)).astype(BF)

        every(self.lead, add)
        for copy in self.ring().second(self.v1.at[self.slot]):
            copy.start()

    def load_block(self):
        self.ring().wait_block()
        for copy in self.loads(True):
            copy.start()

    def add_block(self):
        for copy in self.loads(True):
            copy.wait()
        self.reuse(1)

        def add(i):
            own, left, right = (self.vf[(w, *i)].astype(F32) for w in (2, 0, 1))
            total = own + left + right
            parts = [(i, total)]
            if self.kind == "up":
                parts = [((z, *i), total[ROWS * z : ROWS * (z + 1)]) for z in range(RING)]
            for at, part in parts:
                self.s[(self.slot, *at)] = part
                self.sb[(self.slot, *at)] = part.astype(BF)

        every(self.lead, add)
        self.spread(1).start()

    def total(self, own, came):
        for w in range(RING - 1):
            own = own + came(w).astype(F32)
        return own

    def turn(self):
        self.spread(1).all().wait_recv()
        self.reuse(2)
        q = self.p.index(self.axes[1])

        def total(i):
            return self.total(self.s[(self.slot, q, *i)], lambda w: self.x2[(self.j, w, *i)])

        def put(i, value):
            self.t[self.slot, i] = value
            self.tb[self.slot, i] = value.astype(BF)

        if self.kind != "gate":
            every((RING,), lambda i: put(*i, total(i)))
        else:
            whole = total(())
            for i in range(RING):
                put(i, whole[ROWS * i : ROWS * (i + 1)])
        self.spread(2).start()

    def finish(self):
        self.spread(2).all().wait_recv()
        total = self.total(self.t[self.slot, self.p.index(self.axes[2])], lambda w: self.x3[self.j, w])
        self.out[self.l, :, piece(self.j, self.width)] = total.astype(BF)

    def events(self):
        return (self.start, self.load_opposite, self.add_opposite, self.load_block, self.add_block, self.turn, self.finish)

    def drain(self):
        @pl.loop(0, self.n)
        def _(j):
            self.unit(L - 1, j)
            self.wait_sends(0, j, False)

            @pl.when(j >= self.n - self.SLOTS)
            def _():
                for phase in range(3):
                    self.wait_sends(phase, j, True)


class Reduces:
    PERIOD = ND + 1 + 2 * NJ + 8
    START = {"down": 9, "gate": ND + 1 + 3}
    LAGS = {"down": (0, 3, 4, 7, 8, 12, 16), "gate": (0, 2, 3, 6, 7, 10, 14)}

    def __init__(self, units):
        self.units = units

    def after(self):
        return max(self.at(units[0], -1) + 2 * units[0].n - 2 for units in self.units) + 1 - self.PERIOD

    def at(self, unit, k):
        return self.START[unit.kind] + self.LAGS[unit.kind][k]

    def tick(self, step, i):
        for odd in BOTH:

            @pl.when(i & 1 == odd)
            def _():
                for k in reversed(range(Reduce.EVENTS)):
                    for units in self.units:
                        at = self.at(units[0], k)
                        if at % 2 == odd:
                            self.event(units, k, step, i - at)

    def event(self, units, k, step, q):
        early = q < 0
        q = jnp.where(early, q + self.PERIOD, q)
        step = jnp.where(early, step - 1, step)

        @pl.when((q >= 0) & (q < 2 * units[0].n) & (step >= 0) & (step < L))
        def _():
            for unit in units:
                unit.unit(step, q >> 1)
                unit.events()[k]()

    def drain(self):
        for units in self.units:
            for unit in units:
                unit.drain()


def scale_of(wide):
    return lax.rsqrt(jnp.mean(wide * wide, -1, keepdims=True) + 1e-6)


def save_normed(h, rows, a, at, dst, sems, i):
    wide = h.astype(F32)
    tile = (wide * scale_of(wide)).astype(BF)
    a[rows, :] = tile
    slot = mod(i, 2)
    copy = local(at.at[slot], dst.at[:, rows], sems.at[slot])

    @pl.when(i >= 2)
    def _():
        copy.wait()

    at[slot] = tile.T
    copy.start()


def wait_normed(at, dst, sems):
    for slot in BOTH:
        local(at.at[slot], dst.at[:, piece(slot, MXU)], sems.at[slot]).wait()


TILE = 4 * MXU


def forward(first, along_z, gathers, fulls, ps, qs, ats, acts, hs, xb, a, at, wb, pq, actt, act, dn, sx, sa, sw, so, sd):
    def weights(l, j):
        return [local(fulls[m].at[l, :, piece(j, CH)], wb.at[mod(j, 2), m], sw.at[mod(j, 2), m]) for m in BOTH]

    def outs(l, s):
        slot = mod(s, 2)
        rows, cols = piece(slot, TILE), piece(div(s, 2), CH)
        pairs = [(pq.at[slot, 0], ps.at[l, rows, cols]), (pq.at[slot, 1], qs.at[l, rows, cols]), (actt.at[slot], acts.at[l, cols, rows])]
        return [local(src, dst, so.at[slot, i]) for i, (src, dst) in enumerate(pairs)]

    keep = local(xb, hs.at[0], sx.at[0])
    down = local(fulls[2].at[0], dn, sd.at[0])
    along_z.start()
    gathers.down.event(0, 0)
    along_z.finish(0)
    first.wait()
    keep.start()

    @pl.loop(0, gathers.AHEAD)
    def _(t):
        gathers.tick(t)
        for part in range(1, len(AlongZ.PARTS) - 1):

            @pl.when(t == min(2 * AlongZ.PARTS[part], gathers.AHEAD) - 1)
            def _():
                along_z.finish(part)

        @pl.when(t < T // MXU)
        def _():
            rows = piece(t, MXU)
            save_normed(xb[rows, :], rows, a, at, ats.at[0], sa, t)

    wait_normed(at, ats.at[0], sa)

    for copy in weights(0, 0):
        copy.start()

    @pl.loop(0, L)
    def _(l):
        @pl.loop(0, 2 * NJ)
        def _(s):
            j, i = div(s, 2), mod(s, 2)
            slot = mod(j, 2)

            @pl.when(i == 0)
            def _():
                for copy in weights(l, j):
                    copy.wait()

            gathers.tick(gathers.AHEAD + l * (2 * NJ + gathers.DEEP) + s)

            @pl.when(i == 1)
            def _():
                @pl.when(j < NJ - 1)
                def _():
                    for copy in weights(l, j + 1):
                        copy.start()

                @pl.when((j == NJ - 1) & (l == 0))
                def _():
                    down.start()

            @pl.when(s >= 2)
            def _():
                for copy in outs(l, s - 2):
                    copy.wait()

            for n in range(TILE // MXU):
                rows = piece(i * (TILE // MXU) + n, MXU)
                part = pl.ds(n * MXU, MXU)
                for half in BOTH:
                    cols = pl.ds(half * MXU, MXU)
                    gate, up = (dot(a[rows, :], wb[slot, m, :, cols]) for m in BOTH)
                    h = 0.5 * gate
                    t = jnp.tanh(h)
                    e = 1.0 + t
                    silu = h * e
                    pq[i, 0, part, cols] = silu
                    pq[i, 1, part, cols] = (0.5 * up) * (e * (1.0 + h * (1.0 - t)))
                    tile = (silu * up).astype(BF)
                    act[rows, aligned(j * CH + half * MXU, MXU)] = tile
                    actt[i, cols, part] = tile.T
            for copy in outs(l, s):
                copy.start()

        for s in (2 * NJ - 2, 2 * NJ - 1):
            for copy in outs(l, s):
                copy.wait()

        @pl.when(l == 0)
        def _():
            keep.wait()
            down.wait()

            @pl.loop(0, T // CH)
            def _(i):
                gathers.tick(gathers.AHEAD + 2 * NJ + i)

                @pl.when(i == T // CH - 1)
                def _():
                    for copy in weights(1, 0):
                        copy.start()

                rows = piece(i, CH)
                y = dot(act[rows, :], dn[...]).astype(BF)
                xb[rows, :] = (xb[rows, :].astype(F32) + y.astype(F32)).astype(BF)
                for n in BOTH:
                    sub = piece(2 * i + n, MXU)
                    save_normed(xb[sub, :], sub, a, at, ats.at[1], sa, 2 * i + n)

            wait_normed(at, ats.at[1], sa)
            local(xb, hs.at[1], sx.at[0]).start()

    local(xb, hs.at[1], sx.at[0]).wait()


def by_down(l, tick, first, acts, td, dh, av, st, sl, so):
    parts = 3

    def load(part):
        rows = piece(part, FF // parts)
        return local(acts.at[l, rows, :], av.at[rows, :], sl.at[part])

    for part in range(parts):
        load(part).start()

    def out(i):
        return local(st.at[mod(i, 2)], td.at[l, :, piece(i, MXU)], so.at[mod(i, 2)])

    @pl.loop(0, ND + 1)
    def _(n):
        i = n - 1

        @pl.when(i >= 2)
        def _():
            out(i - 2).wait()

        tick(n)

        @pl.when(i == 0)
        def _():
            first()

            @pl.loop(0, parts)
            def _(part):
                load(part).wait()
                rows = piece(part, FF // parts)
                st[0, rows, :] = dot(av[rows, :], dh[:, :MXU]).astype(BF)

        @pl.when(i > 0)
        def _():
            st[mod(i, 2)] = dot(av[...], dh[:, piece(i, MXU)]).astype(BF)

        @pl.when(i >= 0)
        def _():
            out(i).start()

    for i in (ND - 2, ND - 1):
        out(i).wait()


def by_gate_and_up(l, tick, ahead, wdf, ps, qs, ats, dgs, terms, dh, atv, wdb, pq, dgu, stw, sl, sw, sp, sd, so):
    tiles = T // TILE

    def weights(j):
        return local(wdf.at[l, piece(j, CH), :], wdb.at[mod(j, 2)], sw.at[mod(j, 2)])

    def factors(j, i):
        rows, cols = piece(i, TILE), piece(j, CH)
        return [local(src.at[l, rows, cols], pq.at[m, rows], sp.at[i, m]) for m, src in enumerate((qs, ps))]

    def load_factors(j):
        for i in range(tiles):
            for copy in factors(j, i):
                copy.start()

    def hidden(j):
        return [local(dgu.at[m], dgs[m].at[:, piece(j, CH)], sd.at[m]) for m in BOTH]

    def out(j):
        return [local(stw.at[m], terms[m].at[l, :, piece(j, CH)], so.at[m]) for m in BOTH]

    load = local(ats.at[l], atv, sl)
    weights(0).start()
    load_factors(0)
    load.start()

    def to_hidden(j):
        weights(j).wait()

        @pl.when(j < NJ - 1)
        def _():
            weights(j + 1).start()

        @pl.when(j > 0)
        def _():
            for copy in hidden(j - 1):
                copy.wait()

        @pl.loop(0, tiles)
        def _(i):
            for copy in factors(j, i):
                copy.wait()

            for n in range(TILE // MXU):
                rows = piece(i * (TILE // MXU) + n, MXU)
                for half in BOTH:
                    cols = pl.ds(half * MXU, MXU)
                    by_act = dot(dh[rows, :], wdb[mod(j, 2), cols, :], NT).astype(BF).astype(F32)
                    for m in BOTH:
                        dgu[m, rows, cols] = (by_act * pq[m, rows, cols]).astype(BF)

        for copy in hidden(j):
            copy.start()

    def to_weights(j):
        @pl.when(j == 0)
        def _():
            load.wait()

        @pl.when(j < NJ - 1)
        def _():
            load_factors(j + 1)

        @pl.when(j == NJ - 1)
        def _():
            ahead.start()

        for m in BOTH:
            stw[m] = dot(atv[...], dgu[m]).astype(BF)
        for copy in out(j):
            copy.start()

    @pl.loop(0, 2 * NJ)
    def _(h):
        j, late = div(h, 2), mod(h, 2)

        @pl.when((late == 1) & (j > 0))
        def _():
            for copy in out(j - 1):
                copy.wait()

        tick(ND + 1 + h)
        pl.when(late == 0)(lambda: to_hidden(j))
        pl.when(late == 1)(lambda: to_weights(j))

    for copy in hidden(NJ - 1) + out(NJ - 1):
        copy.wait()


def by_input(l, tick, ahead, full, dgs, hs, dh, first, second, gt, ht, sw, sg, sh):
    after = local(full.at[l], second, sw)
    tiles = T // MXU

    def rows_of(i):
        rows, slot = piece(i, MXU), mod(i, 2)
        return [local(dgs[m].at[rows, :], gt.at[slot, m], sg.at[slot, m]) for m in BOTH] + [local(hs.at[l, rows, :], ht.at[slot], sh.at[slot])]

    for copy in rows_of(0) + [after]:
        copy.start()

    @pl.loop(0, tiles)
    def _(i):
        tick(ND + 1 + 2 * NJ + i)
        for copy in rows_of(i):
            copy.wait()

        @pl.when(i < tiles - 1)
        def _():
            for copy in rows_of(i + 1):
                copy.start()

        @pl.when(i == 0)
        def _():
            ahead.wait()
            after.wait()

        rows, slot = piece(i, MXU), mod(i, 2)
        by_a = [dot(gt[slot, m], w[...], NT).astype(BF).astype(F32) for m, w in enumerate((first, second))]
        total = by_a[0] + by_a[1]
        wide = ht[slot].astype(F32)
        scale = scale_of(wide)
        along = jnp.mean(total * wide, -1, keepdims=True) * (scale * scale * scale)
        by_h = (total * scale - wide * along).astype(BF).astype(F32)
        dh[rows, :] = (dh[rows, :].astype(F32) + by_h).astype(BF)


def kernel(x, dy, wz, wd, dx, og, ou, od, *refs):
    def take(n):
        nonlocal refs
        head, refs = refs[:n], refs[n:]
        return head

    fulls, (ps, qs, ats, acts, hs), dgs, terms = take(3), take(5), take(2), take(3)
    hbm = [take(2) for _ in KINDS]
    zbuf, zcat, zs, zr = take(4)
    sems = take(4)
    far = [take(2) for _ in KINDS]
    rsems = [take(3) for _ in KINDS]
    sx, sa, sw, so, sd, sp, sg = take(7)
    place = Place()
    gathers = Gathers(place, fulls, zcat, wd, *sems)
    dma, vm = pltpu.SemaphoreType.DMA, pltpu.VMEM

    def ahead(xb, a, at, wb, pq, actt, act, dn):
        first = local(x, xb, sx.at[0])
        first.start()
        place.greet([place.to(a, by) for a in "xyz" for by in range(1, RING)] + [place.partner()])
        along_z = AlongZ(place, wz, zbuf, zcat, zs, zr)
        forward(first, along_z, gathers, fulls, ps, qs, ats, acts, hs, xb, a, at, wb, pq, actt, act, dn, sx, sa, sw, so, sd)
        gathers.drain()

    pl.run_scoped(
        ahead,
        vm((T, D), BF),
        vm((T, D), BF),
        vm((2, D, MXU), BF),
        vm((2, 2, D, CH), BF),
        vm((2, 2, TILE, CH), F32),
        vm((2, CH, TILE), BF),
        vm((T, FF), BF),
        vm((FF, D), BF),
    )

    def back(dh, *near):
        split = [near[i * 8 : i * 8 + 8] for i in range(3)]
        units = [
            Reduce(place, kind, terms[i], (og, ou, od)[i], hbm[i], far[i], split[i], rsems[i]) for i, kind in enumerate(KINDS)
        ]
        reduces = Reduces([units[2:], units[:2]])
        first = local(dy, dh, sx.at[0])
        first.start()

        @pl.loop(0, L)
        def _(step):
            l = L - 1 - step

            def tick(i):
                reduces.tick(step, i)

            pl.run_scoped(
                lambda av, st: by_down(
                    l, tick, lambda: pl.when(step == 0)(first.wait), acts, terms[2], dh, av, st, sp.at[0], so.at[0]
                ),
                vm((FF, T), BF),
                vm((2, FF, MXU), BF),
            )

            def rest(weight):
                ahead = local(fulls[0].at[l], weight, sx.at[0])
                pl.run_scoped(
                    lambda *v: by_gate_and_up(
                        l, tick, ahead, fulls[2], ps, qs, ats, dgs, terms, dh, *v, sd.at[0], sw.at[0], sp, sg.at[0], so.at[0]
                    ),
                    vm((D, T), BF),
                    vm((2, CH, D), BF),
                    vm((2, T, CH), F32),
                    vm((2, T, CH), BF),
                    vm((2, D, CH), BF),
                )
                pl.run_scoped(
                    lambda *v: by_input(l, tick, ahead, fulls[1], dgs, hs, dh, weight, *v, sa.at[0], sg, sd),
                    vm((D, FF), BF),
                    vm((2, 2, MXU, FF), BF),
                    vm((2, MXU, D), BF),
                )

            pl.run_scoped(rest, vm((D, FF), BF))

        end = local(dh, dx, sx.at[0])
        end.start()

        @pl.loop(0, reduces.after())
        def _(i):
            reduces.tick(L, i)

        end.wait()
        reduces.drain()

    pl.run_scoped(back, vm((T, D), BF), *(v for kind in KINDS for v in Reduce.scratch(kind)[2]))


KINDS = ("gate", "up", "down")


def call(x, dy, wz, wd):
    made = [Reduce.scratch(kind) for kind in KINDS]
    vmem, hbm = pl.BlockSpec(memory_space=pltpu.VMEM), pl.BlockSpec(memory_space=pltpu.HBM)
    dma, vm = pltpu.SemaphoreType.DMA, pltpu.VMEM

    def shape(*dims, dtype=BF):
        return jax.ShapeDtypeStruct(dims, dtype)

    work = [shape(L, D, FF), shape(L, D, FF), shape(L, FF, D)]
    work += [shape(L, T, FF, dtype=F32), shape(L, T, FF, dtype=F32), shape(L, D, T), shape(L, FF, T), shape(L, T, D)]
    work += [shape(T, FF), shape(T, FF), shape(L, D, FF), shape(L, D, FF), shape(L, FF, D)]
    work += [s for m in made for s in m[0]]
    outs = [shape(L, ROWS, FF), shape(L, ROWS, FF), shape(L, DROWS, D)]
    return pl.pallas_call(
        kernel,
        out_shape=(shape(T, D), *outs, *work),
        in_specs=[hbm, hbm, vmem, vmem],
        out_specs=(hbm, *(vmem for _ in outs), *(hbm for _ in work)),
        scratch_shapes=[
            vm((RING, UNITS, 2, ROWS, HC), BF),
            vm((UNITS, 2, JOINED, HC), BF),
            dma((len(AlongZ.PARTS) - 1, RING - 1)),
            dma((len(AlongZ.PARTS) - 1, RING - 1)),
            dma((NJ, 2, GatherUp.GROUPS + 1)),
            dma((NJ, 2, GatherUp.GROUPS)),
            dma((L, GatherDown.GROUPS + 1)),
            dma((L, GatherDown.GROUPS)),
            *(s for m in made for s in m[1]),
            *(s for m in made for s in m[3]),
            dma((1,)),
            dma((2,)),
            dma((2, 2)),
            dma((2, 3)),
            dma((2,)),
            dma((2, 3)),
            dma((2, 2)),
        ],
        name="train",
        compiler_params=pltpu.CompilerParams(collective_id=0, has_side_effects=True, vmem_limit_bytes=67_000_000),
    )(x, dy, wz, wd)[:4]


def solution(mesh):
    def step(x, dy, w_gate, w_up, w_down):
        wz = jnp.stack([w_gate, w_up], 1).reshape(L, 2, ROWS, NJ, 2, HC)
        wz = lax.dynamic_index_in_dim(wz, lax.axis_index("rep"), 4, keepdims=False).transpose(0, 3, 1, 2, 4).reshape(UNITS, 2, ROWS, HC)
        by_x, *by_w = call(x[0], dy[0], wz, w_down)
        return (by_x[None], *by_w)

    both, rows = P(("rep", "dp"), None, None), P(None, "dp", None)
    return jax.shard_map(
        step,
        mesh=mesh,
        in_specs=(both, both, rows, rows, rows),
        out_specs=(both, *(P("rep", "dp", None),) * 3),
        check_vma=False,
    )
```

```python
import jax
import jax.numpy as jnp
from jax import lax
from jax.experimental import pallas as pl
from jax.experimental.pallas import tpu as pltpu
from jax.sharding import PartitionSpec as P

MESH = pl.DeviceIdType.MESH
BF = jnp.bfloat16
F32 = jnp.float32
L, D, FF, T = 2, 1280, 3072, 2048
BOTH = range(2)
RING = 4
ROWS = D // 64
JOINED = RING * ROWS
DROWS = FF // 64
CH = 512
HC = CH // 2
NJ = FF // CH
UNITS = L * NJ
MXU = 256
ND = D // MXU
ALL = slice(None)
HALVES = (lambda: ALL, lambda: pl.ds(0, 2), lambda: pl.ds(2, 2))
NN = (((1,), (0,)), ((), ()))
NT = (((1,), (1,)), ((), ()))
LANES = 128


def dot(a, b, dims=NN):
    return lax.dot_general(a, b, dims, preferred_element_type=F32)


def local(src, dst, sem):
    return pltpu.make_async_copy(src, dst, sem)


def remote(src, dst, send, recv, device):
    return pltpu.make_async_remote_copy(src_ref=src, dst_ref=dst, send_sem=send, recv_sem=recv, device_id=device, device_id_type=MESH)


def aligned(start, size):
    return pl.ds(pl.multiple_of(start, LANES), size)


def piece(index, size):
    return aligned(index * size, size)


def mod(a, n):
    return lax.rem(a, n)


def div(a, n):
    return lax.div(a, n)


def side(way):
    return 1 - 2 * way


class Place:
    def __init__(self):
        self.core = lax.axis_index("rep")
        self.dp = lax.axis_index("dp")
        self.other = 1 - self.core
        self.place, self.device = {}, {}
        for stride, axis in ((RING**2, "x"), (RING, "y"), (1, "z")):
            at = mod(div(self.dp, stride), RING)
            for by in range(RING):
                self.place[axis, by] = mod(at + by, RING)
                self.device[axis, by] = (self.core, self.dp + (self.place[axis, by] - at) * stride)

    def to(self, axis, by):
        return self.device[axis, by % RING]

    def index(self, axis, by=0):
        return self.place[axis, by % RING]

    def partner(self):
        return (self.other, self.dp)

    def greet(self, others):
        barrier = pltpu.get_barrier_semaphore()
        for other in others:
            pl.semaphore_signal(barrier, inc=1, device_id=other, device_id_type=MESH)
        pl.semaphore_wait(barrier, len(others))


class Gather:
    def __init__(self, place, full, own, send, recv):
        self.p, self.full, self.own, self.send, self.recv = place, full, own, send, recv

    def ring(self, axis, ref, parts):
        whole, low, high = parts
        right, left = self.p.to(axis, 1), self.p.to(axis, -1)
        return [(lambda: ref(0, whole()), right), (lambda: ref(0, whole()), left), (lambda: ref(-1, low()), right), (lambda: ref(1, high()), left)]

    def hand(self, ref):
        return [(lambda by=by: ref(by), self.p.partner()) for by in (0, -1, 1, 2)]

    def copy(self, k):
        ref, device = self.table()[k][0](), self.table()[k][1]
        group = min(k // 2, self.GROUPS - 1)
        return remote(self.mine() if k < 2 else ref, ref, self.send.at[(*self.slot, group)], self.recv.at[(*self.slot, group)], device)

    def all_of(self, group):
        blocks = RING ** (group // 2) * (1 if group % 2 else 2)
        ref = self.some(RING**self.RINGS if group == self.GROUPS - 1 else blocks)
        return remote(ref, ref, self.send.at[(*self.slot, group)], self.recv.at[(*self.slot, group)], self.p.partner())

    def keep(self):
        return local(self.mine(), self.table()[0][0](), self.send.at[(*self.slot, self.GROUPS)])

    def event(self, k, l, j=0):
        self.unit(l, j)
        ends = 2 * self.RINGS
        starts = [2 * k, 2 * k + 1] if k < ends else []
        hand = {ends - 2: [0], ends - 1: [1, 2], ends: [3]}.get(k, [])
        if k < ends:
            self.free(k)
        if k == ends - 2:
            self.free(ends)
        if k == 0:
            self.keep().start()
        else:
            self.all_of(k - 1).wait_recv()
        if k == 2:
            self.keep().wait()
        for i in starts + [2 * ends + i for i in hand]:
            self.copy(i).start()

    def free(self, group):
        pass

    def drain(self, l, j=0):
        self.unit(l, j)
        for group in range(self.GROUPS):
            self.all_of(group).wait_send()


def first_blocks(count, dims):
    index = []
    for _ in range(dims):
        index.insert(0, ALL if count >= RING else pl.ds(0, count) if count > 1 else 0)
        count = max(count // RING, 1)
    return tuple(index)


class GatherUp(Gather):
    RINGS = 2
    GROUPS = 2 * RINGS + 1

    def __init__(self, which, *rest):
        super().__init__(*rest)
        self.which = which
        self.axes = "yx" if which else "xy"

    def unit(self, l, j):
        self.l, self.j, self.slot = l, j, (j, self.which)
        self.start = j * CH + self.p.core * HC

    def free(self, group):
        @pl.when(self.l > 0)
        def _():
            self.all_of(group).wait_send()

    def mine(self):
        return self.own.at[self.l * NJ + self.j, self.which]

    def cols(self, lo=0, size=HC):
        return aligned(self.start + lo, size)

    def view(self):
        return self.full.reshape(L, RING, RING, JOINED, FF)

    def row(self, b, cols, a):
        return self.view().at[self.l, b, a, :, cols] if self.which else self.view().at[self.l, a, b, :, cols]

    def some(self, count):
        return self.view().at[(self.l, *first_blocks(count, 2), ALL, self.cols())]

    def table(self):
        p = self.p
        a, b = self.axes
        parts = (self.cols, lambda: self.cols(0, LANES), lambda: self.cols(LANES, LANES))
        first = self.ring(a, lambda by, c: self.row(p.index(b), c, p.index(a, by)), parts)
        second = self.ring(b, lambda by, part: self.row(p.index(b, by), self.cols(), part), HALVES)
        return first + second + self.hand(lambda by: self.row(p.index(b, by), self.cols(), ALL))


class GatherDown(Gather):
    RINGS = 3
    GROUPS = 2 * RINGS + 1
    HALF = D // 2
    CUT = 384
    TICKS = ((-1, 1, 6, 8, 10, 17, 20, 21), (17, 19, 21, 23, 25, 32, 36, 37))

    def unit(self, l, _):
        self.l, self.slot = l, (l,)

    def cols(self):
        return aligned(self.p.core * self.HALF, self.HALF)

    def mine(self):
        return self.own.at[self.l, :, self.cols()]

    def view(self):
        return self.full.reshape(L, RING, RING, RING, DROWS, D)

    def some(self, count):
        return self.view().at[(self.l, *first_blocks(count, 3), ALL, self.cols())]

    def table(self):
        p = self.p
        x, y, z = (p.index(a) for a in "xyz")
        start = p.core * self.HALF
        parts = (self.cols, lambda: aligned(start, self.CUT), lambda: aligned(start + self.CUT, self.HALF - self.CUT))
        full, v = self.view(), self.l
        first = self.ring("x", lambda by, c: full.at[v, p.index("x", by), y, z, :, c], parts)
        second = self.ring("y", lambda by, part: full.at[v, part, p.index("y", by), z, :, self.cols()], HALVES)
        third = self.ring("z", lambda by, part: full.at[v, part, :, p.index("z", by), :, self.cols()], HALVES)
        return first + second + third + self.hand(lambda by: full.at[v, :, :, p.index("z", by), :, self.cols()])


class Gathers:
    LAGS = (0, 3, 5, 7, 8, 9)
    AHEAD = LAGS[-1] + 1
    DEEP = T // CH

    def __init__(self, place, fulls, zcat, wd, us, ur, ds, dr):
        self.ups = [GatherUp(m, place, fulls[m], zcat, us, ur) for m in BOTH]
        self.down = GatherDown(place, fulls[2], wd, ds, dr)

    def tick(self, t):
        for odd in BOTH:

            @pl.when(t & 1 == odd)
            def _():
                for k in reversed(range(len(self.LAGS))):
                    if self.LAGS[k] % 2 == odd:
                        self.step(k, t - self.LAGS[k])

        for k, (one, two) in enumerate(zip(*GatherDown.TICKS)):

            @pl.when((t == one) | (t == two))
            def _():
                self.down.event(k, jnp.where(t == two, 1, 0))

    def step(self, k, q):
        late = q >= 2 * NJ + self.DEEP
        q = jnp.where(late, q - self.DEEP, jnp.where(q < 2 * NJ, q, -1))

        @pl.when((q >= 0) & (q < 2 * UNITS))
        def _():
            l = jnp.where(late, 1, 0)
            for up in self.ups:
                up.event(k, l, (q >> 1) - NJ * l)

    def drain(self):
        @pl.loop(0, NJ)
        def _(j):
            for up in self.ups:
                up.drain(L - 1, j)

        @pl.loop(0, L)
        def _(v):
            self.down.drain(v)


class AlongZ:
    def __init__(self, place, wz, zbuf, zcat, send, recv):
        self.p, self.wz, self.zbuf, self.zcat, self.send, self.recv = place, wz, zbuf, zcat, send, recv
        self.z = place.index("z")

    PARTS = (0, 1, 3, NJ, UNITS)

    def copy(self, part, by, receive):
        units = pl.ds(self.PARTS[part], self.PARTS[part + 1] - self.PARTS[part])
        slot = self.p.index("z", -by) if receive else self.z
        sems = (self.send.at[part, by - 1], self.recv.at[part, by - 1])
        return remote(self.wz.at[units], self.zbuf.at[slot, units], *sems, self.p.to("z", by))

    def start(self):
        for part in range(len(self.PARTS) - 1):
            for by in range(1, RING):
                self.copy(part, by, False).start()
        self.zbuf[self.z] = self.wz[...]

    def finish(self, part):
        for receive in (True, False):
            for by in range(1, RING):
                copy = self.copy(part, by, receive)
                copy.wait_recv() if receive else copy.wait_send()

        @pl.loop(self.PARTS[part], self.PARTS[part + 1])
        def _(u):
            for m in BOTH:
                pieces = [self.zbuf[i, u, m].astype(F32) for i in range(RING)]
                self.zcat[u, m] = jnp.concatenate(pieces, axis=0).astype(BF)


class Ring:
    def __init__(self, place, axis, src, opposite, block, send, recv):
        self.p, self.axis, self.src, self.opposite, self.block, self.send, self.recv = place, axis, src, opposite, block, send, recv

    def copy(self, step, part, way, src, dst):
        return remote(src, dst, self.send(step), self.recv(2 * part + way), self.p.to(self.axis, side(way)))

    def first(self):
        p, a = self.p, self.axis
        far = [self.copy(0, 0, w, self.src(p.index(a, 2), w), self.opposite(w)) for w in BOTH]
        near = [self.copy(0, 1, w, self.src(p.index(a, side(w)), 1 - w), self.block(w, 1 - w)) for w in BOTH]
        return far + near

    def second(self, sums):
        return [self.copy(1, 1, w, sums.at[w], self.block(w, w)) for w in BOTH]

    def wait_opposite(self):
        for w in BOTH:
            self.copy(0, 0, w, self.opposite(w), self.opposite(w)).wait_recv()

    def wait_block(self):
        for w in BOTH:
            self.copy(0, 1, w, self.block(w), self.block(w)).wait_recv()

    def wait_sent(self, step, ref):
        self.copy(step, 0, 0, ref, ref).wait_send()


class Spread:
    def __init__(self, place, axis, src, came, send, recv):
        self.p, self.axis, self.src, self.came, self.send, self.recv = place, axis, src, came, send, recv

    def start(self):
        for by in range(1, RING):
            to = self.p.to(self.axis, by)
            remote(self.src.at[self.p.index(self.axis, by)], self.came.at[by - 1], self.send, self.recv, to).start()

    def all(self):
        return remote(self.came, self.came, self.send, self.recv, self.p.to(self.axis, 1))


def every(lead, body):
    if not lead:
        body(())
        return
    count = 1
    for n in lead:
        count *= n

    @pl.loop(0, count)
    def _(i):
        body((div(i, lead[-1]), mod(i, lead[-1])) if len(lead) == 2 else (i,))


class Reduce:
    EVENTS = 7
    SLOTS = 2
    KINDS = {
        "gate": ("xyz", NJ, CH, (RING,), JOINED, ROWS),
        "up": ("yzx", NJ, CH, (RING,), JOINED, ROWS),
        "down": ("zxy", ND, MXU, (RING, RING), DROWS, DROWS),
    }

    def __init__(self, place, kind, term, out, hbm, far, near, sems):
        self.p, self.kind, self.out = place, kind, out
        self.axes, self.n, self.width, self.lead, _, _ = self.KINDS[kind]
        self.down = kind == "down"
        self.term_ref = term.reshape(L, RING, RING, RING, DROWS, D) if self.down else term.reshape(L, RING, RING, JOINED, FF)
        self.half = self.width // 2
        self.count = L * self.n
        self.x1o, self.x1f = hbm
        self.x2, self.x3 = far
        self.vo, self.vw, self.v1, self.vf, self.s, self.sb, self.t, self.tb = near
        self.ls, self.send, self.recv = sems

    def unit(self, step, j):
        self.l, self.j, self.u = L - 1 - step, j, step * self.n + j
        self.slot = self.u & 1

    @classmethod
    def scratch(cls, kind):
        _, n, w, lead, rows, last = cls.KINDS[kind]
        h, count = w // 2, L * n
        block, end = (*lead, rows), (last,)
        kept = (RING, RING, ROWS) if kind == "up" else block
        mid = kept[1:]
        dma, vm = pltpu.SemaphoreType.DMA, pltpu.VMEM
        hbm = [jax.ShapeDtypeStruct((count, 2, *block, c), BF) for c in (h, w)]
        far = [vm((n, RING - 1, *shape, w), BF) for shape in (mid, end)]
        near = [vm((2, *block, h), BF)] * 2 + [vm((cls.SLOTS, 2, *block, h), BF), vm((3, *block, w), BF)]
        near += [vm((cls.SLOTS, *kept, w), dtype) for dtype in (F32, BF)]
        near += [vm((cls.SLOTS, RING, *end, w), dtype) for dtype in (F32, BF)]
        return hbm, far, near, [dma((7,)), dma((n, RING)), dma((n, 2 * RING))]

    def halves(self, half):
        return pl.ds(half * self.half, self.half)

    def cut(self, ref, half):
        return ref.at[(ALL,) * (len(ref.shape) - 1) + (self.halves(half),)]

    def term(self, q, half=None):
        start = self.j * self.width
        cols = aligned(start, self.width) if half is None else aligned(start + half * self.half, self.half)
        if self.down:
            return self.term_ref.at[self.l, :, :, q, :, cols]
        if self.kind == "up":
            return self.term_ref.at[self.l, :, q, :, cols]
        return self.term_ref.at[self.l, q, :, :, cols]

    def ring(self, j=None):
        j = self.j if j is None else j
        opposite, block = self.x1o.at[self.u], self.x1f.at[self.u]
        sems = (lambda k: self.send.at[j, k], lambda k: self.recv.at[j, k])
        return Ring(self.p, self.axes[0], self.term, lambda w: opposite.at[w], lambda w, h=None: block.at[w] if h is None else self.cut(block.at[w], h), *sems)

    def spread(self, phase, j=None):
        j = self.j if j is None else j
        src, came = ((self.sb, self.x2), (self.tb, self.x3))[phase - 1]
        return Spread(self.p, self.axes[phase], src.at[self.slot], came.at[j], self.send.at[j, 1 + phase], self.recv.at[j, RING - 1 + phase])

    def loads(self, blocks):
        a = self.axes[0]
        if blocks:
            pairs = [(self.x1f.at[self.u, w], self.vf.at[w]) for w in BOTH] + [(self.term(self.p.index(a)), self.vf.at[2])]
        else:
            pairs = [(self.x1o.at[self.u, w], self.vo.at[w]) for w in BOTH]
            pairs += [(self.term(self.p.index(a, side(w)), w), self.vw.at[w]) for w in BOTH]
        return [local(s, d, self.ls.at[4 * blocks + i]) for i, (s, d) in enumerate(pairs)]

    def wait_sends(self, phase, j, second):
        if phase:
            self.spread(phase, j).all().wait_send()
        else:
            self.ring(j).wait_sent(int(second), self.v1.at[0] if second else self.x1f.at[0])

    def reuse(self, phase, second=False):
        back = self.SLOTS if second or phase else self.n

        @pl.when(self.u >= back)
        def _():
            j = self.j - back
            self.wait_sends(phase, jnp.where(j < 0, j + self.n, j), second)

    def start(self):
        self.reuse(0)
        for copy in self.ring().first():
            copy.start()

    def load_opposite(self):
        self.ring().wait_opposite()
        for copy in self.loads(False):
            copy.start()

    def add_opposite(self):
        for copy in self.loads(False):
            copy.wait()
        self.reuse(0, True)

        def add(i):
            for w in BOTH:
                self.v1[(self.slot, w, *i)] = (self.vo[(w, *i)].astype(F32) + self.vw[(w, *i)].astype(F32)).astype(BF)

        every(self.lead, add)
        for copy in self.ring().second(self.v1.at[self.slot]):
            copy.start()

    def load_block(self):
        self.ring().wait_block()
        for copy in self.loads(True):
            copy.start()

    def add_block(self):
        for copy in self.loads(True):
            copy.wait()
        self.reuse(1)

        def add(i):
            own, left, right = (self.vf[(w, *i)].astype(F32) for w in (2, 0, 1))
            total = own + left + right
            parts = [(i, total)]
            if self.kind == "up":
                parts = [((z, *i), total[ROWS * z : ROWS * (z + 1)]) for z in range(RING)]
            for at, part in parts:
                self.s[(self.slot, *at)] = part
                self.sb[(self.slot, *at)] = part.astype(BF)

        every(self.lead, add)
        self.spread(1).start()

    def total(self, own, came):
        for w in range(RING - 1):
            own = own + came(w).astype(F32)
        return own

    def turn(self):
        self.spread(1).all().wait_recv()
        self.reuse(2)
        q = self.p.index(self.axes[1])

        def total(i):
            return self.total(self.s[(self.slot, q, *i)], lambda w: self.x2[(self.j, w, *i)])

        def put(i, value):
            self.t[self.slot, i] = value
            self.tb[self.slot, i] = value.astype(BF)

        if self.kind != "gate":
            every((RING,), lambda i: put(*i, total(i)))
        else:
            whole = total(())
            for i in range(RING):
                put(i, whole[ROWS * i : ROWS * (i + 1)])
        self.spread(2).start()

    def finish(self):
        self.spread(2).all().wait_recv()
        total = self.total(self.t[self.slot, self.p.index(self.axes[2])], lambda w: self.x3[self.j, w])
        self.out[self.l, :, piece(self.j, self.width)] = total.astype(BF)

    def events(self):
        return (self.start, self.load_opposite, self.add_opposite, self.load_block, self.add_block, self.turn, self.finish)

    def drain(self):
        @pl.loop(0, self.n)
        def _(j):
            self.unit(L - 1, j)
            self.wait_sends(0, j, False)

            @pl.when(j >= self.n - self.SLOTS)
            def _():
                for phase in range(3):
                    self.wait_sends(phase, j, True)


class Reduces:
    PERIOD = ND + 1 + 2 * NJ + 8
    START = {"down": 9, "gate": ND + 1 + 3}
    LAGS = {"down": (0, 3, 4, 7, 8, 12, 16), "gate": (0, 2, 3, 6, 7, 10, 14)}

    def __init__(self, units):
        self.units = units

    def after(self):
        return max(self.at(units[0], -1) + 2 * units[0].n - 2 for units in self.units) + 1 - self.PERIOD

    def at(self, unit, k):
        return self.START[unit.kind] + self.LAGS[unit.kind][k]

    def tick(self, step, i):
        for odd in BOTH:

            @pl.when(i & 1 == odd)
            def _():
                for k in reversed(range(Reduce.EVENTS)):
                    for units in self.units:
                        at = self.at(units[0], k)
                        if at % 2 == odd:
                            self.event(units, k, step, i - at)

    def event(self, units, k, step, q):
        early = q < 0
        q = jnp.where(early, q + self.PERIOD, q)
        step = jnp.where(early, step - 1, step)

        @pl.when((q >= 0) & (q < 2 * units[0].n) & (step >= 0) & (step < L))
        def _():
            for unit in units:
                unit.unit(step, q >> 1)
                unit.events()[k]()

    def drain(self):
        for units in self.units:
            for unit in units:
                unit.drain()


def scale_of(wide):
    return lax.rsqrt(jnp.mean(wide * wide, -1, keepdims=True) + 1e-6)


def save_normed(h, rows, a, at, dst, sems, i):
    wide = h.astype(F32)
    tile = (wide * scale_of(wide)).astype(BF)
    a[rows, :] = tile
    slot = mod(i, 2)
    copy = local(at.at[slot], dst.at[:, rows], sems.at[slot])

    @pl.when(i >= 2)
    def _():
        copy.wait()

    at[slot] = tile.T
    copy.start()


def wait_normed(at, dst, sems):
    for slot in BOTH:
        local(at.at[slot], dst.at[:, piece(slot, MXU)], sems.at[slot]).wait()


TILE = 4 * MXU


def forward(first, along_z, gathers, fulls, ps, qs, ats, acts, hs, xb, a, at, wb, pq, actt, act, dn, sx, sa, sw, so, sd):
    def weights(l, j):
        return [local(fulls[m].at[l, :, piece(j, CH)], wb.at[mod(j, 2), m], sw.at[mod(j, 2), m]) for m in BOTH]

    def outs(l, s):
        slot = mod(s, 2)
        rows, cols = piece(slot, TILE), piece(div(s, 2), CH)
        pairs = [(pq.at[slot, 0], ps.at[l, rows, cols]), (pq.at[slot, 1], qs.at[l, rows, cols]), (actt.at[slot], acts.at[l, cols, rows])]
        return [local(src, dst, so.at[slot, i]) for i, (src, dst) in enumerate(pairs)]

    keep = local(xb, hs.at[0], sx.at[0])
    down = local(fulls[2].at[0], dn, sd.at[0])
    along_z.start()
    gathers.down.event(0, 0)
    along_z.finish(0)
    first.wait()
    keep.start()

    @pl.loop(0, gathers.AHEAD)
    def _(t):
        gathers.tick(t)
        for part in range(1, len(AlongZ.PARTS) - 1):

            @pl.when(t == min(2 * AlongZ.PARTS[part], NJ + 1) - 1)
            def _():
                along_z.finish(part)

        @pl.when(t < T // MXU)
        def _():
            rows = piece(t, MXU)
            save_normed(xb[rows, :], rows, a, at, ats.at[0], sa, t)

    wait_normed(at, ats.at[0], sa)

    for copy in weights(0, 0):
        copy.start()

    @pl.loop(0, L)
    def _(l):
        @pl.loop(0, 2 * NJ)
        def _(s):
            j, i = div(s, 2), mod(s, 2)
            slot = mod(j, 2)

            @pl.when(i == 0)
            def _():
                for copy in weights(l, j):
                    copy.wait()

            gathers.tick(gathers.AHEAD + l * (2 * NJ + gathers.DEEP) + s)

            @pl.when(i == 1)
            def _():
                @pl.when(j < NJ - 1)
                def _():
                    for copy in weights(l, j + 1):
                        copy.start()

                @pl.when((j == NJ - 1) & (l == 0))
                def _():
                    down.start()

            @pl.when(s >= 2)
            def _():
                for copy in outs(l, s - 2):
                    copy.wait()

            for n in range(TILE // MXU):
                rows = piece(i * (TILE // MXU) + n, MXU)
                part = pl.ds(n * MXU, MXU)
                for half in BOTH:
                    cols = pl.ds(half * MXU, MXU)
                    gate, up = (dot(a[rows, :], wb[slot, m, :, cols]) for m in BOTH)
                    h = 0.5 * gate
                    t = jnp.tanh(h)
                    e = 1.0 + t
                    silu = h * e
                    pq[i, 0, part, cols] = silu
                    pq[i, 1, part, cols] = (0.5 * up) * (e * (1.0 + h * (1.0 - t)))
                    tile = (silu * up).astype(BF)
                    act[rows, aligned(j * CH + half * MXU, MXU)] = tile
                    actt[i, cols, part] = tile.T
            for copy in outs(l, s):
                copy.start()

        for s in (2 * NJ - 2, 2 * NJ - 1):
            for copy in outs(l, s):
                copy.wait()

        @pl.when(l == 0)
        def _():
            keep.wait()
            down.wait()

            @pl.loop(0, T // CH)
            def _(i):
                gathers.tick(gathers.AHEAD + 2 * NJ + i)

                @pl.when(i == T // CH - 1)
                def _():
                    for copy in weights(1, 0):
                        copy.start()

                rows = piece(i, CH)
                y = dot(act[rows, :], dn[...]).astype(BF)
                xb[rows, :] = (xb[rows, :].astype(F32) + y.astype(F32)).astype(BF)
                for n in BOTH:
                    sub = piece(2 * i + n, MXU)
                    save_normed(xb[sub, :], sub, a, at, ats.at[1], sa, 2 * i + n)

            wait_normed(at, ats.at[1], sa)
            local(xb, hs.at[1], sx.at[0]).start()

    local(xb, hs.at[1], sx.at[0]).wait()


def by_down(l, tick, first, acts, td, dh, av, st, sl, so):
    parts = 3

    def load(part):
        rows = piece(part, FF // parts)
        return local(acts.at[l, rows, :], av.at[rows, :], sl.at[part])

    for part in range(parts):
        load(part).start()

    def out(i):
        return local(st.at[mod(i, 2)], td.at[l, :, piece(i, MXU)], so.at[mod(i, 2)])

    @pl.loop(0, ND + 1)
    def _(n):
        i = n - 1

        @pl.when(i >= 2)
        def _():
            out(i - 2).wait()

        tick(n)

        @pl.when(i == 0)
        def _():
            first()

            @pl.loop(0, parts)
            def _(part):
                load(part).wait()
                rows = piece(part, FF // parts)
                st[0, rows, :] = dot(av[rows, :], dh[:, :MXU]).astype(BF)

        @pl.when(i > 0)
        def _():
            st[mod(i, 2)] = dot(av[...], dh[:, piece(i, MXU)]).astype(BF)

        @pl.when(i >= 0)
        def _():
            out(i).start()

    for i in (ND - 2, ND - 1):
        out(i).wait()


def by_gate_and_up(l, tick, ahead, wdf, ps, qs, ats, dgs, terms, dh, atv, wdb, pq, dgu, stw, sl, sw, sp, sd, so):
    tiles = T // TILE

    def weights(j):
        return local(wdf.at[l, piece(j, CH), :], wdb.at[mod(j, 2)], sw.at[mod(j, 2)])

    def factors(j, i):
        rows, cols = piece(i, TILE), piece(j, CH)
        return [local(src.at[l, rows, cols], pq.at[m, rows], sp.at[i, m]) for m, src in enumerate((qs, ps))]

    def load_factors(j):
        for i in range(tiles):
            for copy in factors(j, i):
                copy.start()

    def hidden(j):
        return [local(dgu.at[m], dgs[m].at[:, piece(j, CH)], sd.at[m]) for m in BOTH]

    def out(j):
        return [local(stw.at[m], terms[m].at[l, :, piece(j, CH)], so.at[m]) for m in BOTH]

    load = local(ats.at[l], atv, sl)
    weights(0).start()
    load_factors(0)
    load.start()

    def to_hidden(j):
        weights(j).wait()

        @pl.when(j < NJ - 1)
        def _():
            weights(j + 1).start()

        @pl.when(j > 0)
        def _():
            for copy in hidden(j - 1):
                copy.wait()

        @pl.loop(0, tiles)
        def _(i):
            for copy in factors(j, i):
                copy.wait()

            for n in range(TILE // MXU):
                rows = piece(i * (TILE // MXU) + n, MXU)
                for half in BOTH:
                    cols = pl.ds(half * MXU, MXU)
                    by_act = dot(dh[rows, :], wdb[mod(j, 2), cols, :], NT).astype(BF).astype(F32)
                    for m in BOTH:
                        dgu[m, rows, cols] = (by_act * pq[m, rows, cols]).astype(BF)

        for copy in hidden(j):
            copy.start()

    def to_weights(j):
        @pl.when(j == 0)
        def _():
            load.wait()

        @pl.when(j < NJ - 1)
        def _():
            load_factors(j + 1)

        @pl.when(j == NJ - 1)
        def _():
            ahead.start()

        for m in BOTH:
            stw[m] = dot(atv[...], dgu[m]).astype(BF)
        for copy in out(j):
            copy.start()

    @pl.loop(0, 2 * NJ)
    def _(h):
        j, late = div(h, 2), mod(h, 2)

        @pl.when((late == 1) & (j > 0))
        def _():
            for copy in out(j - 1):
                copy.wait()

        tick(ND + 1 + h)
        pl.when(late == 0)(lambda: to_hidden(j))
        pl.when(late == 1)(lambda: to_weights(j))

    for copy in hidden(NJ - 1) + out(NJ - 1):
        copy.wait()


def by_input(l, tick, ahead, full, dgs, hs, dh, first, second, gt, ht, sw, sg, sh):
    after = local(full.at[l], second, sw)
    tiles = T // MXU

    def rows_of(i):
        rows, slot = piece(i, MXU), mod(i, 2)
        return [local(dgs[m].at[rows, :], gt.at[slot, m], sg.at[slot, m]) for m in BOTH] + [local(hs.at[l, rows, :], ht.at[slot], sh.at[slot])]

    for copy in rows_of(0) + [after]:
        copy.start()

    @pl.loop(0, tiles)
    def _(i):
        tick(ND + 1 + 2 * NJ + i)
        for copy in rows_of(i):
            copy.wait()

        @pl.when(i < tiles - 1)
        def _():
            for copy in rows_of(i + 1):
                copy.start()

        @pl.when(i == 0)
        def _():
            ahead.wait()
            after.wait()

        rows, slot = piece(i, MXU), mod(i, 2)
        by_a = [dot(gt[slot, m], w[...], NT).astype(BF).astype(F32) for m, w in enumerate((first, second))]
        total = by_a[0] + by_a[1]
        wide = ht[slot].astype(F32)
        scale = scale_of(wide)
        along = jnp.mean(total * wide, -1, keepdims=True) * (scale * scale * scale)
        by_h = (total * scale - wide * along).astype(BF).astype(F32)
        dh[rows, :] = (dh[rows, :].astype(F32) + by_h).astype(BF)


def kernel(x, dy, wz, wd, dx, og, ou, od, *refs):
    def take(n):
        nonlocal refs
        head, refs = refs[:n], refs[n:]
        return head

    fulls, (ps, qs, ats, acts, hs), dgs, terms = take(3), take(5), take(2), take(3)
    hbm = [take(2) for _ in KINDS]
    zbuf, zcat, zs, zr = take(4)
    sems = take(4)
    far = [take(2) for _ in KINDS]
    rsems = [take(3) for _ in KINDS]
    sx, sa, sw, so, sd, sp, sg = take(7)
    place = Place()
    gathers = Gathers(place, fulls, zcat, wd, *sems)
    dma, vm = pltpu.SemaphoreType.DMA, pltpu.VMEM

    def ahead(xb, a, at, wb, pq, actt, act, dn):
        first = local(x, xb, sx.at[0])
        first.start()
        place.greet([place.to(a, by) for a in "xyz" for by in range(1, RING)] + [place.partner()])
        along_z = AlongZ(place, wz, zbuf, zcat, zs, zr)
        forward(first, along_z, gathers, fulls, ps, qs, ats, acts, hs, xb, a, at, wb, pq, actt, act, dn, sx, sa, sw, so, sd)
        gathers.drain()

    pl.run_scoped(
        ahead,
        vm((T, D), BF),
        vm((T, D), BF),
        vm((2, D, MXU), BF),
        vm((2, 2, D, CH), BF),
        vm((2, 2, TILE, CH), F32),
        vm((2, CH, TILE), BF),
        vm((T, FF), BF),
        vm((FF, D), BF),
    )

    def back(dh, *near):
        split = [near[i * 8 : i * 8 + 8] for i in range(3)]
        units = [
            Reduce(place, kind, terms[i], (og, ou, od)[i], hbm[i], far[i], split[i], rsems[i]) for i, kind in enumerate(KINDS)
        ]
        reduces = Reduces([units[2:], units[:2]])
        first = local(dy, dh, sx.at[0])
        first.start()

        @pl.loop(0, L)
        def _(step):
            l = L - 1 - step

            def tick(i):
                reduces.tick(step, i)

            pl.run_scoped(
                lambda av, st: by_down(
                    l, tick, lambda: pl.when(step == 0)(first.wait), acts, terms[2], dh, av, st, sp.at[0], so.at[0]
                ),
                vm((FF, T), BF),
                vm((2, FF, MXU), BF),
            )

            def rest(weight):
                ahead = local(fulls[0].at[l], weight, sx.at[0])
                pl.run_scoped(
                    lambda *v: by_gate_and_up(
                        l, tick, ahead, fulls[2], ps, qs, ats, dgs, terms, dh, *v, sd.at[0], sw.at[0], sp, sg.at[0], so.at[0]
                    ),
                    vm((D, T), BF),
                    vm((2, CH, D), BF),
                    vm((2, T, CH), F32),
                    vm((2, T, CH), BF),
                    vm((2, D, CH), BF),
                )
                pl.run_scoped(
                    lambda *v: by_input(l, tick, ahead, fulls[1], dgs, hs, dh, weight, *v, sa.at[0], sg, sd),
                    vm((D, FF), BF),
                    vm((2, 2, MXU, FF), BF),
                    vm((2, MXU, D), BF),
                )

            pl.run_scoped(rest, vm((D, FF), BF))

        end = local(dh, dx, sx.at[0])
        end.start()

        @pl.loop(0, reduces.after())
        def _(i):
            reduces.tick(L, i)

        end.wait()
        reduces.drain()

    pl.run_scoped(back, vm((T, D), BF), *(v for kind in KINDS for v in Reduce.scratch(kind)[2]))


KINDS = ("gate", "up", "down")


def call(x, dy, wz, wd):
    made = [Reduce.scratch(kind) for kind in KINDS]
    vmem, hbm = pl.BlockSpec(memory_space=pltpu.VMEM), pl.BlockSpec(memory_space=pltpu.HBM)
    dma, vm = pltpu.SemaphoreType.DMA, pltpu.VMEM

    def shape(*dims, dtype=BF):
        return jax.ShapeDtypeStruct(dims, dtype)

    work = [shape(L, D, FF), shape(L, D, FF), shape(L, FF, D)]
    work += [shape(L, T, FF, dtype=F32), shape(L, T, FF, dtype=F32), shape(L, D, T), shape(L, FF, T), shape(L, T, D)]
    work += [shape(T, FF), shape(T, FF), shape(L, D, FF), shape(L, D, FF), shape(L, FF, D)]
    work += [s for m in made for s in m[0]]
    outs = [shape(L, ROWS, FF), shape(L, ROWS, FF), shape(L, DROWS, D)]
    return pl.pallas_call(
        kernel,
        out_shape=(shape(T, D), *outs, *work),
        in_specs=[hbm, hbm, vmem, vmem],
        out_specs=(hbm, *(vmem for _ in outs), *(hbm for _ in work)),
        scratch_shapes=[
            vm((RING, UNITS, 2, ROWS, HC), BF),
            vm((UNITS, 2, JOINED, HC), BF),
            dma((len(AlongZ.PARTS) - 1, RING - 1)),
            dma((len(AlongZ.PARTS) - 1, RING - 1)),
            dma((NJ, 2, GatherUp.GROUPS + 1)),
            dma((NJ, 2, GatherUp.GROUPS)),
            dma((L, GatherDown.GROUPS + 1)),
            dma((L, GatherDown.GROUPS)),
            *(s for m in made for s in m[1]),
            *(s for m in made for s in m[3]),
            dma((1,)),
            dma((2,)),
            dma((2, 2)),
            dma((2, 3)),
            dma((2,)),
            dma((2, 3)),
            dma((2, 2)),
        ],
        name="train",
        compiler_params=pltpu.CompilerParams(collective_id=0, has_side_effects=True, vmem_limit_bytes=67_000_000),
    )(x, dy, wz, wd)[:4]


def solution(mesh):
    def step(x, dy, w_gate, w_up, w_down):
        wz = jnp.stack([w_gate, w_up], 1).reshape(L, 2, ROWS, NJ, 2, HC)
        wz = lax.dynamic_index_in_dim(wz, lax.axis_index("rep"), 4, keepdims=False).transpose(0, 3, 1, 2, 4).reshape(UNITS, 2, ROWS, HC)
        by_x, *by_w = call(x[0], dy[0], wz, w_down)
        return (by_x[None], *by_w)

    both, rows = P(("rep", "dp"), None, None), P(None, "dp", None)
    return jax.shard_map(
        step,
        mesh=mesh,
        in_specs=(both, both, rows, rows, rows),
        out_specs=(both, *(P("rep", "dp", None),) * 3),
        check_vma=False,
    )
```
